32 devices in a mesh: sweep: 2 (over y), expert: 4 (over z), dp: 4 (over x, core).
Axes of the slice: x: 2, y: 2, z: 4, core: 2. Of those that a mesh axis runs over, the one named last changes fastest.
Arguments:
- tokens: bfloat16 [4096, 1536], P(('sweep', 'expert', 'dp')), parts along dimension 0, may hold values from -6 to 6
- expert_ids: int32 [4096, 8], P(('sweep', 'expert', 'dp')), parts along dimension 0, may hold values from 0 to 63, all different within a row; in each aligned block of 128 rows (0 to 127, 128 to 255, ...) at most 20 rows name the same one
- gate_weights: float32 [4096, 8], P(('sweep', 'expert', 'dp')), parts along dimension 0, may hold values from 0.1 to 0.6
- expert_in: bfloat16 [128, 1536, 768], P(('sweep', 'expert'), 'dp'), parts along dimension 0, may hold values from -0.15625 to 0.15625
- expert_out: bfloat16 [128, 768, 1536], P(('sweep', 'expert'), None, 'dp'), parts along dimension 0, may hold values from -0.21875 to 0.21875
- shared_in: bfloat16 [3072, 768], P(('sweep', 'dp')), parts along dimension 0, may hold values from -0.15625 to 0.15625
- shared_out: bfloat16 [1536, 1536], P('sweep', 'dp'), parts along dimension 0, may hold values from -0.21875 to 0.21875
Outputs:
- block_out: bfloat16 [4096, 1536], P(('sweep', 'expert', 'dp')), parts along dimension 0
The draws below stay inside these ranges and needn't reach their ends.
There are 2 independent parts, one for each index of `sweep`. The reference program is written for one: setup_inputs(seed, part) draws one part's arguments, and reference() takes and returns one part's arrays. A program takes and returns all parts, laid end to end along the dimension named above; each array names one. Nothing has to cross between parts.
Inputs may be any that keep to these rules, and one draw needn't show every extreme that they name: `expert_ids`: each token names 8 different experts. In each aligned block of 128 tokens (the tokens of one device) no expert is named by more than 20 tokens; some blocks have an expert named by exactly 20.
All inputs are finite; a program needn't handle non-finite values.
Results may differ from the reference program's by a relative error of at most 0.0051.
Values may be sent and summed in bfloat16 or wider, within the bound.
A program may use at most 192 MiB of HBM per device.

```python
import math
import jax
import jax.numpy as jnp
import numpy as np
from jax import lax

D = 1536
FF = 768
EXPERTS = 64
TOPK = 8
TOK_DEV = 128
CAP = 20
TOKENS = 2048


def levels(rng, shape, split, least, top_value):
    def one(position, parts):
        heights = jax.random.uniform(jax.random.fold_in(jax.random.fold_in(rng, 6), position), (parts,), jnp.float32, least / len(split), top_value / len(split))
        return jnp.repeat(jnp.exp(heights), shape[position] // parts).reshape((-1,) + (1,) * (len(shape) - position - 1))

    loudness = one(*split[0])
    for cut in split[1:]:
        loudness = loudness * one(*cut)
    return loudness


def assign_block(key, own, number, rows, amount, top, reach, slope):
    sequence = jax.random.permutation(key, amount)
    heavy_load, usual = load_shares(amount, rows * top, reach, slope, True), load_shares(amount, rows * top, reach, slope, False)
    places = jnp.arange(amount)

    def named(lengths, rotation):
        used = int((lengths > 0).sum())
        fixed = max(1, used // 4)
        moved = fixed + (places - fixed + rotation * (used - fixed)) % max(1, amount - fixed)
        return jnp.zeros((amount,), jnp.int32).at[sequence[jnp.where(places < fixed, places, moved)]].set(jnp.asarray(lengths, jnp.int32))

    lengths = jnp.where(number % 4 == 0, named(heavy_load, number // 4), named(usual, number - number // 4 - 1))
    mixed = jax.random.permutation(jax.random.fold_in(own, 3), amount)
    donor, taker = mixed[0:amount // 2 * 2:2], mixed[1:amount // 2 * 2:2]
    margin = jnp.minimum(lengths[donor] - 1, reach - lengths[taker]) // 2
    margin = jnp.where((donor == sequence[0]) | (taker == sequence[0]) | (lengths[taker] == 0), 0, jnp.maximum(margin, 0))
    moved = jax.random.randint(jax.random.fold_in(own, 4), (amount // 2,), 0, 1 << 20) % (margin + 1)
    lengths = lengths.at[donor].add(-moved).at[taker].add(moved)
    labels = jnp.searchsorted(jnp.cumsum(lengths), jnp.arange(rows * top), side="right").astype(jnp.int32)
    listing = labels.reshape(top, rows).T
    listing = listing[jax.random.permutation(jax.random.fold_in(own, 1), rows)]
    rotation = jax.random.randint(jax.random.fold_in(own, 2), (rows, 1), 0, top)
    return jnp.take_along_axis(listing, (jnp.arange(top)[None, :] + rotation) % top, axis=1)


def load_shares(amount, total, reach, lean, full):
    loads = [(1 << 20) // math.isqrt(grade ** lean) + 1 for grade in range(1, amount + 1)]
    largest = reach if full else min(reach, max(-(-total // amount), total * loads[0] // sum(loads)))
    least = 1 if total - largest >= amount - 1 else 0
    given, spare = [largest] + [least] * (amount - 1), total - largest - least * (amount - 1)
    while spare > 0:
        movable = [i for i in range(1, amount) if given[i] < largest] or [i for i in range(1, amount) if given[i] < reach]
        mass, budget = sum([loads[i] for i in movable]), spare
        for i in movable:
            extra = min(reach - given[i], max(1, budget * loads[i] // mass), spare)
            given[i] = given[i] + extra
            spare = spare - extra
    return np.array(given)


def scatter_about(own_key, dims, scale, limit, cuts=(), kind=jnp.bfloat16):
    level = levels(own_key, dims, cuts, -0.22, 0.18) if cuts else 1.0
    values = jax.random.normal(own_key, dims, jnp.float32) * scale * level
    return jnp.minimum(jnp.maximum(values, -limit), limit).astype(kind)


def setup_inputs(seed: int = 0, part: int = 0) -> dict:
    seeds = jax.random.split(jax.random.key(seed), 8)
    part_splits = jax.random.split(jax.random.fold_in(seeds[7], part), 8)
    tokens = scatter_about(part_splits[0], (TOKENS, D), 1.0, 6.0, ((0, 16),))
    expert_ids_keys = jax.random.split(jax.random.fold_in(part_splits[1], 1), TOKENS // TOK_DEV)
    expert_ids_turns = jax.random.permutation(jax.random.fold_in(part_splits[1], 3), TOKENS // TOK_DEV)
    expert_ids = jax.vmap(lambda own, number: assign_block(jax.random.fold_in(part_splits[1], 2), own, number, TOK_DEV, EXPERTS, TOPK, CAP, 2))(expert_ids_keys, expert_ids_turns).reshape((TOKENS, TOPK))
    gate_weights = jnp.clip(0.1 + 0.5 * jax.random.uniform(part_splits[2], (TOKENS, TOPK), jnp.float32) ** levels(part_splits[2], (TOKENS, TOPK), ((0, 16),), -0.2, 0.2), 0.1, 0.6)
    expert_in = scatter_about(part_splits[3], (EXPERTS, D, FF), D ** -0.5, 0.15625, ((0, 4), (1, 4)))
    expert_out = scatter_about(part_splits[4], (EXPERTS, FF, D), FF ** -0.5, 0.21875, ((0, 4), (2, 4)))
    shared_in = scatter_about(part_splits[5], (D, FF), D ** -0.5, 0.15625, ((0, 4),))
    shared_out = scatter_about(part_splits[6], (FF, D), FF ** -0.5, 0.21875, ((1, 4),))
    return dict(tokens=tokens, expert_ids=expert_ids, gate_weights=gate_weights, expert_in=expert_in, expert_out=expert_out, shared_in=shared_in, shared_out=shared_out)


def layer_norm(tokens):
    values = tokens.astype(jnp.float32)
    center = values - lax.optimization_barrier(jnp.mean(values, axis=-1, keepdims=True))
    spread = lax.optimization_barrier(jnp.mean(center * center, axis=-1, keepdims=True))
    return (center * lax.rsqrt(spread + 1e-06)).astype(jnp.bfloat16)

def reference(tokens, expert_ids, gate_weights, expert_in, expert_out, shared_in, shared_out):
    normed = layer_norm(tokens)
    token_count = tokens.shape[0]
    model_width = tokens.shape[1]
    expert_count = expert_in.shape[0]
    place_count = token_count // TOK_DEV * CAP
    expert_iota = jnp.arange(expert_count, dtype=jnp.int32)
    matches = (expert_ids[:, :, None] == expert_iota[None, None, :]).astype(jnp.int32)
    per_token = lax.optimization_barrier(jnp.sum(matches, axis=1, dtype=jnp.int32))
    earlier = jnp.cumsum(per_token, axis=0, dtype=jnp.int32) - per_token
    slot_of = jnp.take_along_axis(earlier, expert_ids, axis=1).astype(jnp.int32)
    anchors = jnp.broadcast_to(jnp.arange(token_count, dtype=jnp.int32)[:, None], expert_ids.shape)
    slot_table = jnp.full((expert_count, place_count), token_count, jnp.int32)
    slot_table = slot_table.at[expert_ids, slot_of].set(anchors)
    gate_table = jnp.zeros((expert_count, place_count), jnp.float32)
    gate_table = gate_table.at[expert_ids, slot_of].set(gate_weights.astype(jnp.float32))
    padded = jnp.concatenate([normed, jnp.zeros((1, model_width), jnp.bfloat16)], axis=0)

    def expert_step(summed, inputs):
        row_index, gate_rows, weight_in, weight_out = inputs
        gathered = padded[row_index]
        hidden = jax.nn.gelu(jnp.dot(gathered, weight_in, preferred_element_type=jnp.float32)).astype(jnp.bfloat16)
        result = jnp.dot(hidden, weight_out, preferred_element_type=jnp.float32).astype(jnp.bfloat16)
        summed = summed.at[row_index].add(result.astype(jnp.float32) * gate_rows[:, None])
        return (summed, None)
    start_sum = jnp.zeros((token_count + 1, model_width), jnp.float32)
    summed, _ = lax.scan(expert_step, start_sum, (slot_table, gate_table, expert_in, expert_out))
    routed = summed[:token_count]
    shared_hidden = jax.nn.gelu(jnp.dot(normed, shared_in, preferred_element_type=jnp.float32)).astype(jnp.bfloat16)
    shared_result = jnp.dot(shared_hidden, shared_out, preferred_element_type=jnp.float32)
    return (tokens.astype(jnp.float32) + shared_result + routed).astype(jnp.bfloat16)
```

```python
import functools

import jax
import jax.numpy as jnp
from jax import lax
from jax.experimental import pallas as pl
from jax.experimental.pallas import tpu as pltpu
from jax.sharding import PartitionSpec as P

CAP = 20
GROUP = 4


def layer_norm(tokens):
    values = tokens.astype(jnp.float32)
    center = values - jnp.mean(values, axis=-1, keepdims=True)
    spread = jnp.mean(center * center, axis=-1, keepdims=True)
    return (center * lax.rsqrt(spread + 1e-06)).astype(jnp.bfloat16)


def first_kernel(runs, run_tokens, x_ref, key_ref, w_ref, out_ref, rows_ref):
    slots = out_ref.shape[3]
    for j in range(runs):
        span = slice(j * run_tokens, (j + 1) * run_tokens)
        row = lax.broadcasted_iota(jnp.int32, (slots, run_tokens), 0)
        pick = jnp.where(row == key_ref[0, :, span], 1.0, 0.0).astype(jnp.bfloat16)
        rows_ref[j * slots : (j + 1) * slots, :] = jnp.dot(
            pick, x_ref[span, :], preferred_element_type=jnp.float32
        ).astype(jnp.bfloat16)
    pre = jnp.dot(rows_ref[...], w_ref[0], preferred_element_type=jnp.float32)
    for j in range(runs):
        out_ref[j, 0, 0] = pre[j * slots : (j + 1) * slots].astype(jnp.bfloat16)


def first_projection(x, keys, weight, first, count, runs, run_tokens, slots):
    width, hidden = weight.shape[1:]
    chunk = runs * run_tokens
    chunks = x.shape[0] // chunk
    total = count * chunks * runs * slots
    return pl.pallas_call(
        functools.partial(first_kernel, runs, run_tokens),
        grid=(count, chunks),
        in_specs=[
            pl.BlockSpec((chunk, width), lambda e, c: (c, 0)),
            pl.BlockSpec((1, 1, chunk), lambda e, c: (e + first, 0, c)),
            pl.BlockSpec((1, width, hidden), lambda e, c: (e + first, 0, 0)),
        ],
        out_specs=pl.BlockSpec((runs, 1, 1, slots, hidden), lambda e, c: (0, e, c, 0, 0)),
        out_shape=jax.ShapeDtypeStruct((runs, count, chunks, slots, hidden), jnp.bfloat16),
        scratch_shapes=[pltpu.VMEM((runs * slots, width), jnp.bfloat16)],
        cost_estimate=pl.CostEstimate(
            flops=2 * total * width * (hidden + run_tokens),
            bytes_accessed=2 * (count * width * hidden + total * hidden + x.size),
            transcendentals=0,
        ),
    )(x, keys, weight)


def second_kernel(runs, run_tokens, h_ref, key_ref, gate_ref, w_ref, *refs):
    carry_ref, (out_ref, total_ref) = refs[0] if len(refs) == 3 else None, refs[-2:]
    expert = pl.program_id(1)
    slots = h_ref.shape[3]

    @pl.when(expert == 0)
    def _():
        total_ref[...] = jnp.zeros_like(total_ref) if carry_ref is None else carry_ref[...]

    h = jnp.concatenate([h_ref[j, 0, 0] for j in range(runs)], axis=0)
    result = jnp.dot(h, w_ref[0], preferred_element_type=jnp.float32)
    for j in range(runs):
        span = slice(j * run_tokens, (j + 1) * run_tokens)
        row = lax.broadcasted_iota(jnp.int32, (slots, run_tokens), 0)
        match = row == key_ref[0, :, span]
        gate = jnp.sum(jnp.where(match, gate_ref[0, :, span], 0.0), axis=1, keepdims=True)
        scaled = (result[j * slots : (j + 1) * slots] * gate).astype(jnp.bfloat16)
        total_ref[span, :] += lax.dot_general(
            jnp.where(match, 1.0, 0.0).astype(jnp.bfloat16),
            scaled,
            (((0,), (0,)), ((), ())),
            preferred_element_type=jnp.float32,
        )

    @pl.when(expert == pl.num_programs(1) - 1)
    def _():
        out_ref[...] = total_ref[...].astype(out_ref.dtype)


def second_projection(hidden, keys, gates, weight, carry, kind, first, runs, run_tokens):
    _, count, chunks, slots, depth = hidden.shape
    width = weight.shape[2]
    chunk = runs * run_tokens
    total = count * chunks * runs * slots
    carries = [] if carry is None else [carry]
    return pl.pallas_call(
        functools.partial(second_kernel, runs, run_tokens),
        grid=(chunks, count),
        in_specs=[
            pl.BlockSpec((runs, 1, 1, slots, depth), lambda c, e: (0, e, c, 0, 0)),
            pl.BlockSpec((1, 1, chunk), lambda c, e: (e + first, 0, c)),
            pl.BlockSpec((1, 1, chunk), lambda c, e: (e + first, 0, c)),
            pl.BlockSpec((1, depth, width), lambda c, e: (e + first, 0, 0)),
        ]
        + [pl.BlockSpec((chunk, width), lambda c, e: (c, 0)) for _ in carries],
        out_specs=pl.BlockSpec((chunk, width), lambda c, e: (c, 0)),
        out_shape=jax.ShapeDtypeStruct((chunks * chunk, width), kind),
        scratch_shapes=[pltpu.VMEM((chunk, width), jnp.float32)],
        cost_estimate=pl.CostEstimate(
            flops=2 * total * width * (depth + 3 * run_tokens),
            bytes_accessed=2 * (count * depth * width + total * depth) + 4 * chunks * chunk * width,
            transcendentals=0,
        ),
    )(hidden, keys, gates, weight, *carries)


def per_device(tokens, expert_ids, gate_weights, expert_in, expert_out, shared_in, shared_out):
    row_count, model_width = tokens.shape
    pick_count = expert_ids.shape[1]
    local_count = expert_in.shape[0]
    runs = lax.axis_size("dp")
    block_count = runs * lax.axis_size("expert")
    run_tokens = GROUP * row_count
    slots = GROUP * CAP
    halves = 2 if local_count % 2 == 0 else 1

    normed = layer_norm(tokens)
    full_shared_in = lax.all_gather(shared_in, "dp", axis=0, tiled=True)
    full_shared_out = lax.all_gather(shared_out, "dp", axis=1, tiled=True)

    named = jnp.concatenate([expert_ids.astype(jnp.float32), gate_weights], axis=1).T
    named = lax.all_gather(named, ("expert", "dp"), axis=0, tiled=False)
    ids, gates = named[:, :pick_count], named[:, pick_count:]
    columns = lax.all_to_all(normed, "dp", split_axis=1, concat_axis=0, tiled=True)
    columns, full_shared_in, full_shared_out = lax.optimization_barrier(
        (columns, full_shared_in, full_shared_out)
    )
    x = lax.all_gather(columns, "expert", axis=0, tiled=True)

    owned = lax.axis_index("expert") * local_count + jnp.arange(local_count, dtype=jnp.int32)
    matches = ids[:, :, None, :] == owned.astype(jnp.float32)[:, None]
    chosen = jnp.any(matches, axis=1)
    gate_of = jnp.sum(jnp.where(matches, gates[:, :, None, :], 0.0), axis=1)
    order = jnp.arange(row_count, dtype=jnp.int32)
    before = (order[:, None] < order[None, :]).astype(jnp.bfloat16)
    earlier = jnp.einsum(
        "bej,ji->bei", chosen.astype(jnp.bfloat16), before, preferred_element_type=jnp.float32
    ).astype(jnp.int32)
    base = jnp.arange(block_count, dtype=jnp.int32) % GROUP * CAP
    keys = jnp.where(chosen, earlier + base[:, None, None], -1)

    def by_expert(table):
        return table.transpose(1, 0, 2).reshape(local_count, 1, block_count * row_count)

    keys, gate_of = by_expert(keys), by_expert(gate_of)

    count = local_count // halves
    parts = []
    for half in range(halves):
        pre = first_projection(
            x, keys, expert_in, half * count, count, runs, run_tokens, slots
        )
        parts.append(lax.psum_scatter(pre, "dp", scatter_dimension=0, tiled=True))

    hidden = []
    for pre in parts:
        act = jax.nn.gelu(pre.astype(jnp.float32)).astype(jnp.bfloat16)
        hidden.append(lax.all_gather(act, "dp", axis=0, tiled=True))

    shared_pre = jnp.dot(normed, full_shared_in, preferred_element_type=jnp.float32)
    shared_hidden = jax.nn.gelu(shared_pre).astype(jnp.bfloat16)
    shared_result = jnp.dot(shared_hidden, full_shared_out, preferred_element_type=jnp.float32)

    routed = None
    for half, h in enumerate(hidden):
        kind = jnp.bfloat16 if half == halves - 1 else jnp.float32
        routed = second_projection(
            h, keys, gate_of, expert_out, routed, kind, half * count, runs, run_tokens
        )
    width = routed.shape[1]
    pieces = lax.all_to_all(
        routed.reshape(block_count, row_count, width),
        ("expert", "dp"),
        split_axis=0,
        concat_axis=0,
        tiled=True,
    ).reshape(-1, runs, row_count, width)
    own = jnp.sum(pieces.astype(jnp.float32), axis=0).transpose(1, 0, 2)
    own = own.reshape(row_count, model_width)
    return (tokens.astype(jnp.float32) + shared_result + own).astype(jnp.bfloat16)


def start_of(index, size):
    return pl.ds(pl.multiple_of(index * size, size), size)


def fused_kernel(
    sizes,
    tok_ref,
    named_ref,
    win_hbm,
    wout_hbm,
    sin_hbm,
    sout_hbm,
    out_ref,
    norm,
    xall,
    meta,
    win,
    wout,
    sin,
    sout,
    keys,
    gates,
    pick,
    gslot,
    rows,
    send,
    recv,
    ssend,
    srecv,
    shared,
    scaled,
    own,
    psend,
    precv,
    zsend,
    zrecv,
    fsend,
    frecv,
    lsem,
    wssem,
    wrsem,
    xsem,
    zssem,
    zrsem,
    rssem,
    rrsem,
    mssem,
    mrsem,
    pssem,
    prsem,
    ssem,
    srsem,
    dssem,
    drsem,
    ossem,
    orsem,
):
    planes, chips, cores = sizes
    dp = chips * cores
    n = planes * dp
    tok_rows, width = tok_ref.shape
    picks = named_ref.shape[0] // 2
    half = width // chips
    part = half // cores
    experts = win.shape[0]
    local = experts * cores
    slots = pick.shape[2]
    span = pick.shape[3]
    own_rows = chips * tok_rows

    z = lax.axis_index("expert")
    d = lax.axis_index("dp")
    c = d % cores
    x = d // cores
    oc = 1 - c
    ox = 1 - x
    partner = {"dp": x * cores + oc}
    across = {"dp": ox * cores + c}
    s = c * chips + x

    def remote(src, dst, s_sem, r_sem, device):
        return pltpu.make_async_remote_copy(
            src_ref=src,
            dst_ref=dst,
            send_sem=s_sem,
            recv_sem=r_sem,
            device_id=device,
            device_id_type=pl.DeviceIdType.MESH,
        )

    def loop(first, last, body):
        def step(i, carry):
            body(i)
            return carry

        lax.fori_loop(first, last, step, 0)

    def place(r):
        spot = lax.rem(z * dp + d + r, n)
        return {"expert": spot // dp, "dp": lax.rem(spot, dp)}

    def local_in(e):
        return pltpu.make_async_copy(
            win_hbm.at[c * experts + e], win.at[e, start_of(c, part)], lsem.at[e]
        )

    def local_out(e):
        return pltpu.make_async_copy(
            wout_hbm.at[c * experts + e],
            wout.at[e, :, start_of(c, part)],
            lsem.at[experts + e],
        )

    def local_shared_in():
        return pltpu.make_async_copy(sin_hbm, sin.at[start_of(c, part)], lsem.at[2 * experts])

    def local_shared_out():
        return pltpu.make_async_copy(
            sout_hbm, sout.at[:, start_of(c, part)], lsem.at[2 * experts + 1]
        )

    def partner_in(e):
        return remote(
            win_hbm.at[oc * experts + e],
            win.at[e, start_of(c, part)],
            wssem.at[e],
            wrsem.at[e],
            partner,
        )

    def partner_out(e):
        return remote(
            wout_hbm.at[oc * experts + e],
            wout.at[e, :, start_of(c, part)],
            wssem.at[experts + e],
            wrsem.at[experts + e],
            partner,
        )

    def partner_shared_in():
        return remote(
            sin_hbm,
            sin.at[start_of(c, part)],
            wssem.at[2 * experts],
            wrsem.at[2 * experts],
            partner,
        )

    def partner_shared_out():
        return remote(
            sout_hbm,
            sout.at[:, start_of(c, part)],
            wssem.at[2 * experts + 1],
            wrsem.at[2 * experts + 1],
            partner,
        )

    def token_swap():
        return remote(
            norm.at[:, start_of(ox, half)], xall.at[z, c, x], xsem.at[0], xsem.at[1], across
        )

    def to_plane(i, b):
        return remote(
            xall.at[z, c, b],
            xall.at[z, c, b],
            zssem.at[i - 1, b],
            zrsem.at[i - 1, b],
            {"expert": lax.rem(z - i + planes, planes)},
        )

    def relay(i, b):
        p = lax.rem(z + i, planes)
        return remote(
            xall.at[p, c, b], xall.at[p, c, b], rssem.at[i, b], rrsem.at[i, b], partner
        )

    def tell(r):
        return remote(named_ref, meta.at[z, s], mssem.at[r], mrsem.at[r], place(r))

    def swap(k, e):
        return remote(send.at[k, e], recv.at[k, e], pssem.at[k, e], prsem.at[k, e], across)

    def shared_swap(b):
        return remote(ssend.at[b], srecv.at[b], ssem.at[b], srsem.at[b], across)

    def pair(k):
        return remote(psend.at[k], precv.at[k], dssem.at[k], drsem.at[k], partner)

    def give(k):
        return remote(
            zsend.at[k],
            zrecv.at[k],
            ossem.at[k],
            orsem.at[k],
            {"expert": lax.rem(z + k + 1, planes)},
        )

    def finish():
        return remote(fsend, frecv, xsem.at[2], xsem.at[3], across)

    barrier = pltpu.get_barrier_semaphore()
    loop(
        1,
        n,
        lambda r: pl.semaphore_signal(
            barrier, inc=1, device_id=place(r), device_id_type=pl.DeviceIdType.MESH
        ),
    )
    local_shared_in().start()
    loop(0, experts, lambda e: local_in(e).start())
    local_shared_out().start()
    loop(0, experts, lambda e: local_out(e).start())

    values = tok_ref[...].astype(jnp.float32)
    center = values - jnp.mean(values, axis=-1, keepdims=True)
    spread = jnp.mean(center * center, axis=-1, keepdims=True)
    norm[...] = (center * lax.rsqrt(spread + 1e-06)).astype(jnp.bfloat16)
    xall[z, c, x] = norm[:, start_of(x, half)]
    meta[z, s] = named_ref[...]

    pl.semaphore_wait(barrier, n - 1)
    token_swap().start()
    relay(0, x).start()
    loop(1, planes, lambda i: to_plane(i, x).start())
    partner_shared_in().start()
    loop(1, n, lambda r: tell(r).start())
    loop(0, experts, lambda e: partner_in(e).start())
    partner_shared_out().start()
    loop(0, experts, lambda e: partner_out(e).start())

    def shared_first(b):
        pre = jnp.dot(xall[z, c, b], sin[...], preferred_element_type=jnp.float32)
        ssend[b] = pre.astype(jnp.bfloat16)
        shared_swap(b).start()

    local_shared_in().wait()
    partner_shared_in().wait_recv()
    shared_first(x)
    token_swap().wait_recv()
    relay(0, ox).start()
    loop(1, planes, lambda i: to_plane(i, ox).start())
    shared_first(ox)
    loop(1, n, lambda r: tell(r).wait_recv())

    before = jnp.where(
        lax.broadcasted_iota(jnp.int32, (tok_rows, tok_rows), 0)
        < lax.broadcasted_iota(jnp.int32, (tok_rows, tok_rows), 1),
        1.0,
        0.0,
    ).astype(jnp.bfloat16)

    def first_stage(k, weights_wait):
        i = lax.rem(k + 1, planes)
        p = lax.rem(z + i, planes)
        turn = lax.rem(k, 2)

        ids = jnp.concatenate([meta[p, b, :picks] for b in range(dp)], axis=1)
        weights = jnp.concatenate([meta[p, b, picks:] for b in range(dp)], axis=1)
        chosen, gate = [], []
        for e in range(experts):
            match = ids == (z * local + c * experts + e).astype(jnp.float32)
            chosen.append(jnp.max(jnp.where(match, 1.0, 0.0), axis=0, keepdims=True))
            gate.append(jnp.sum(jnp.where(match, weights, 0.0), axis=0, keepdims=True))
        chosen = jnp.concatenate(chosen, axis=0)
        gates[...] = jnp.concatenate(gate, axis=0)
        for b in range(dp):
            lanes = slice(b * tok_rows, (b + 1) * tok_rows)
            mine = chosen[:, lanes]
            earlier = jnp.dot(
                mine.astype(jnp.bfloat16), before, preferred_element_type=jnp.float32
            )
            keys[:, lanes] = jnp.where(mine > 0.5, earlier + float(b * CAP), -1.0).astype(
                jnp.int32
            )

        def choose(e):
            row = lax.broadcasted_iota(jnp.int32, (slots, span), 0)
            match = row == keys[pl.ds(e, 1), :]
            pick[turn, e] = jnp.where(match, 1.0, 0.0).astype(jnp.bfloat16)
            gate = jnp.sum(
                jnp.where(match, gates[pl.ds(e, 1), :], 0.0), axis=1, keepdims=True
            )
            gslot[turn, e] = jnp.broadcast_to(gate, gslot.shape[2:])

        loop(0, experts, choose)

        @pl.when(i > 0)
        def _():
            for b in range(chips):
                to_plane(lax.max(i, 1), b).wait_recv()
                relay(i, b).start()

        for b in range(chips):
            relay(i, b).wait_recv()
        plane = xall[p].reshape(span, half)
        chosen_rows = jnp.dot(
            pick[turn].reshape(experts * slots, span), plane, preferred_element_type=jnp.float32
        )
        rows[...] = chosen_rows.astype(jnp.bfloat16).reshape(rows.shape)

        def project(e):
            if weights_wait:
                local_in(e).wait()
                partner_in(e).wait_recv()
            pre = jnp.dot(rows[e], win[e], preferred_element_type=jnp.float32)
            send[k, e] = pre.astype(jnp.bfloat16)
            swap(k, e).start()

        loop(0, experts, project)

    def second_stage(k):
        turn = lax.rem(k, 2)

        def project(e):
            swap(k, e).wait_recv()
            total = send[k, e].astype(jnp.float32) + recv[k, e].astype(jnp.float32)
            h = jax.nn.gelu(total).astype(jnp.bfloat16)
            result = jnp.dot(h, wout[e], preferred_element_type=jnp.float32)
            scaled[e] = (result * gslot[turn, e][:, :1]).astype(jnp.bfloat16)

        loop(0, experts, project)

        def combine(core):
            lanes = start_of(core, own_rows)
            return lax.dot_general(
                pick[turn, :, :, lanes].reshape(experts * slots, own_rows),
                scaled[...].reshape(experts * slots, half),
                (((0,), (0,)), ((), ())),
                preferred_element_type=jnp.float32,
            )

        psend[k] = combine(oc).astype(jnp.bfloat16)
        pair(k).start()
        own[...] = combine(c)
        pair(k).wait_recv()
        own[...] += precv[k].astype(jnp.float32)

    def shared_second():
        local_shared_out().wait()
        partner_shared_out().wait_recv()
        for b in range(chips):
            shared_swap(b).wait_recv()
        total = ssend[...].astype(jnp.float32) + srecv[...].astype(jnp.float32)
        h = jax.nn.gelu(total).astype(jnp.bfloat16).reshape(own_rows, -1)
        shared[...] = jnp.dot(h, sout[...], preferred_element_type=jnp.float32)

    first_stage(0, True)
    shared_second()
    for e in range(experts):
        local_out(e).wait()
        partner_out(e).wait_recv()

    def plane_step(k):
        first_stage(k + 1, False)
        second_stage(k)
        zsend[k] = own[...].astype(jnp.bfloat16)
        give(k).start()

    loop(0, planes - 1, plane_step)
    second_stage(planes - 1)
    total = own[...] + shared[...]
    for k in range(planes - 1):
        give(k).wait_recv()
        total = total + zrecv[k].astype(jnp.float32)
    own[...] = total
    fsend[...] = own[start_of(ox, tok_rows), :].astype(jnp.bfloat16)
    finish().start()
    mine = start_of(x, half)
    theirs = start_of(ox, half)
    out_ref[:, mine] = (
        tok_ref[:, mine].astype(jnp.float32) + own[start_of(x, tok_rows), :]
    ).astype(out_ref.dtype)
    finish().wait_recv()
    out_ref[:, theirs] = (
        tok_ref[:, theirs].astype(jnp.float32) + frecv[...].astype(jnp.float32)
    ).astype(out_ref.dtype)

    token_swap().wait_send()
    partner_shared_in().wait_send()
    partner_shared_out().wait_send()
    finish().wait_send()
    loop(1, n, lambda r: tell(r).wait_send())

    def weights_sent(e):
        partner_in(e).wait_send()
        partner_out(e).wait_send()

    loop(0, experts, weights_sent)
    for b in range(chips):
        shared_swap(b).wait_send()

        def sent(i):
            relay(i, b).wait_send()

        loop(0, planes, sent)
        loop(1, planes, lambda i: to_plane(i, b).wait_send())

    def plane_sent(k):
        loop(0, experts, lambda e: swap(k, e).wait_send())
        pair(k).wait_send()

    loop(0, planes, plane_sent)
    loop(0, planes - 1, lambda k: give(k).wait_send())


def fused(tokens, expert_ids, gate_weights, expert_in, expert_out, shared_in, shared_out):
    tok_rows, width = tokens.shape
    picks = expert_ids.shape[1]
    planes, dp = lax.axis_size("expert"), lax.axis_size("dp")
    cores, chips = 2, dp // 2
    local, part, hidden = expert_in.shape
    experts = local // cores
    half = width // chips
    slots, span = dp * CAP, dp * tok_rows
    own_rows = chips * tok_rows
    named = jnp.concatenate([expert_ids.astype(jnp.float32), gate_weights], axis=1).T
    bf16, f32 = jnp.bfloat16, jnp.float32
    vmem, dma = pltpu.VMEM, pltpu.SemaphoreType.DMA
    scratch = [
        vmem((tok_rows, width), bf16),
        vmem((planes, cores, chips, tok_rows, half), bf16),
        vmem((planes, dp, 2 * picks, tok_rows), f32),
        vmem((experts, half, hidden), bf16),
        vmem((experts, hidden, half), bf16),
        vmem((half, hidden), bf16),
        vmem((hidden, half), bf16),
        vmem((experts, span), jnp.int32),
        vmem((experts, span), f32),
        vmem((2, experts, slots, span), bf16),
        vmem((2, experts, slots, 128), f32),
        vmem((experts, slots, half), bf16),
        vmem((planes, experts, slots, hidden), bf16),
        vmem((planes, experts, slots, hidden), bf16),
        vmem((chips, tok_rows, hidden), bf16),
        vmem((chips, tok_rows, hidden), bf16),
        vmem((own_rows, half), f32),
        vmem((experts, slots, half), bf16),
        vmem((own_rows, half), f32),
        vmem((planes, own_rows, half), bf16),
        vmem((planes, own_rows, half), bf16),
        vmem((planes - 1, own_rows, half), bf16),
        vmem((planes - 1, own_rows, half), bf16),
        vmem((tok_rows, half), bf16),
        vmem((tok_rows, half), bf16),
        dma((2 * experts + 2,)),
        dma((2 * experts + 2,)),
        dma((2 * experts + 2,)),
        dma((4,)),
        dma((planes - 1, chips)),
        dma((planes - 1, chips)),
        dma((planes, chips)),
        dma((planes, chips)),
        dma((planes * dp,)),
        dma((planes * dp,)),
        dma((planes, experts)),
        dma((planes, experts)),
        dma((chips,)),
        dma((chips,)),
        dma((planes,)),
        dma((planes,)),
        dma((planes - 1,)),
        dma((planes - 1,)),
    ]
    whole = pl.BlockSpec(memory_space=pltpu.VMEM)
    apart = pl.BlockSpec(memory_space=pl.ANY)
    return pl.pallas_call(
        functools.partial(fused_kernel, (planes, chips, cores)),
        in_specs=[whole, whole, apart, apart, apart, apart],
        out_specs=whole,
        out_shape=jax.ShapeDtypeStruct((tok_rows, width), tokens.dtype),
        scratch_shapes=scratch,
        compiler_params=pltpu.CompilerParams(
            collective_id=0, has_side_effects=True, vmem_limit_bytes=63 * 1024 * 1024
        ),
    )(tokens, named, expert_in, expert_out, shared_in, shared_out)


def fits(mesh, args):
    planes, dp = mesh.shape["expert"], mesh.shape["dp"]
    tokens, expert_in = args[0], args[3]
    return (
        dp == 4
        and 1 < planes <= 8
        and expert_in.shape[0] // (mesh.shape["sweep"] * planes) % 2 == 0
        and expert_in.shape[0] // (mesh.shape["sweep"] * planes) <= 16
        and tokens.shape[0] // (mesh.shape["sweep"] * planes * dp) == 128
    )


def solution(mesh):
    placed = (
        P(("sweep", "expert", "dp"), None),
        P(("sweep", "expert", "dp"), None),
        P(("sweep", "expert", "dp"), None),
        P(("sweep", "expert"), "dp", None),
        P(("sweep", "expert"), None, "dp"),
        P(("sweep", "dp"), None),
        P("sweep", "dp"),
    )

    def run(*args):
        return jax.shard_map(
            fused if fits(mesh, args) else per_device,
            mesh=mesh,
            in_specs=placed,
            out_specs=P(("sweep", "expert", "dp"), None),
            check_vma=False,
        )(*args)

    return run
```

```python
import functools

import jax
import jax.numpy as jnp
from jax import lax
from jax.experimental import pallas as pl
from jax.experimental.pallas import tpu as pltpu
from jax.sharding import PartitionSpec as P

CAP = 20
GROUP = 4


def layer_norm(tokens):
    values = tokens.astype(jnp.float32)
    center = values - jnp.mean(values, axis=-1, keepdims=True)
    spread = jnp.mean(center * center, axis=-1, keepdims=True)
    return (center * lax.rsqrt(spread + 1e-06)).astype(jnp.bfloat16)


def first_kernel(runs, run_tokens, x_ref, key_ref, w_ref, out_ref, rows_ref):
    slots = out_ref.shape[3]
    for j in range(runs):
        span = slice(j * run_tokens, (j + 1) * run_tokens)
        row = lax.broadcasted_iota(jnp.int32, (slots, run_tokens), 0)
        pick = jnp.where(row == key_ref[0, :, span], 1.0, 0.0).astype(jnp.bfloat16)
        rows_ref[j * slots : (j + 1) * slots, :] = jnp.dot(
            pick, x_ref[span, :], preferred_element_type=jnp.float32
        ).astype(jnp.bfloat16)
    pre = jnp.dot(rows_ref[...], w_ref[0], preferred_element_type=jnp.float32)
    for j in range(runs):
        out_ref[j, 0, 0] = pre[j * slots : (j + 1) * slots].astype(jnp.bfloat16)


def first_projection(x, keys, weight, first, count, runs, run_tokens, slots):
    width, hidden = weight.shape[1:]
    chunk = runs * run_tokens
    chunks = x.shape[0] // chunk
    total = count * chunks * runs * slots
    return pl.pallas_call(
        functools.partial(first_kernel, runs, run_tokens),
        grid=(count, chunks),
        in_specs=[
            pl.BlockSpec((chunk, width), lambda e, c: (c, 0)),
            pl.BlockSpec((1, 1, chunk), lambda e, c: (e + first, 0, c)),
            pl.BlockSpec((1, width, hidden), lambda e, c: (e + first, 0, 0)),
        ],
        out_specs=pl.BlockSpec((runs, 1, 1, slots, hidden), lambda e, c: (0, e, c, 0, 0)),
        out_shape=jax.ShapeDtypeStruct((runs, count, chunks, slots, hidden), jnp.bfloat16),
        scratch_shapes=[pltpu.VMEM((runs * slots, width), jnp.bfloat16)],
        cost_estimate=pl.CostEstimate(
            flops=2 * total * width * (hidden + run_tokens),
            bytes_accessed=2 * (count * width * hidden + total * hidden + x.size),
            transcendentals=0,
        ),
    )(x, keys, weight)


def second_kernel(runs, run_tokens, h_ref, key_ref, gate_ref, w_ref, *refs):
    carry_ref, (out_ref, total_ref) = refs[0] if len(refs) == 3 else None, refs[-2:]
    expert = pl.program_id(1)
    slots = h_ref.shape[3]

    @pl.when(expert == 0)
    def _():
        total_ref[...] = jnp.zeros_like(total_ref) if carry_ref is None else carry_ref[...]

    h = jnp.concatenate([h_ref[j, 0, 0] for j in range(runs)], axis=0)
    result = jnp.dot(h, w_ref[0], preferred_element_type=jnp.float32)
    for j in range(runs):
        span = slice(j * run_tokens, (j + 1) * run_tokens)
        row = lax.broadcasted_iota(jnp.int32, (slots, run_tokens), 0)
        match = row == key_ref[0, :, span]
        gate = jnp.sum(jnp.where(match, gate_ref[0, :, span], 0.0), axis=1, keepdims=True)
        scaled = (result[j * slots : (j + 1) * slots] * gate).astype(jnp.bfloat16)
        total_ref[span, :] += lax.dot_general(
            jnp.where(match, 1.0, 0.0).astype(jnp.bfloat16),
            scaled,
            (((0,), (0,)), ((), ())),
            preferred_element_type=jnp.float32,
        )

    @pl.when(expert == pl.num_programs(1) - 1)
    def _():
        out_ref[...] = total_ref[...].astype(out_ref.dtype)


def second_projection(hidden, keys, gates, weight, carry, kind, first, runs, run_tokens):
    _, count, chunks, slots, depth = hidden.shape
    width = weight.shape[2]
    chunk = runs * run_tokens
    total = count * chunks * runs * slots
    carries = [] if carry is None else [carry]
    return pl.pallas_call(
        functools.partial(second_kernel, runs, run_tokens),
        grid=(chunks, count),
        in_specs=[
            pl.BlockSpec((runs, 1, 1, slots, depth), lambda c, e: (0, e, c, 0, 0)),
            pl.BlockSpec((1, 1, chunk), lambda c, e: (e + first, 0, c)),
            pl.BlockSpec((1, 1, chunk), lambda c, e: (e + first, 0, c)),
            pl.BlockSpec((1, depth, width), lambda c, e: (e + first, 0, 0)),
        ]
        + [pl.BlockSpec((chunk, width), lambda c, e: (c, 0)) for _ in carries],
        out_specs=pl.BlockSpec((chunk, width), lambda c, e: (c, 0)),
        out_shape=jax.ShapeDtypeStruct((chunks * chunk, width), kind),
        scratch_shapes=[pltpu.VMEM((chunk, width), jnp.float32)],
        cost_estimate=pl.CostEstimate(
            flops=2 * total * width * (depth + 3 * run_tokens),
            bytes_accessed=2 * (count * depth * width + total * depth) + 4 * chunks * chunk * width,
            transcendentals=0,
        ),
    )(hidden, keys, gates, weight, *carries)


def per_device(tokens, expert_ids, gate_weights, expert_in, expert_out, shared_in, shared_out):
    row_count, model_width = tokens.shape
    pick_count = expert_ids.shape[1]
    local_count = expert_in.shape[0]
    runs = lax.axis_size("dp")
    block_count = runs * lax.axis_size("expert")
    run_tokens = GROUP * row_count
    slots = GROUP * CAP
    halves = 2 if local_count % 2 == 0 else 1

    normed = layer_norm(tokens)
    full_shared_in = lax.all_gather(shared_in, "dp", axis=0, tiled=True)
    full_shared_out = lax.all_gather(shared_out, "dp", axis=1, tiled=True)

    named = jnp.concatenate([expert_ids.astype(jnp.float32), gate_weights], axis=1).T
    named = lax.all_gather(named, ("expert", "dp"), axis=0, tiled=False)
    ids, gates = named[:, :pick_count], named[:, pick_count:]
    columns = lax.all_to_all(normed, "dp", split_axis=1, concat_axis=0, tiled=True)
    columns, full_shared_in, full_shared_out = lax.optimization_barrier(
        (columns, full_shared_in, full_shared_out)
    )
    x = lax.all_gather(columns, "expert", axis=0, tiled=True)

    owned = lax.axis_index("expert") * local_count + jnp.arange(local_count, dtype=jnp.int32)
    matches = ids[:, :, None, :] == owned.astype(jnp.float32)[:, None]
    chosen = jnp.any(matches, axis=1)
    gate_of = jnp.sum(jnp.where(matches, gates[:, :, None, :], 0.0), axis=1)
    order = jnp.arange(row_count, dtype=jnp.int32)
    before = (order[:, None] < order[None, :]).astype(jnp.bfloat16)
    earlier = jnp.einsum(
        "bej,ji->bei", chosen.astype(jnp.bfloat16), before, preferred_element_type=jnp.float32
    ).astype(jnp.int32)
    base = jnp.arange(block_count, dtype=jnp.int32) % GROUP * CAP
    keys = jnp.where(chosen, earlier + base[:, None, None], -1)

    def by_expert(table):
        return table.transpose(1, 0, 2).reshape(local_count, 1, block_count * row_count)

    keys, gate_of = by_expert(keys), by_expert(gate_of)

    count = local_count // halves
    parts = []
    for half in range(halves):
        pre = first_projection(
            x, keys, expert_in, half * count, count, runs, run_tokens, slots
        )
        parts.append(lax.psum_scatter(pre, "dp", scatter_dimension=0, tiled=True))

    hidden = []
    for pre in parts:
        act = jax.nn.gelu(pre.astype(jnp.float32)).astype(jnp.bfloat16)
        hidden.append(lax.all_gather(act, "dp", axis=0, tiled=True))

    shared_pre = jnp.dot(normed, full_shared_in, preferred_element_type=jnp.float32)
    shared_hidden = jax.nn.gelu(shared_pre).astype(jnp.bfloat16)
    shared_result = jnp.dot(shared_hidden, full_shared_out, preferred_element_type=jnp.float32)

    routed = None
    for half, h in enumerate(hidden):
        kind = jnp.bfloat16 if half == halves - 1 else jnp.float32
        routed = second_projection(
            h, keys, gate_of, expert_out, routed, kind, half * count, runs, run_tokens
        )
    width = routed.shape[1]
    pieces = lax.all_to_all(
        routed.reshape(block_count, row_count, width),
        ("expert", "dp"),
        split_axis=0,
        concat_axis=0,
        tiled=True,
    ).reshape(-1, runs, row_count, width)
    own = jnp.sum(pieces.astype(jnp.float32), axis=0).transpose(1, 0, 2)
    own = own.reshape(row_count, model_width)
    return (tokens.astype(jnp.float32) + shared_result + own).astype(jnp.bfloat16)


def start_of(index, size):
    return pl.ds(pl.multiple_of(index * size, size), size)


HEAD = 4


def fused_kernel(
    sizes,
    tok_hbm,
    ids_hbm,
    gate_hbm,
    win_hbm,
    wout_hbm,
    sin_hbm,
    sout_hbm,
    out_ref,
    tok,
    ids_in,
    gate_in,
    norm,
    xall,
    meta,
    win,
    wout,
    sin,
    sout,
    keys,
    gates,
    pick,
    gslot,
    rows,
    send,
    recv,
    ssend,
    srecv,
    shared,
    scaled,
    own,
    other,
    psend,
    precv,
    osend,
    orecv,
    zsend,
    zrecv,
    fsend,
    frecv,
    isem,
    lsem,
    wssem,
    wrsem,
    xssem,
    xrsem,
    zssem,
    zrsem,
    rssem,
    rrsem,
    pssem,
    prsem,
    ssem,
    srsem,
    dssem,
    drsem,
    bssem,
    brsem,
    ossem,
    orsem,
    fssem,
    frsem,
):
    planes, chips, cores = sizes
    dp = chips * cores
    tok_rows, width = tok.shape
    picks = ids_in.shape[0]
    half = width // chips
    part = half // cores
    experts = win.shape[0]
    local = experts * cores
    slots, span = pick.shape[2:]
    own_rows = chips * tok_rows
    last = planes - 1
    head = min(HEAD, experts)

    z = lax.axis_index("expert")
    d = lax.axis_index("dp")
    c = d % cores
    x = d // cores
    oc = 1 - c
    ox = 1 - x
    partner = {"dp": x * cores + oc}
    across = {"dp": ox * cores + c}
    mesh_ids = pl.DeviceIdType.MESH

    def remote(src, dst, s_sem, r_sem, device):
        return pltpu.make_async_remote_copy(
            src_ref=src,
            dst_ref=dst,
            send_sem=s_sem,
            recv_sem=r_sem,
            device_id=device,
            device_id_type=mesh_ids,
        )

    def loop(first, end, body):
        def step(i, carry):
            body(i)
            return carry

        lax.fori_loop(first, end, step, 0)

    def plane_at(i):
        return {"expert": lax.rem(z + i, planes)}

    def local_in(e):
        return pltpu.make_async_copy(
            win_hbm.at[c * experts + e], win.at[e, start_of(c, part)], lsem.at[e]
        )

    def local_out(e):
        return pltpu.make_async_copy(
            wout_hbm.at[c * experts + e],
            wout.at[e, :, start_of(c, part)],
            lsem.at[experts + e],
        )

    def local_shared_in():
        return pltpu.make_async_copy(sin_hbm, sin.at[start_of(c, part)], lsem.at[2 * experts])

    def local_shared_out():
        return pltpu.make_async_copy(
            sout_hbm, sout.at[:, start_of(c, part)], lsem.at[2 * experts + 1]
        )

    def partner_in(e):
        return remote(
            win_hbm.at[oc * experts + e],
            win.at[e, start_of(c, part)],
            wssem.at[e],
            wrsem.at[e],
            partner,
        )

    def partner_out(e):
        return remote(
            wout_hbm.at[oc * experts + e],
            wout.at[e, :, start_of(c, part)],
            wssem.at[experts + e],
            wrsem.at[experts + e],
            partner,
        )

    def partner_shared_in():
        return remote(
            sin_hbm,
            sin.at[start_of(c, part)],
            wssem.at[2 * experts],
            wrsem.at[2 * experts],
            partner,
        )

    def partner_shared_out():
        return remote(
            sout_hbm,
            sout.at[:, start_of(c, part)],
            wssem.at[2 * experts + 1],
            wrsem.at[2 * experts + 1],
            partner,
        )

    def block(p, b, kind):
        return meta.at[p, c * chips + b] if kind else xall.at[p, c, b]

    def token_swap(kind):
        src = meta.at[z, c * chips + x] if kind else norm.at[:, start_of(ox, half)]
        return remote(src, block(z, x, kind), xssem.at[kind], xrsem.at[kind], across)

    def to_plane(i, b, kind):
        ref = block(z, b, kind)
        return remote(
            ref, ref, zssem.at[i - 1, b, kind], zrsem.at[i - 1, b, kind], plane_at(planes - i)
        )

    def relay(i, b, kind):
        ref = block(lax.rem(z + i, planes), b, kind)
        return remote(ref, ref, rssem.at[i, b, kind], rrsem.at[i, b, kind], partner)

    def swap(k, e):
        return remote(send.at[k, e], recv.at[k, e], pssem.at[k, e], prsem.at[k, e], across)

    def shared_swap(b):
        return remote(ssend.at[b], srecv.at[b], ssem.at[b], srsem.at[b], across)

    def pair(k):
        return remote(psend.at[k], precv.at[k], dssem.at[k], drsem.at[k], partner)

    def own_pair(b):
        return remote(osend.at[b], orecv.at[b], bssem.at[b], brsem.at[b], partner)

    def give(k):
        return remote(zsend.at[k], zrecv.at[k], ossem.at[k], orsem.at[k], plane_at(k + 1))

    def finish():
        return remote(fsend, frecv, fssem.at[0], frsem.at[0], across)

    barrier = pltpu.get_barrier_semaphore()
    for device in [across, partner] + [plane_at(i) for i in range(1, planes)]:
        pl.semaphore_signal(barrier, inc=1, device_id=device, device_id_type=mesh_ids)
    read_tok = pltpu.make_async_copy(tok_hbm, tok, isem.at[0])
    read_ids = pltpu.make_async_copy(ids_hbm, ids_in, isem.at[1])
    read_gate = pltpu.make_async_copy(gate_hbm, gate_in, isem.at[2])
    read_tok.start()
    read_ids.start()
    read_gate.start()
    local_shared_in().start()
    loop(0, experts, lambda e: local_in(e).start())
    local_shared_out().start()
    loop(0, experts, lambda e: local_out(e).start())
    read_ids.wait()
    read_gate.wait()
    meta[z, c * chips + x, :picks] = ids_in[...].astype(jnp.float32)
    meta[z, c * chips + x, picks:] = gate_in[...]
    read_tok.wait()
    values = tok[...].astype(jnp.float32)
    center = values - jnp.mean(values, axis=-1, keepdims=True)
    spread = jnp.mean(center * center, axis=-1, keepdims=True)
    norm[...] = (center * lax.rsqrt(spread + 1e-06)).astype(jnp.bfloat16)
    xall[z, c, x] = norm[:, start_of(x, half)]

    pl.semaphore_wait(barrier, planes + 1)
    early = min(3, experts)
    for kind in (1, 0):
        token_swap(kind).start()
    for kind in (1, 0):
        relay(0, x, kind).start()
    for kind in (1, 0):
        to_plane(1, x, kind).start()
    partner_shared_in().start()
    loop(0, early, lambda e: partner_in(e).start())

    def shared_first(b):
        pre = jnp.dot(xall[z, c, b], sin[...], preferred_element_type=jnp.float32)
        ssend[b] = pre.astype(jnp.bfloat16)
        shared_swap(b).start()

    local_shared_in().wait()
    partner_shared_in().wait_recv()
    shared_first(x)
    for kind in (1, 0):
        token_swap(kind).wait_recv()
        relay(0, ox, kind).start()
        to_plane(1, ox, kind).start()

    def to_others(i):
        for kind in (1, 0):
            to_plane(i, x, kind).start()
        for kind in (1, 0):
            to_plane(i, ox, kind).start()

    loop(2, planes, to_others)
    loop(early, experts, lambda e: partner_in(e).start())
    partner_shared_out().start()
    loop(0, experts, lambda e: partner_out(e).start())
    shared_first(ox)

    before = jnp.where(
        lax.broadcasted_iota(jnp.int32, (tok_rows, tok_rows), 0)
        < lax.broadcasted_iota(jnp.int32, (tok_rows, tok_rows), 1),
        1.0,
        0.0,
    ).astype(jnp.bfloat16)

    def first_stage(k, turn, mine):
        i = lax.rem(k + 1, planes)
        p = lax.rem(z + i, planes)
        if not mine:
            for kind in (1, 0):
                for b in range(chips):
                    to_plane(i, b, kind).wait_recv()
                    relay(i, b, kind).start()
        for b in range(chips):
            relay(i, b, 1).wait_recv()

        ids = jnp.concatenate([meta[p, b, :picks] for b in range(dp)], axis=1)
        weights = jnp.concatenate([meta[p, b, picks:] for b in range(dp)], axis=1)
        chosen, gate = [], []
        for e in range(experts):
            match = ids == (z * local + c * experts + e).astype(jnp.float32)
            chosen.append(jnp.max(jnp.where(match, 1.0, 0.0), axis=0, keepdims=True))
            gate.append(jnp.sum(jnp.where(match, weights, 0.0), axis=0, keepdims=True))
        chosen = jnp.concatenate(chosen, axis=0)
        gates[...] = jnp.concatenate(gate, axis=0)
        for b in range(dp):
            lanes = slice(b * tok_rows, (b + 1) * tok_rows)
            named = chosen[:, lanes]
            earlier = jnp.dot(
                named.astype(jnp.bfloat16), before, preferred_element_type=jnp.float32
            )
            keys[:, lanes] = jnp.where(named > 0.5, earlier + float(b * CAP), -1.0).astype(
                jnp.int32
            )

        def choose(e):
            row = lax.broadcasted_iota(jnp.int32, (slots, span), 0)
            match = row == keys[pl.ds(e, 1), :]
            pick[turn, e] = jnp.where(match, 1.0, 0.0).astype(jnp.bfloat16)
            gate = jnp.sum(
                jnp.where(match, gates[pl.ds(e, 1), :], 0.0), axis=1, keepdims=True
            )
            gslot[turn, e] = jnp.broadcast_to(gate, gslot.shape[2:])

        loop(0, experts, choose)
        for b in range(chips):
            relay(i, b, 0).wait_recv()
        plane = xall[p].reshape(span, half)
        chosen_rows = jnp.dot(
            pick[turn].reshape(experts * slots, span), plane, preferred_element_type=jnp.float32
        )
        rows[...] = chosen_rows.astype(jnp.bfloat16).reshape(rows.shape)

        def project(e):
            if mine:
                local_in(e).wait()
                partner_in(e).wait_recv()
            pre = jnp.dot(rows[e], win[e], preferred_element_type=jnp.float32)
            send[k, e] = pre.astype(jnp.bfloat16)

        def project_and_send(e):
            project(e)
            swap(k, e).start()

        if mine:
            loop(0, head, project_and_send)
            loop(head, experts, project)
        else:
            loop(0, experts, project_and_send)

    def second_stage(k, turn, first, end):
        def project(e):
            swap(k, e).wait_recv()
            total = send[k, e].astype(jnp.float32) + recv[k, e].astype(jnp.float32)
            h = jax.nn.gelu(total).astype(jnp.bfloat16)
            result = jnp.dot(h, wout[e], preferred_element_type=jnp.float32)
            scaled[e] = (result * gslot[turn, e][:, :1]).astype(jnp.bfloat16)

        loop(first, end, project)

    def combine(turn, first, end, lanes, count):
        return lax.dot_general(
            pick[turn, first:end, :, lanes].reshape((end - first) * slots, count),
            scaled[first:end].reshape((end - first) * slots, half),
            (((0,), (0,)), ((), ())),
            preferred_element_type=jnp.float32,
        )

    first_stage(last, 2, True)
    first_stage(0, 0, False)

    local_shared_out().wait()
    partner_shared_out().wait_recv()
    for b in range(chips):
        shared_swap(b).wait_recv()
    total = ssend[...].astype(jnp.float32) + srecv[...].astype(jnp.float32)
    h = jax.nn.gelu(total).astype(jnp.bfloat16).reshape(own_rows, -1)
    shared[...] = jnp.dot(h, sout[...], preferred_element_type=jnp.float32)

    def out_weights(e):
        local_out(e).wait()
        partner_out(e).wait_recv()

    loop(0, experts, out_weights)

    second_stage(last, 2, 0, head)
    own[...] = shared[...] + combine(2, 0, head, start_of(c, own_rows), own_rows)
    other[...] = combine(2, 0, head, start_of(oc, own_rows), own_rows)

    def plane_step(k):
        turn = lax.rem(k, 2)

        @pl.when(k < last - 1)
        def _():
            first_stage(k + 1, lax.rem(k + 1, 2), False)

        @pl.when(k == last - 1)
        def _():
            loop(head, experts, lambda e: swap(last, e).start())

        second_stage(k, turn, 0, experts)
        psend[k] = combine(turn, 0, experts, start_of(oc, own_rows), own_rows).astype(
            jnp.bfloat16
        )
        pair(k).start()
        mine = combine(turn, 0, experts, start_of(c, own_rows), own_rows)
        pair(k).wait_recv()
        zsend[k] = (mine + precv[k].astype(jnp.float32)).astype(jnp.bfloat16)
        give(k).start()

    loop(0, last, plane_step)

    second_stage(last, 2, head, experts)
    for b in (ox, x):
        lanes = start_of(oc * chips + b, tok_rows)
        extra = combine(2, head, experts, lanes, tok_rows)
        osend[b] = (other[start_of(b, tok_rows), :] + extra).astype(jnp.bfloat16)
        own_pair(b).start()
    total = own[...] + combine(2, head, experts, start_of(c, own_rows), own_rows)
    for k in range(last):
        give(k).wait_recv()
        total = total + zrecv[k].astype(jnp.float32)
    own[...] = total
    mine = start_of(x, half)
    theirs = start_of(ox, half)
    own_pair(ox).wait_recv()
    fsend[...] = (own[start_of(ox, tok_rows), :] + orecv[ox].astype(jnp.float32)).astype(
        jnp.bfloat16
    )
    finish().start()
    own_pair(x).wait_recv()
    out_ref[:, mine] = (
        tok[:, mine].astype(jnp.float32)
        + own[start_of(x, tok_rows), :]
        + orecv[x].astype(jnp.float32)
    ).astype(out_ref.dtype)

    for kind in (0, 1):
        token_swap(kind).wait_send()
    partner_shared_in().wait_send()
    partner_shared_out().wait_send()

    def weights_sent(e):
        partner_in(e).wait_send()
        partner_out(e).wait_send()
        loop(0, planes, lambda k: swap(k, e).wait_send())

    loop(0, experts, weights_sent)
    for b in range(chips):
        shared_swap(b).wait_send()
        own_pair(b).wait_send()
        for kind in (0, 1):
            loop(0, planes, lambda i: relay(i, b, kind).wait_send())
            loop(1, planes, lambda i: to_plane(i, b, kind).wait_send())

    def plane_sent(k):
        pair(k).wait_send()
        give(k).wait_send()

    loop(0, last, plane_sent)

    finish().wait()
    out_ref[:, theirs] = (
        tok[:, theirs].astype(jnp.float32) + frecv[...].astype(jnp.float32)
    ).astype(out_ref.dtype)


def fused(tokens, expert_ids, gate_weights, expert_in, expert_out, shared_in, shared_out):
    tok_rows, width = tokens.shape
    picks = expert_ids.shape[1]
    planes, dp = lax.axis_size("expert"), lax.axis_size("dp")
    cores, chips = 2, dp // 2
    local, part, hidden = expert_in.shape
    experts = local // cores
    half = width // chips
    slots, span = dp * CAP, dp * tok_rows
    own_rows = chips * tok_rows
    bf16, f32 = jnp.bfloat16, jnp.float32
    vmem, dma = pltpu.VMEM, pltpu.SemaphoreType.DMA
    scratch = [
        vmem((tok_rows, width), bf16),
        vmem((picks, tok_rows), jnp.int32),
        vmem((picks, tok_rows), f32),
        vmem((tok_rows, width), bf16),
        vmem((planes, cores, chips, tok_rows, half), bf16),
        vmem((planes, dp, 2 * picks, tok_rows), f32),
        vmem((experts, half, hidden), bf16),
        vmem((experts, hidden, half), bf16),
        vmem((half, hidden), bf16),
        vmem((hidden, half), bf16),
        vmem((experts, span), jnp.int32),
        vmem((experts, span), f32),
        vmem((3, experts, slots, span), bf16),
        vmem((3, experts, slots, 128), f32),
        vmem((experts, slots, half), bf16),
        vmem((planes, experts, slots, hidden), bf16),
        vmem((planes, experts, slots, hidden), bf16),
        vmem((chips, tok_rows, hidden), bf16),
        vmem((chips, tok_rows, hidden), bf16),
        vmem((own_rows, half), f32),
        vmem((experts, slots, half), bf16),
        vmem((own_rows, half), f32),
        vmem((own_rows, half), f32),
        vmem((planes - 1, own_rows, half), bf16),
        vmem((planes - 1, own_rows, half), bf16),
        vmem((chips, tok_rows, half), bf16),
        vmem((chips, tok_rows, half), bf16),
        vmem((planes - 1, own_rows, half), bf16),
        vmem((planes - 1, own_rows, half), bf16),
        vmem((tok_rows, half), bf16),
        vmem((tok_rows, half), bf16),
        dma((3,)),
        dma((2 * experts + 2,)),
    ]
    pairs = [
        (2 * experts + 2,),
        (2,),
        (planes - 1, chips, 2),
        (planes, chips, 2),
        (planes, experts),
        (chips,),
        (planes - 1,),
        (chips,),
        (planes - 1,),
        (1,),
    ]
    for shape in pairs:
        scratch += [dma(shape), dma(shape)]
    apart = pl.BlockSpec(memory_space=pl.ANY)
    return pl.pallas_call(
        functools.partial(fused_kernel, (planes, chips, cores)),
        in_specs=[apart] * 7,
        out_specs=pl.BlockSpec(memory_space=pltpu.VMEM),
        out_shape=jax.ShapeDtypeStruct((tok_rows, width), tokens.dtype),
        scratch_shapes=scratch,
        compiler_params=pltpu.CompilerParams(
            collective_id=0, has_side_effects=True, vmem_limit_bytes=63 * 1024 * 1024
        ),
    )(tokens, expert_ids.T, gate_weights.T, expert_in, expert_out, shared_in, shared_out)


def fits(mesh, args):
    planes, dp = mesh.shape["expert"], mesh.shape["dp"]
    tokens, expert_in = args[0], args[3]
    return (
        dp == 4
        and 1 < planes <= 8
        and expert_in.shape[0] // (mesh.shape["sweep"] * planes) % 2 == 0
        and expert_in.shape[0] // (mesh.shape["sweep"] * planes) <= 16
        and tokens.shape[0] // (mesh.shape["sweep"] * planes * dp) == 128
    )


def solution(mesh):
    placed = (
        P(("sweep", "expert", "dp"), None),
        P(("sweep", "expert", "dp"), None),
        P(("sweep", "expert", "dp"), None),
        P(("sweep", "expert"), "dp", None),
        P(("sweep", "expert"), None, "dp"),
        P(("sweep", "dp"), None),
        P("sweep", "dp"),
    )

    def run(*args):
        return jax.shard_map(
            fused if fits(mesh, args) else per_device,
            mesh=mesh,
            in_specs=placed,
            out_specs=P(("sweep", "expert", "dp"), None),
            check_vma=False,
        )(*args)

    return run
```

```python
import functools

import jax
import jax.numpy as jnp
from jax import lax
from jax.experimental import pallas as pl
from jax.experimental.pallas import tpu as pltpu
from jax.sharding import PartitionSpec as P

CAP = 20
GROUP = 4


def layer_norm(tokens):
    values = tokens.astype(jnp.float32)
    center = values - jnp.mean(values, axis=-1, keepdims=True)
    spread = jnp.mean(center * center, axis=-1, keepdims=True)
    return (center * lax.rsqrt(spread + 1e-06)).astype(jnp.bfloat16)


def first_kernel(runs, run_tokens, x_ref, key_ref, w_ref, out_ref, rows_ref):
    slots = out_ref.shape[3]
    for j in range(runs):
        span = slice(j * run_tokens, (j + 1) * run_tokens)
        row = lax.broadcasted_iota(jnp.int32, (slots, run_tokens), 0)
        pick = jnp.where(row == key_ref[0, :, span], 1.0, 0.0).astype(jnp.bfloat16)
        rows_ref[j * slots : (j + 1) * slots, :] = jnp.dot(
            pick, x_ref[span, :], preferred_element_type=jnp.float32
        ).astype(jnp.bfloat16)
    pre = jnp.dot(rows_ref[...], w_ref[0], preferred_element_type=jnp.float32)
    for j in range(runs):
        out_ref[j, 0, 0] = pre[j * slots : (j + 1) * slots].astype(jnp.bfloat16)


def first_projection(x, keys, weight, first, count, runs, run_tokens, slots):
    width, hidden = weight.shape[1:]
    chunk = runs * run_tokens
    chunks = x.shape[0] // chunk
    total = count * chunks * runs * slots
    return pl.pallas_call(
        functools.partial(first_kernel, runs, run_tokens),
        grid=(count, chunks),
        in_specs=[
            pl.BlockSpec((chunk, width), lambda e, c: (c, 0)),
            pl.BlockSpec((1, 1, chunk), lambda e, c: (e + first, 0, c)),
            pl.BlockSpec((1, width, hidden), lambda e, c: (e + first, 0, 0)),
        ],
        out_specs=pl.BlockSpec((runs, 1, 1, slots, hidden), lambda e, c: (0, e, c, 0, 0)),
        out_shape=jax.ShapeDtypeStruct((runs, count, chunks, slots, hidden), jnp.bfloat16),
        scratch_shapes=[pltpu.VMEM((runs * slots, width), jnp.bfloat16)],
        cost_estimate=pl.CostEstimate(
            flops=2 * total * width * (hidden + run_tokens),
            bytes_accessed=2 * (count * width * hidden + total * hidden + x.size),
            transcendentals=0,
        ),
    )(x, keys, weight)


def second_kernel(runs, run_tokens, h_ref, key_ref, gate_ref, w_ref, *refs):
    carry_ref, (out_ref, total_ref) = refs[0] if len(refs) == 3 else None, refs[-2:]
    expert = pl.program_id(1)
    slots = h_ref.shape[3]

    @pl.when(expert == 0)
    def _():
        total_ref[...] = jnp.zeros_like(total_ref) if carry_ref is None else carry_ref[...]

    h = jnp.concatenate([h_ref[j, 0, 0] for j in range(runs)], axis=0)
    result = jnp.dot(h, w_ref[0], preferred_element_type=jnp.float32)
    for j in range(runs):
        span = slice(j * run_tokens, (j + 1) * run_tokens)
        row = lax.broadcasted_iota(jnp.int32, (slots, run_tokens), 0)
        match = row == key_ref[0, :, span]
        gate = jnp.sum(jnp.where(match, gate_ref[0, :, span], 0.0), axis=1, keepdims=True)
        scaled = (result[j * slots : (j + 1) * slots] * gate).astype(jnp.bfloat16)
        total_ref[span, :] += lax.dot_general(
            jnp.where(match, 1.0, 0.0).astype(jnp.bfloat16),
            scaled,
            (((0,), (0,)), ((), ())),
            preferred_element_type=jnp.float32,
        )

    @pl.when(expert == pl.num_programs(1) - 1)
    def _():
        out_ref[...] = total_ref[...].astype(out_ref.dtype)


def second_projection(hidden, keys, gates, weight, carry, kind, first, runs, run_tokens):
    _, count, chunks, slots, depth = hidden.shape
    width = weight.shape[2]
    chunk = runs * run_tokens
    total = count * chunks * runs * slots
    carries = [] if carry is None else [carry]
    return pl.pallas_call(
        functools.partial(second_kernel, runs, run_tokens),
        grid=(chunks, count),
        in_specs=[
            pl.BlockSpec((runs, 1, 1, slots, depth), lambda c, e: (0, e, c, 0, 0)),
            pl.BlockSpec((1, 1, chunk), lambda c, e: (e + first, 0, c)),
            pl.BlockSpec((1, 1, chunk), lambda c, e: (e + first, 0, c)),
            pl.BlockSpec((1, depth, width), lambda c, e: (e + first, 0, 0)),
        ]
        + [pl.BlockSpec((chunk, width), lambda c, e: (c, 0)) for _ in carries],
        out_specs=pl.BlockSpec((chunk, width), lambda c, e: (c, 0)),
        out_shape=jax.ShapeDtypeStruct((chunks * chunk, width), kind),
        scratch_shapes=[pltpu.VMEM((chunk, width), jnp.float32)],
        cost_estimate=pl.CostEstimate(
            flops=2 * total * width * (depth + 3 * run_tokens),
            bytes_accessed=2 * (count * depth * width + total * depth) + 4 * chunks * chunk * width,
            transcendentals=0,
        ),
    )(hidden, keys, gates, weight, *carries)


def per_device(tokens, expert_ids, gate_weights, expert_in, expert_out, shared_in, shared_out):
    row_count, model_width = tokens.shape
    pick_count = expert_ids.shape[1]
    local_count = expert_in.shape[0]
    runs = lax.axis_size("dp")
    block_count = runs * lax.axis_size("expert")
    run_tokens = GROUP * row_count
    slots = GROUP * CAP
    halves = 2 if local_count % 2 == 0 else 1

    normed = layer_norm(tokens)
    full_shared_in = lax.all_gather(shared_in, "dp", axis=0, tiled=True)
    full_shared_out = lax.all_gather(shared_out, "dp", axis=1, tiled=True)

    named = jnp.concatenate([expert_ids.astype(jnp.float32), gate_weights], axis=1).T
    named = lax.all_gather(named, ("expert", "dp"), axis=0, tiled=False)
    ids, gates = named[:, :pick_count], named[:, pick_count:]
    columns = lax.all_to_all(normed, "dp", split_axis=1, concat_axis=0, tiled=True)
    columns, full_shared_in, full_shared_out = lax.optimization_barrier(
        (columns, full_shared_in, full_shared_out)
    )
    x = lax.all_gather(columns, "expert", axis=0, tiled=True)

    owned = lax.axis_index("expert") * local_count + jnp.arange(local_count, dtype=jnp.int32)
    matches = ids[:, :, None, :] == owned.astype(jnp.float32)[:, None]
    chosen = jnp.any(matches, axis=1)
    gate_of = jnp.sum(jnp.where(matches, gates[:, :, None, :], 0.0), axis=1)
    order = jnp.arange(row_count, dtype=jnp.int32)
    before = (order[:, None] < order[None, :]).astype(jnp.bfloat16)
    earlier = jnp.einsum(
        "bej,ji->bei", chosen.astype(jnp.bfloat16), before, preferred_element_type=jnp.float32
    ).astype(jnp.int32)
    base = jnp.arange(block_count, dtype=jnp.int32) % GROUP * CAP
    keys = jnp.where(chosen, earlier + base[:, None, None], -1)

    def by_expert(table):
        return table.transpose(1, 0, 2).reshape(local_count, 1, block_count * row_count)

    keys, gate_of = by_expert(keys), by_expert(gate_of)

    count = local_count // halves
    parts = []
    for half in range(halves):
        pre = first_projection(
            x, keys, expert_in, half * count, count, runs, run_tokens, slots
        )
        parts.append(lax.psum_scatter(pre, "dp", scatter_dimension=0, tiled=True))

    hidden = []
    for pre in parts:
        act = jax.nn.gelu(pre.astype(jnp.float32)).astype(jnp.bfloat16)
        hidden.append(lax.all_gather(act, "dp", axis=0, tiled=True))

    shared_pre = jnp.dot(normed, full_shared_in, preferred_element_type=jnp.float32)
    shared_hidden = jax.nn.gelu(shared_pre).astype(jnp.bfloat16)
    shared_result = jnp.dot(shared_hidden, full_shared_out, preferred_element_type=jnp.float32)

    routed = None
    for half, h in enumerate(hidden):
        kind = jnp.bfloat16 if half == halves - 1 else jnp.float32
        routed = second_projection(
            h, keys, gate_of, expert_out, routed, kind, half * count, runs, run_tokens
        )
    width = routed.shape[1]
    pieces = lax.all_to_all(
        routed.reshape(block_count, row_count, width),
        ("expert", "dp"),
        split_axis=0,
        concat_axis=0,
        tiled=True,
    ).reshape(-1, runs, row_count, width)
    own = jnp.sum(pieces.astype(jnp.float32), axis=0).transpose(1, 0, 2)
    own = own.reshape(row_count, model_width)
    return (tokens.astype(jnp.float32) + shared_result + own).astype(jnp.bfloat16)


def start_of(index, size):
    return pl.ds(pl.multiple_of(index * size, size), size)


HEAD = 3


def plane_orders(planes):
    if planes == 4:
        return ((1, 2, 1, 2), (3, 3, 0, 0), (2, 0, 3, 1))
    return tuple(tuple((z + k) % planes for z in range(planes)) for k in range(1, planes))


def fused_kernel(
    sizes,
    tok_hbm,
    ids_hbm,
    gate_hbm,
    win_hbm,
    wout_hbm,
    sin_hbm,
    sout_hbm,
    out_ref,
    tok,
    ids_in,
    gate_in,
    norm,
    xall,
    meta,
    win,
    wout,
    sin,
    sout,
    keys,
    gates,
    pick,
    gslot,
    rows,
    send,
    recv,
    ssend,
    srecv,
    scaled,
    own,
    other,
    psend,
    precv,
    osend,
    orecv,
    zsend,
    zrecv,
    fsend,
    frecv,
    isem,
    lsem,
    wssem,
    wrsem,
    xssem,
    xrsem,
    zssem,
    zrsem,
    rssem,
    rrsem,
    pssem,
    prsem,
    ssem,
    srsem,
    dssem,
    drsem,
    bssem,
    brsem,
    ossem,
    orsem,
    fssem,
    frsem,
):
    planes, chips, cores = sizes
    dp = chips * cores
    tok_rows, width = tok.shape
    picks = ids_in.shape[0]
    half = width // chips
    part = half // cores
    experts = win.shape[0]
    local = experts * cores
    slots, span = pick.shape[2:]
    own_rows = chips * tok_rows
    last = planes - 1
    head = min(HEAD, experts // 2)
    close = max(experts - 2, head + 1)

    z = lax.axis_index("expert")
    d = lax.axis_index("dp")
    c = d % cores
    x = d // cores
    oc = 1 - c
    ox = 1 - x
    partner = {"dp": x * cores + oc}
    across = {"dp": ox * cores + c}
    mesh_ids = pl.DeviceIdType.MESH

    def remote(src, dst, s_sem, r_sem, device):
        return pltpu.make_async_remote_copy(
            src_ref=src,
            dst_ref=dst,
            send_sem=s_sem,
            recv_sem=r_sem,
            device_id=device,
            device_id_type=mesh_ids,
        )

    def loop(first, end, body):
        def step(i, carry):
            body(i)
            return carry

        lax.fori_loop(first, end, step, 0)

    orders = plane_orders(planes)

    def at_step(k):
        found = 0
        for step, order in enumerate(orders):
            for place, p in enumerate(order):
                hit = jnp.logical_and(k == step, z == place)
                found = jnp.where(hit, p, found)
        return jnp.where(k == last, z, found)

    def local_in(e):
        return pltpu.make_async_copy(
            win_hbm.at[c * experts + e], win.at[e, start_of(c, part)], lsem.at[e]
        )

    def local_out(e):
        return pltpu.make_async_copy(
            wout_hbm.at[c * experts + e],
            wout.at[e, :, start_of(c, part)],
            lsem.at[experts + e],
        )

    def local_shared_in():
        return pltpu.make_async_copy(sin_hbm, sin.at[start_of(c, part)], lsem.at[2 * experts])

    def local_shared_out():
        return pltpu.make_async_copy(
            sout_hbm, sout.at[:, start_of(c, part)], lsem.at[2 * experts + 1]
        )

    def partner_in(e):
        return remote(
            win_hbm.at[oc * experts + e],
            win.at[e, start_of(c, part)],
            wssem.at[e],
            wrsem.at[e],
            partner,
        )

    def partner_out(e):
        return remote(
            wout_hbm.at[oc * experts + e],
            wout.at[e, :, start_of(c, part)],
            wssem.at[experts + e],
            wrsem.at[experts + e],
            partner,
        )

    def partner_shared_in():
        return remote(
            sin_hbm,
            sin.at[start_of(c, part)],
            wssem.at[2 * experts],
            wrsem.at[2 * experts],
            partner,
        )

    def partner_shared_out():
        return remote(
            sout_hbm,
            sout.at[:, start_of(c, part)],
            wssem.at[2 * experts + 1],
            wrsem.at[2 * experts + 1],
            partner,
        )

    def block(p, b, kind):
        return meta.at[p, c * chips + b] if kind else xall.at[p, c, b]

    def token_swap(kind):
        src = meta.at[z, c * chips + x] if kind else norm.at[:, start_of(ox, half)]
        return remote(src, block(z, x, kind), xssem.at[kind], xrsem.at[kind], across)

    def to_plane(p, b, kind):
        ref = block(z, b, kind)
        return remote(
            ref, ref, zssem.at[p, b, kind], zrsem.at[z, b, kind], {"expert": p}
        )

    def from_plane(p, b, kind):
        ref = block(p, b, kind)
        return remote(
            ref, ref, zssem.at[p, b, kind], zrsem.at[p, b, kind], {"expert": p}
        )

    def send_tokens(k, b):
        for p in range(planes):

            @pl.when(z == orders[k][p])
            def _():
                for kind in (1, 0):
                    to_plane(p, b, kind).start()

    def relay(p, b, kind):
        ref = block(p, b, kind)
        return remote(ref, ref, rssem.at[p, b, kind], rrsem.at[p, b, kind], partner)

    def swap(k, e):
        return remote(send.at[k, e], recv.at[k, e], pssem.at[k, e], prsem.at[k, e], across)

    def shared_swap(b):
        return remote(ssend.at[b], srecv.at[b], ssem.at[b], srsem.at[b], across)

    def pair(k):
        return remote(psend.at[k], precv.at[k], dssem.at[k], drsem.at[k], partner)

    def own_pair(b):
        return remote(osend.at[b], orecv.at[b], bssem.at[b], brsem.at[b], partner)

    def give(k):
        return remote(
            zsend.at[k], zrecv.at[z], ossem.at[k], orsem.at[z], {"expert": at_step(k)}
        )

    def given(p):
        return remote(zsend.at[0], zrecv.at[p], ossem.at[0], orsem.at[p], {"expert": p})

    def finish():
        return remote(fsend, frecv, fssem.at[0], frsem.at[0], across)

    barrier = pltpu.get_barrier_semaphore()
    peers = [{"expert": lax.rem(z + i, planes)} for i in range(1, planes)]
    for device in [across, partner] + peers:
        pl.semaphore_signal(barrier, inc=1, device_id=device, device_id_type=mesh_ids)
    read_tok = pltpu.make_async_copy(tok_hbm, tok, isem.at[0])
    read_ids = pltpu.make_async_copy(ids_hbm, ids_in, isem.at[1])
    read_gate = pltpu.make_async_copy(gate_hbm, gate_in, isem.at[2])
    read_tok.start()
    read_ids.start()
    read_gate.start()
    local_shared_in().start()
    loop(0, experts, lambda e: local_in(e).start())
    local_shared_out().start()
    loop(0, experts, lambda e: local_out(e).start())
    read_ids.wait()
    read_gate.wait()
    meta[z, c * chips + x, :picks] = ids_in[...].astype(jnp.float32)
    meta[z, c * chips + x, picks:] = gate_in[...]
    read_tok.wait()
    values = tok[...].astype(jnp.float32)
    center = values - jnp.mean(values, axis=-1, keepdims=True)
    spread = jnp.mean(center * center, axis=-1, keepdims=True)
    norm[...] = (center * lax.rsqrt(spread + 1e-06)).astype(jnp.bfloat16)
    xall[z, c, x] = norm[:, start_of(x, half)]

    pl.semaphore_wait(barrier, planes + 1)
    early = min(3, experts)
    for kind in (1, 0):
        token_swap(kind).start()
    for kind in (1, 0):
        relay(z, x, kind).start()
    send_tokens(0, x)
    partner_shared_in().start()
    loop(0, early, lambda e: partner_in(e).start())

    def shared_first(b):
        pre = jnp.dot(xall[z, c, b], sin[...], preferred_element_type=jnp.float32)
        ssend[b] = pre.astype(jnp.bfloat16)

    local_shared_in().wait()
    partner_shared_in().wait_recv()
    shared_first(x)
    shared_swap(x).start()
    for kind in (1, 0):
        token_swap(kind).wait_recv()
        relay(z, ox, kind).start()
    send_tokens(0, ox)
    loop(early, experts, lambda e: partner_in(e).start())
    partner_shared_out().start()
    loop(0, experts, lambda e: partner_out(e).start())
    shared_first(ox)
    shared_swap(ox).start()

    before = jnp.where(
        lax.broadcasted_iota(jnp.int32, (tok_rows, tok_rows), 0)
        < lax.broadcasted_iota(jnp.int32, (tok_rows, tok_rows), 1),
        1.0,
        0.0,
    ).astype(jnp.bfloat16)

    def first_stage(k, turn, mine):
        p = z if mine else at_step(k)
        if not mine:
            for kind in (1, 0):
                for b in range(chips):
                    from_plane(p, b, kind).wait_recv()
                    relay(p, b, kind).start()
            for step in range(1, last):

                @pl.when(k == step - 1)
                def _():
                    for b in (x, ox):
                        send_tokens(step, b)

        for b in range(chips):
            relay(p, b, 1).wait_recv()

        ids = jnp.concatenate([meta[p, b, :picks] for b in range(dp)], axis=1)
        weights = jnp.concatenate([meta[p, b, picks:] for b in range(dp)], axis=1)
        chosen, gate = [], []
        for e in range(experts):
            match = ids == (z * local + c * experts + e).astype(jnp.float32)
            chosen.append(jnp.max(jnp.where(match, 1.0, 0.0), axis=0, keepdims=True))
            gate.append(jnp.sum(jnp.where(match, weights, 0.0), axis=0, keepdims=True))
        chosen = jnp.concatenate(chosen, axis=0)
        gates[...] = jnp.concatenate(gate, axis=0)
        for b in range(dp):
            lanes = slice(b * tok_rows, (b + 1) * tok_rows)
            named = chosen[:, lanes]
            earlier = jnp.dot(
                named.astype(jnp.bfloat16), before, preferred_element_type=jnp.float32
            )
            keys[:, lanes] = jnp.where(named > 0.5, earlier + float(b * CAP), -1.0).astype(
                jnp.int32
            )

        def choose(e):
            row = lax.broadcasted_iota(jnp.int32, (slots, span), 0)
            match = row == keys[pl.ds(e, 1), :]
            pick[turn, e] = jnp.where(match, 1.0, 0.0).astype(jnp.bfloat16)
            gate = jnp.sum(
                jnp.where(match, gates[pl.ds(e, 1), :], 0.0), axis=1, keepdims=True
            )
            gslot[turn, e] = jnp.broadcast_to(gate, gslot.shape[2:])

        loop(0, experts, choose)
        for b in range(chips):
            relay(p, b, 0).wait_recv()
        plane = xall[p].reshape(span, half)
        chosen_rows = jnp.dot(
            pick[turn].reshape(experts * slots, span), plane, preferred_element_type=jnp.float32
        )
        rows[...] = chosen_rows.astype(jnp.bfloat16).reshape(rows.shape)

        def project(e):
            if mine:
                local_in(e).wait()
                partner_in(e).wait_recv()
            pre = jnp.dot(rows[e], win[e], preferred_element_type=jnp.float32)
            send[k, e] = pre.astype(jnp.bfloat16)

        def project_and_send(e):
            project(e)
            swap(k, e).start()

        if mine:
            loop(0, head, project_and_send)
            loop(head, experts, project)
        else:
            loop(0, experts, project_and_send)

    def second_stage(k, turn, first, end):
        def project(e):
            swap(k, e).wait_recv()
            total = send[k, e].astype(jnp.float32) + recv[k, e].astype(jnp.float32)
            h = jax.nn.gelu(total).astype(jnp.bfloat16)
            result = jnp.dot(h, wout[e], preferred_element_type=jnp.float32)
            scaled[e] = (result * gslot[turn, e][:, :1]).astype(jnp.bfloat16)

        loop(first, end, project)

    def combine(turn, first, end, lanes, count):
        return lax.dot_general(
            pick[turn, first:end, :, lanes].reshape((end - first) * slots, count),
            scaled[first:end].reshape((end - first) * slots, half),
            (((0,), (0,)), ((), ())),
            preferred_element_type=jnp.float32,
        )

    first_stage(last, 2, True)
    first_stage(0, 0, False)

    local_shared_out().wait()
    partner_shared_out().wait_recv()

    def shared_second(b):
        shared_swap(b).wait_recv()
        total = ssend[b].astype(jnp.float32) + srecv[b].astype(jnp.float32)
        h = jax.nn.gelu(total).astype(jnp.bfloat16)
        own[start_of(b, tok_rows), :] += jnp.dot(
            h, sout[...], preferred_element_type=jnp.float32
        )

    def out_weights(e):
        local_out(e).wait()
        partner_out(e).wait_recv()

    loop(0, experts, out_weights)

    second_stage(last, 2, 0, head)
    own[...] = combine(2, 0, head, start_of(c, own_rows), own_rows)
    other[...] = combine(2, 0, head, start_of(oc, own_rows), own_rows)
    for b in range(chips):
        shared_second(b)

    def plane_step(k):
        turn = lax.rem(k, 2)

        @pl.when(k < last - 1)
        def _():
            first_stage(k + 1, lax.rem(k + 1, 2), False)

        @pl.when(k == last - 1)
        def _():
            loop(head, experts, lambda e: swap(last, e).start())

        second_stage(k, turn, 0, experts)
        psend[k] = combine(turn, 0, experts, start_of(oc, own_rows), own_rows).astype(
            jnp.bfloat16
        )
        pair(k).start()
        mine = combine(turn, 0, experts, start_of(c, own_rows), own_rows)
        pair(k).wait_recv()
        zsend[k] = (mine + precv[k].astype(jnp.float32)).astype(jnp.bfloat16)
        give(k).start()

    loop(0, last, plane_step)

    second_stage(last, 2, head, close)
    own[...] += combine(2, head, close, start_of(c, own_rows), own_rows)
    other[...] += combine(2, head, close, start_of(oc, own_rows), own_rows)
    second_stage(last, 2, close, experts)
    for b in (ox, x):
        lanes = start_of(oc * chips + b, tok_rows)
        extra = combine(2, close, experts, lanes, tok_rows)
        osend[b] = (other[start_of(b, tok_rows), :] + extra).astype(jnp.bfloat16)
        own_pair(b).start()
    total = own[...] + combine(2, close, experts, start_of(c, own_rows), own_rows)
    for r in range(1, planes):
        p = lax.rem(z + r, planes)
        given(p).wait_recv()
        total = total + zrecv[p].astype(jnp.float32)
    own[...] = total
    mine = start_of(x, half)
    theirs = start_of(ox, half)
    own_pair(ox).wait_recv()
    fsend[...] = (own[start_of(ox, tok_rows), :] + orecv[ox].astype(jnp.float32)).astype(
        jnp.bfloat16
    )
    finish().start()
    own_pair(x).wait_recv()
    out_ref[:, mine] = (
        tok[:, mine].astype(jnp.float32)
        + own[start_of(x, tok_rows), :]
        + orecv[x].astype(jnp.float32)
    ).astype(out_ref.dtype)

    for kind in (0, 1):
        token_swap(kind).wait_send()
    partner_shared_in().wait_send()
    partner_shared_out().wait_send()

    def weights_sent(e):
        partner_in(e).wait_send()
        partner_out(e).wait_send()
        loop(0, planes, lambda k: swap(k, e).wait_send())

    loop(0, experts, weights_sent)
    for b in range(chips):
        shared_swap(b).wait_send()
        own_pair(b).wait_send()
        for kind in (0, 1):
            loop(0, planes, lambda p: relay(p, b, kind).wait_send())
            loop(
                1,
                planes,
                lambda r: to_plane(lax.rem(z + r, planes), b, kind).wait_send(),
            )

    def plane_sent(k):
        pair(k).wait_send()
        give(k).wait_send()

    loop(0, last, plane_sent)

    finish().wait()
    out_ref[:, theirs] = (
        tok[:, theirs].astype(jnp.float32) + frecv[...].astype(jnp.float32)
    ).astype(out_ref.dtype)


def fused(tokens, expert_ids, gate_weights, expert_in, expert_out, shared_in, shared_out):
    tok_rows, width = tokens.shape
    picks = expert_ids.shape[1]
    planes, dp = lax.axis_size("expert"), lax.axis_size("dp")
    cores, chips = 2, dp // 2
    local, part, hidden = expert_in.shape
    experts = local // cores
    half = width // chips
    slots, span = dp * CAP, dp * tok_rows
    own_rows = chips * tok_rows
    bf16, f32 = jnp.bfloat16, jnp.float32
    vmem, dma = pltpu.VMEM, pltpu.SemaphoreType.DMA
    scratch = [
        vmem((tok_rows, width), bf16),
        vmem((picks, tok_rows), jnp.int32),
        vmem((picks, tok_rows), f32),
        vmem((tok_rows, width), bf16),
        vmem((planes, cores, chips, tok_rows, half), bf16),
        vmem((planes, dp, 2 * picks, tok_rows), f32),
        vmem((experts, half, hidden), bf16),
        vmem((experts, hidden, half), bf16),
        vmem((half, hidden), bf16),
        vmem((hidden, half), bf16),
        vmem((experts, span), jnp.int32),
        vmem((experts, span), f32),
        vmem((3, experts, slots, span), bf16),
        vmem((3, experts, slots, 128), f32),
        vmem((experts, slots, half), bf16),
        vmem((planes, experts, slots, hidden), bf16),
        vmem((planes, experts, slots, hidden), bf16),
        vmem((chips, tok_rows, hidden), bf16),
        vmem((chips, tok_rows, hidden), bf16),
        vmem((experts, slots, half), bf16),
        vmem((own_rows, half), f32),
        vmem((own_rows, half), f32),
        vmem((planes - 1, own_rows, half), bf16),
        vmem((planes - 1, own_rows, half), bf16),
        vmem((chips, tok_rows, half), bf16),
        vmem((chips, tok_rows, half), bf16),
        vmem((planes - 1, own_rows, half), bf16),
        vmem((planes, own_rows, half), bf16),
        vmem((tok_rows, half), bf16),
        vmem((tok_rows, half), bf16),
        dma((3,)),
        dma((2 * experts + 2,)),
    ]
    pairs = [
        (2 * experts + 2,),
        (2,),
        (planes, chips, 2),
        (planes, chips, 2),
        (planes, experts),
        (chips,),
        (planes - 1,),
        (chips,),
        (planes,),
        (1,),
    ]
    for shape in pairs:
        scratch += [dma(shape), dma(shape)]
    apart = pl.BlockSpec(memory_space=pl.ANY)
    return pl.pallas_call(
        functools.partial(fused_kernel, (planes, chips, cores)),
        in_specs=[apart] * 7,
        out_specs=pl.BlockSpec(memory_space=pltpu.VMEM),
        out_shape=jax.ShapeDtypeStruct((tok_rows, width), tokens.dtype),
        scratch_shapes=scratch,
        compiler_params=pltpu.CompilerParams(
            collective_id=0, has_side_effects=True, vmem_limit_bytes=63 * 1024 * 1024
        ),
    )(tokens, expert_ids.T, gate_weights.T, expert_in, expert_out, shared_in, shared_out)


def fits(mesh, args):
    planes, dp = mesh.shape["expert"], mesh.shape["dp"]
    tokens, expert_in = args[0], args[3]
    return (
        dp == 4
        and 1 < planes <= 8
        and expert_in.shape[0] // (mesh.shape["sweep"] * planes) % 2 == 0
        and expert_in.shape[0] // (mesh.shape["sweep"] * planes) <= 16
        and tokens.shape[0] // (mesh.shape["sweep"] * planes * dp) == 128
    )


def solution(mesh):
    placed = (
        P(("sweep", "expert", "dp"), None),
        P(("sweep", "expert", "dp"), None),
        P(("sweep", "expert", "dp"), None),
        P(("sweep", "expert"), "dp", None),
        P(("sweep", "expert"), None, "dp"),
        P(("sweep", "dp"), None),
        P("sweep", "dp"),
    )

    def run(*args):
        return jax.shard_map(
            fused if fits(mesh, args) else per_device,
            mesh=mesh,
            in_specs=placed,
            out_specs=P(("sweep", "expert", "dp"), None),
            check_vma=False,
        )(*args)

    return run
```

```python
import functools

import jax
import jax.numpy as jnp
from jax import lax
from jax.experimental import pallas as pl
from jax.experimental.pallas import tpu as pltpu
from jax.sharding import PartitionSpec as P

CAP = 20
GROUP = 4


def layer_norm(tokens):
    values = tokens.astype(jnp.float32)
    center = values - jnp.mean(values, axis=-1, keepdims=True)
    spread = jnp.mean(center * center, axis=-1, keepdims=True)
    return (center * lax.rsqrt(spread + 1e-06)).astype(jnp.bfloat16)


def first_kernel(runs, run_tokens, x_ref, key_ref, w_ref, out_ref, rows_ref):
    slots = out_ref.shape[3]
    for j in range(runs):
        span = slice(j * run_tokens, (j + 1) * run_tokens)
        row = lax.broadcasted_iota(jnp.int32, (slots, run_tokens), 0)
        pick = jnp.where(row == key_ref[0, :, span], 1.0, 0.0).astype(jnp.bfloat16)
        rows_ref[j * slots : (j + 1) * slots, :] = jnp.dot(
            pick, x_ref[span, :], preferred_element_type=jnp.float32
        ).astype(jnp.bfloat16)
    pre = jnp.dot(rows_ref[...], w_ref[0], preferred_element_type=jnp.float32)
    for j in range(runs):
        out_ref[j, 0, 0] = pre[j * slots : (j + 1) * slots].astype(jnp.bfloat16)


def first_projection(x, keys, weight, first, count, runs, run_tokens, slots):
    width, hidden = weight.shape[1:]
    chunk = runs * run_tokens
    chunks = x.shape[0] // chunk
    total = count * chunks * runs * slots
    return pl.pallas_call(
        functools.partial(first_kernel, runs, run_tokens),
        grid=(count, chunks),
        in_specs=[
            pl.BlockSpec((chunk, width), lambda e, c: (c, 0)),
            pl.BlockSpec((1, 1, chunk), lambda e, c: (e + first, 0, c)),
            pl.BlockSpec((1, width, hidden), lambda e, c: (e + first, 0, 0)),
        ],
        out_specs=pl.BlockSpec((runs, 1, 1, slots, hidden), lambda e, c: (0, e, c, 0, 0)),
        out_shape=jax.ShapeDtypeStruct((runs, count, chunks, slots, hidden), jnp.bfloat16),
        scratch_shapes=[pltpu.VMEM((runs * slots, width), jnp.bfloat16)],
        cost_estimate=pl.CostEstimate(
            flops=2 * total * width * (hidden + run_tokens),
            bytes_accessed=2 * (count * width * hidden + total * hidden + x.size),
            transcendentals=0,
        ),
    )(x, keys, weight)


def second_kernel(runs, run_tokens, h_ref, key_ref, gate_ref, w_ref, *refs):
    carry_ref, (out_ref, total_ref) = refs[0] if len(refs) == 3 else None, refs[-2:]
    expert = pl.program_id(1)
    slots = h_ref.shape[3]

    @pl.when(expert == 0)
    def _():
        total_ref[...] = jnp.zeros_like(total_ref) if carry_ref is None else carry_ref[...]

    h = jnp.concatenate([h_ref[j, 0, 0] for j in range(runs)], axis=0)
    result = jnp.dot(h, w_ref[0], preferred_element_type=jnp.float32)
    for j in range(runs):
        span = slice(j * run_tokens, (j + 1) * run_tokens)
        row = lax.broadcasted_iota(jnp.int32, (slots, run_tokens), 0)
        match = row == key_ref[0, :, span]
        gate = jnp.sum(jnp.where(match, gate_ref[0, :, span], 0.0), axis=1, keepdims=True)
        scaled = (result[j * slots : (j + 1) * slots] * gate).astype(jnp.bfloat16)
        total_ref[span, :] += lax.dot_general(
            jnp.where(match, 1.0, 0.0).astype(jnp.bfloat16),
            scaled,
            (((0,), (0,)), ((), ())),
            preferred_element_type=jnp.float32,
        )

    @pl.when(expert == pl.num_programs(1) - 1)
    def _():
        out_ref[...] = total_ref[...].astype(out_ref.dtype)


def second_projection(hidden, keys, gates, weight, carry, kind, first, runs, run_tokens):
    _, count, chunks, slots, depth = hidden.shape
    width = weight.shape[2]
    chunk = runs * run_tokens
    total = count * chunks * runs * slots
    carries = [] if carry is None else [carry]
    return pl.pallas_call(
        functools.partial(second_kernel, runs, run_tokens),
        grid=(chunks, count),
        in_specs=[
            pl.BlockSpec((runs, 1, 1, slots, depth), lambda c, e: (0, e, c, 0, 0)),
            pl.BlockSpec((1, 1, chunk), lambda c, e: (e + first, 0, c)),
            pl.BlockSpec((1, 1, chunk), lambda c, e: (e + first, 0, c)),
            pl.BlockSpec((1, depth, width), lambda c, e: (e + first, 0, 0)),
        ]
        + [pl.BlockSpec((chunk, width), lambda c, e: (c, 0)) for _ in carries],
        out_specs=pl.BlockSpec((chunk, width), lambda c, e: (c, 0)),
        out_shape=jax.ShapeDtypeStruct((chunks * chunk, width), kind),
        scratch_shapes=[pltpu.VMEM((chunk, width), jnp.float32)],
        cost_estimate=pl.CostEstimate(
            flops=2 * total * width * (depth + 3 * run_tokens),
            bytes_accessed=2 * (count * depth * width + total * depth) + 4 * chunks * chunk * width,
            transcendentals=0,
        ),
    )(hidden, keys, gates, weight, *carries)


def per_device(tokens, expert_ids, gate_weights, expert_in, expert_out, shared_in, shared_out):
    row_count, model_width = tokens.shape
    pick_count = expert_ids.shape[1]
    local_count = expert_in.shape[0]
    runs = lax.axis_size("dp")
    block_count = runs * lax.axis_size("expert")
    run_tokens = GROUP * row_count
    slots = GROUP * CAP
    halves = 2 if local_count % 2 == 0 else 1

    normed = layer_norm(tokens)
    full_shared_in = lax.all_gather(shared_in, "dp", axis=0, tiled=True)
    full_shared_out = lax.all_gather(shared_out, "dp", axis=1, tiled=True)

    named = jnp.concatenate([expert_ids.astype(jnp.float32), gate_weights], axis=1).T
    named = lax.all_gather(named, ("expert", "dp"), axis=0, tiled=False)
    ids, gates = named[:, :pick_count], named[:, pick_count:]
    columns = lax.all_to_all(normed, "dp", split_axis=1, concat_axis=0, tiled=True)
    columns, full_shared_in, full_shared_out = lax.optimization_barrier(
        (columns, full_shared_in, full_shared_out)
    )
    x = lax.all_gather(columns, "expert", axis=0, tiled=True)

    owned = lax.axis_index("expert") * local_count + jnp.arange(local_count, dtype=jnp.int32)
    matches = ids[:, :, None, :] == owned.astype(jnp.float32)[:, None]
    chosen = jnp.any(matches, axis=1)
    gate_of = jnp.sum(jnp.where(matches, gates[:, :, None, :], 0.0), axis=1)
    order = jnp.arange(row_count, dtype=jnp.int32)
    before = (order[:, None] < order[None, :]).astype(jnp.bfloat16)
    earlier = jnp.einsum(
        "bej,ji->bei", chosen.astype(jnp.bfloat16), before, preferred_element_type=jnp.float32
    ).astype(jnp.int32)
    base = jnp.arange(block_count, dtype=jnp.int32) % GROUP * CAP
    keys = jnp.where(chosen, earlier + base[:, None, None], -1)

    def by_expert(table):
        return table.transpose(1, 0, 2).reshape(local_count, 1, block_count * row_count)

    keys, gate_of = by_expert(keys), by_expert(gate_of)

    count = local_count // halves
    parts = []
    for half in range(halves):
        pre = first_projection(
            x, keys, expert_in, half * count, count, runs, run_tokens, slots
        )
        parts.append(lax.psum_scatter(pre, "dp", scatter_dimension=0, tiled=True))

    hidden = []
    for pre in parts:
        act = jax.nn.gelu(pre.astype(jnp.float32)).astype(jnp.bfloat16)
        hidden.append(lax.all_gather(act, "dp", axis=0, tiled=True))

    shared_pre = jnp.dot(normed, full_shared_in, preferred_element_type=jnp.float32)
    shared_hidden = jax.nn.gelu(shared_pre).astype(jnp.bfloat16)
    shared_result = jnp.dot(shared_hidden, full_shared_out, preferred_element_type=jnp.float32)

    routed = None
    for half, h in enumerate(hidden):
        kind = jnp.bfloat16 if half == halves - 1 else jnp.float32
        routed = second_projection(
            h, keys, gate_of, expert_out, routed, kind, half * count, runs, run_tokens
        )
    width = routed.shape[1]
    pieces = lax.all_to_all(
        routed.reshape(block_count, row_count, width),
        ("expert", "dp"),
        split_axis=0,
        concat_axis=0,
        tiled=True,
    ).reshape(-1, runs, row_count, width)
    own = jnp.sum(pieces.astype(jnp.float32), axis=0).transpose(1, 0, 2)
    own = own.reshape(row_count, model_width)
    return (tokens.astype(jnp.float32) + shared_result + own).astype(jnp.bfloat16)


def start_of(index, size):
    return pl.ds(pl.multiple_of(index * size, size), size)


HEAD = 3


def plane_orders(planes):
    if planes == 4:
        return ((1, 2, 1, 2), (3, 3, 0, 0), (2, 0, 3, 1))
    return tuple(tuple((z + k) % planes for z in range(planes)) for k in range(1, planes))


def fused_kernel(
    sizes,
    tok_hbm,
    ids_hbm,
    gate_hbm,
    win_hbm,
    wout_hbm,
    sin_hbm,
    sout_hbm,
    out_ref,
    tok,
    ids_in,
    gate_in,
    norm,
    xall,
    meta,
    win,
    wout,
    sin,
    sout,
    keys,
    gates,
    pick,
    gslot,
    rows,
    send,
    recv,
    ssend,
    srecv,
    scaled,
    own,
    other,
    psend,
    precv,
    osend,
    orecv,
    zsend,
    zrecv,
    fsend,
    frecv,
    isem,
    lsem,
    wssem,
    wrsem,
    xssem,
    xrsem,
    zssem,
    zrsem,
    rssem,
    rrsem,
    pssem,
    prsem,
    ssem,
    srsem,
    dssem,
    drsem,
    bssem,
    brsem,
    ossem,
    orsem,
    fssem,
    frsem,
):
    planes, chips, cores = sizes
    dp = chips * cores
    tok_rows, width = tok.shape
    picks = ids_in.shape[0]
    half = width // chips
    part = half // cores
    experts = win.shape[0]
    local = experts * cores
    slots, span = pick.shape[2:]
    own_rows = chips * tok_rows
    last = planes - 1
    head = min(HEAD, experts // 2)
    close = max(experts - 1, head + 1)

    z = lax.axis_index("expert")
    d = lax.axis_index("dp")
    c = d % cores
    x = d // cores
    oc = 1 - c
    ox = 1 - x
    partner = {"dp": x * cores + oc}
    across = {"dp": ox * cores + c}
    mesh_ids = pl.DeviceIdType.MESH

    def remote(src, dst, s_sem, r_sem, device):
        return pltpu.make_async_remote_copy(
            src_ref=src,
            dst_ref=dst,
            send_sem=s_sem,
            recv_sem=r_sem,
            device_id=device,
            device_id_type=mesh_ids,
        )

    def loop(first, end, body):
        def step(i, carry):
            body(i)
            return carry

        lax.fori_loop(first, end, step, 0)

    orders = plane_orders(planes)

    def at_step(k):
        found = 0
        for step, order in enumerate(orders):
            for place, p in enumerate(order):
                hit = jnp.logical_and(k == step, z == place)
                found = jnp.where(hit, p, found)
        return jnp.where(k == last, z, found)

    def mine_of(core):
        return pl.ds(core * experts, experts)

    def local_in():
        return pltpu.make_async_copy(
            win_hbm.at[mine_of(c)], win.at[:, start_of(c, part)], lsem.at[0]
        )

    def local_out():
        return pltpu.make_async_copy(
            wout_hbm.at[mine_of(c)], wout.at[:, :, start_of(c, part)], lsem.at[1]
        )

    def local_shared_in():
        return pltpu.make_async_copy(sin_hbm, sin.at[start_of(c, part)], lsem.at[2])

    def local_shared_out():
        return pltpu.make_async_copy(sout_hbm, sout.at[:, start_of(c, part)], lsem.at[3])

    def partner_in(group):
        first, count = ((0, head), (head, experts - head))[group]
        return remote(
            win_hbm.at[pl.ds(oc * experts + first, count)],
            win.at[pl.ds(first, count), start_of(c, part)],
            wssem.at[group],
            wrsem.at[group],
            partner,
        )

    def partner_out():
        return remote(
            wout_hbm.at[mine_of(oc)],
            wout.at[:, :, start_of(c, part)],
            wssem.at[2],
            wrsem.at[2],
            partner,
        )

    def partner_shared_in():
        return remote(sin_hbm, sin.at[start_of(c, part)], wssem.at[3], wrsem.at[3], partner)

    def partner_shared_out():
        return remote(
            sout_hbm, sout.at[:, start_of(c, part)], wssem.at[4], wrsem.at[4], partner
        )

    def block(p, b, kind):
        return meta.at[p, c * chips + b] if kind else xall.at[p, c, b]

    def token_swap(kind):
        src = meta.at[z, c * chips + x] if kind else norm.at[:, start_of(ox, half)]
        return remote(src, block(z, x, kind), xssem.at[kind], xrsem.at[kind], across)

    def both(p, kind):
        return meta.at[p, pl.ds(c * chips, chips)] if kind else xall.at[p, c]

    def to_plane(p, b, kind):
        ref = block(z, b, kind)
        return remote(ref, ref, zssem.at[kind], zrsem.at[z, kind], {"expert": p})

    def from_plane(p, kind):
        ref = both(p, kind)
        return remote(ref, ref, zssem.at[kind], zrsem.at[p, kind], {"expert": p})

    def send_tokens(k, b):
        for p in range(planes):

            @pl.when(z == orders[k][p])
            def _():
                for kind in (1, 0):
                    to_plane(p, b, kind).start()

    def relay_block(b, kind):
        ref = block(z, b, kind)
        return remote(ref, ref, rssem.at[kind], rrsem.at[z, kind], partner)

    def relay(p, kind):
        ref = both(p, kind)
        return remote(ref, ref, rssem.at[kind], rrsem.at[p, kind], partner)

    def tokens_sent(kind, count, s_sem):
        ref = meta.at[pl.ds(0, count), pl.ds(0, chips)] if kind else xall.at[pl.ds(0, count), 0]
        return remote(ref, ref, s_sem.at[kind], zrsem.at[0, kind], partner)

    def swap(k, e):
        return remote(send.at[k, e], recv.at[k, e], pssem.at[0], prsem.at[k, e], across)

    def shared_swap(b):
        return remote(ssend.at[b], srecv.at[b], ssem.at[0], srsem.at[b], across)

    def pair(k):
        return remote(psend.at[k], precv.at[k], dssem.at[0], drsem.at[k], partner)

    def own_pair(b):
        return remote(osend.at[b], orecv.at[b], bssem.at[0], brsem.at[b], partner)

    def give(k):
        return remote(
            zsend.at[k], zrecv.at[z], ossem.at[0], orsem.at[0], {"expert": at_step(k)}
        )

    def given():
        return remote(zsend, zrecv.at[pl.ds(0, last)], ossem.at[0], orsem.at[0], partner)

    def finish():
        return remote(fsend, frecv, fssem.at[0], frsem.at[0], across)

    barrier = pltpu.get_barrier_semaphore()
    peers = [{"expert": lax.rem(z + i, planes)} for i in range(1, planes)]
    for device in [across, partner] + peers:
        pl.semaphore_signal(barrier, inc=1, device_id=device, device_id_type=mesh_ids)
    read_tok = pltpu.make_async_copy(tok_hbm, tok, isem.at[0])
    read_ids = pltpu.make_async_copy(ids_hbm, ids_in, isem.at[1])
    read_gate = pltpu.make_async_copy(gate_hbm, gate_in, isem.at[2])
    read_tok.start()
    read_ids.start()
    read_gate.start()
    local_shared_in().start()
    local_in().start()
    local_shared_out().start()
    local_out().start()
    read_ids.wait()
    read_gate.wait()
    meta[z, c * chips + x, :picks] = ids_in[...].astype(jnp.float32)
    meta[z, c * chips + x, picks:] = gate_in[...]
    read_tok.wait()
    values = tok[...].astype(jnp.float32)
    center = values - jnp.mean(values, axis=-1, keepdims=True)
    spread = jnp.mean(center * center, axis=-1, keepdims=True)
    norm[...] = (center * lax.rsqrt(spread + 1e-06)).astype(jnp.bfloat16)
    xall[z, c, x] = norm[:, start_of(x, half)]

    pl.semaphore_wait(barrier, planes + 1)
    for kind in (1, 0):
        token_swap(kind).start()
    partner_shared_in().start()
    for kind in (1, 0):
        relay_block(x, kind).start()
    send_tokens(0, x)
    partner_in(0).start()

    def shared_first(b):
        pre = jnp.dot(xall[z, c, b], sin[...], preferred_element_type=jnp.float32)
        ssend[b] = pre.astype(jnp.bfloat16)

    local_shared_in().wait()
    partner_shared_in().wait_recv()
    shared_first(x)
    shared_swap(x).start()
    for kind in (1, 0):
        token_swap(kind).wait_recv()
        relay_block(ox, kind).start()
    send_tokens(0, ox)
    partner_in(1).start()
    partner_shared_out().start()
    partner_out().start()
    shared_first(ox)
    shared_swap(ox).start()

    before = jnp.where(
        lax.broadcasted_iota(jnp.int32, (tok_rows, tok_rows), 0)
        < lax.broadcasted_iota(jnp.int32, (tok_rows, tok_rows), 1),
        1.0,
        0.0,
    ).astype(jnp.bfloat16)

    def first_stage(k, turn, mine):
        p = z if mine else at_step(k)
        if not mine:
            for kind in (1, 0):
                from_plane(p, kind).wait_recv()
                relay(p, kind).start()
            for step in range(1, last):

                @pl.when(k == step - 1)
                def _():
                    for b in (x, ox):
                        send_tokens(step, b)

        relay(p, 1).wait_recv()

        ids = jnp.concatenate([meta[p, b, :picks] for b in range(dp)], axis=1)
        weights = jnp.concatenate([meta[p, b, picks:] for b in range(dp)], axis=1)
        chosen, gate = [], []
        for e in range(experts):
            match = ids == (z * local + c * experts + e).astype(jnp.float32)
            chosen.append(jnp.max(jnp.where(match, 1.0, 0.0), axis=0, keepdims=True))
            gate.append(jnp.sum(jnp.where(match, weights, 0.0), axis=0, keepdims=True))
        chosen = jnp.concatenate(chosen, axis=0)
        gates[...] = jnp.concatenate(gate, axis=0)
        for b in range(dp):
            lanes = slice(b * tok_rows, (b + 1) * tok_rows)
            named = chosen[:, lanes]
            earlier = jnp.dot(
                named.astype(jnp.bfloat16), before, preferred_element_type=jnp.float32
            )
            keys[:, lanes] = jnp.where(named > 0.5, earlier + float(b * CAP), -1.0).astype(
                jnp.int32
            )

        def choose(e):
            row = lax.broadcasted_iota(jnp.int32, (slots, span), 0)
            match = row == keys[pl.ds(e, 1), :]
            pick[turn, e] = jnp.where(match, 1.0, 0.0).astype(jnp.bfloat16)
            gate = jnp.sum(
                jnp.where(match, gates[pl.ds(e, 1), :], 0.0), axis=1, keepdims=True
            )
            gslot[turn, e] = jnp.broadcast_to(gate, gslot.shape[2:])

        loop(0, experts, choose)
        relay(p, 0).wait_recv()
        plane = xall[p].reshape(span, half)
        chosen_rows = jnp.dot(
            pick[turn].reshape(experts * slots, span), plane, preferred_element_type=jnp.float32
        )
        rows[...] = chosen_rows.astype(jnp.bfloat16).reshape(rows.shape)

        def project(e):
            pre = jnp.dot(rows[e], win[e], preferred_element_type=jnp.float32)
            send[k, e] = pre.astype(jnp.bfloat16)

        def project_and_send(e):
            project(e)
            swap(k, e).start()

        if mine:
            local_in().wait()
            partner_in(0).wait_recv()
            loop(0, head, project_and_send)
            partner_in(1).wait_recv()
            loop(head, experts, project)
        else:
            loop(0, experts, project_and_send)

    def second_stage(k, turn, first, end):
        def project(e):
            swap(k, e).wait_recv()
            total = send[k, e].astype(jnp.float32) + recv[k, e].astype(jnp.float32)
            h = jax.nn.gelu(total).astype(jnp.bfloat16)
            result = jnp.dot(h, wout[e], preferred_element_type=jnp.float32)
            scaled[e] = (result * gslot[turn, e][:, :1]).astype(jnp.bfloat16)

        loop(first, end, project)

    def combine(turn, first, end, lanes, count):
        return lax.dot_general(
            pick[turn, first:end, :, lanes].reshape((end - first) * slots, count),
            scaled[first:end].reshape((end - first) * slots, half),
            (((0,), (0,)), ((), ())),
            preferred_element_type=jnp.float32,
        )

    first_stage(last, 2, True)
    first_stage(0, 0, False)

    local_shared_out().wait()
    partner_shared_out().wait_recv()

    def shared_second(b):
        shared_swap(b).wait_recv()
        total = ssend[b].astype(jnp.float32) + srecv[b].astype(jnp.float32)
        h = jax.nn.gelu(total).astype(jnp.bfloat16)
        own[start_of(b, tok_rows), :] += jnp.dot(
            h, sout[...], preferred_element_type=jnp.float32
        )

    local_out().wait()
    partner_out().wait_recv()

    second_stage(last, 2, 0, head)
    own[...] = combine(2, 0, head, start_of(c, own_rows), own_rows)
    other[...] = combine(2, 0, head, start_of(oc, own_rows), own_rows)
    for b in range(chips):
        shared_second(b)

    def plane_step(k):
        turn = lax.rem(k, 2)

        @pl.when(k < last - 1)
        def _():
            first_stage(k + 1, lax.rem(k + 1, 2), False)

        @pl.when(k == last - 1)
        def _():
            loop(head, experts, lambda e: swap(last, e).start())

        second_stage(k, turn, 0, experts)
        psend[k] = combine(turn, 0, experts, start_of(oc, own_rows), own_rows).astype(
            jnp.bfloat16
        )
        pair(k).start()
        mine = combine(turn, 0, experts, start_of(c, own_rows), own_rows)
        pair(k).wait_recv()
        zsend[k] = (mine + precv[k].astype(jnp.float32)).astype(jnp.bfloat16)
        give(k).start()

    loop(0, last, plane_step)

    second_stage(last, 2, head, close)
    own[...] += combine(2, head, close, start_of(c, own_rows), own_rows)
    other[...] += combine(2, head, close, start_of(oc, own_rows), own_rows)
    second_stage(last, 2, close, experts)
    for b in (ox, x):
        lanes = start_of(oc * chips + b, tok_rows)
        extra = combine(2, close, experts, lanes, tok_rows)
        osend[b] = (other[start_of(b, tok_rows), :] + extra).astype(jnp.bfloat16)
        own_pair(b).start()
    total = own[...] + combine(2, close, experts, start_of(c, own_rows), own_rows)
    given().wait_recv()
    for r in range(1, planes):
        total = total + zrecv[lax.rem(z + r, planes)].astype(jnp.float32)
    own[...] = total
    mine = start_of(x, half)
    theirs = start_of(ox, half)
    own_pair(ox).wait_recv()
    fsend[...] = (own[start_of(ox, tok_rows), :] + orecv[ox].astype(jnp.float32)).astype(
        jnp.bfloat16
    )
    finish().start()
    own_pair(x).wait_recv()
    out_ref[:, mine] = (
        tok[:, mine].astype(jnp.float32)
        + own[start_of(x, tok_rows), :]
        + orecv[x].astype(jnp.float32)
    ).astype(out_ref.dtype)

    for kind in (0, 1):
        token_swap(kind).wait_send()
        tokens_sent(kind, last, zssem).wait_send()
        tokens_sent(kind, planes, rssem).wait_send()
        partner_in(kind).wait_send()
    partner_shared_in().wait_send()
    partner_shared_out().wait_send()
    partner_out().wait_send()
    remote(send, recv, pssem.at[0], prsem.at[0, 0], across).wait_send()
    remote(ssend, srecv, ssem.at[0], srsem.at[0], across).wait_send()
    remote(osend, orecv, bssem.at[0], brsem.at[0], partner).wait_send()
    remote(psend, precv, dssem.at[0], drsem.at[0], partner).wait_send()
    given().wait_send()

    finish().wait()
    out_ref[:, theirs] = (
        tok[:, theirs].astype(jnp.float32) + frecv[...].astype(jnp.float32)
    ).astype(out_ref.dtype)


def fused(tokens, expert_ids, gate_weights, expert_in, expert_out, shared_in, shared_out):
    tok_rows, width = tokens.shape
    picks = expert_ids.shape[1]
    planes, dp = lax.axis_size("expert"), lax.axis_size("dp")
    cores, chips = 2, dp // 2
    local, part, hidden = expert_in.shape
    experts = local // cores
    half = width // chips
    slots, span = dp * CAP, dp * tok_rows
    own_rows = chips * tok_rows
    bf16, f32 = jnp.bfloat16, jnp.float32
    vmem, dma = pltpu.VMEM, pltpu.SemaphoreType.DMA
    scratch = [
        vmem((tok_rows, width), bf16),
        vmem((picks, tok_rows), jnp.int32),
        vmem((picks, tok_rows), f32),
        vmem((tok_rows, width), bf16),
        vmem((planes, cores, chips, tok_rows, half), bf16),
        vmem((planes, dp, 2 * picks, tok_rows), f32),
        vmem((experts, half, hidden), bf16),
        vmem((experts, hidden, half), bf16),
        vmem((half, hidden), bf16),
        vmem((hidden, half), bf16),
        vmem((experts, span), jnp.int32),
        vmem((experts, span), f32),
        vmem((3, experts, slots, span), bf16),
        vmem((3, experts, slots, 128), f32),
        vmem((experts, slots, half), bf16),
        vmem((planes, experts, slots, hidden), bf16),
        vmem((planes, experts, slots, hidden), bf16),
        vmem((chips, tok_rows, hidden), bf16),
        vmem((chips, tok_rows, hidden), bf16),
        vmem((experts, slots, half), bf16),
        vmem((own_rows, half), f32),
        vmem((own_rows, half), f32),
        vmem((planes - 1, own_rows, half), bf16),
        vmem((planes - 1, own_rows, half), bf16),
        vmem((chips, tok_rows, half), bf16),
        vmem((chips, tok_rows, half), bf16),
        vmem((planes - 1, own_rows, half), bf16),
        vmem((planes, own_rows, half), bf16),
        vmem((tok_rows, half), bf16),
        vmem((tok_rows, half), bf16),
        dma((3,)),
        dma((4,)),
    ]
    pairs = [
        ((5,), (5,)),
        ((2,), (2,)),
        ((2,), (planes, 2)),
        ((2,), (planes, 2)),
        ((1,), (planes, experts)),
        ((1,), (chips,)),
        ((1,), (planes - 1,)),
        ((1,), (chips,)),
        ((1,), (1,)),
        ((1,), (1,)),
    ]
    for sent, received in pairs:
        scratch += [dma(sent), dma(received)]
    apart = pl.BlockSpec(memory_space=pl.ANY)
    return pl.pallas_call(
        functools.partial(fused_kernel, (planes, chips, cores)),
        in_specs=[apart] * 7,
        out_specs=pl.BlockSpec(memory_space=pltpu.VMEM),
        out_shape=jax.ShapeDtypeStruct((tok_rows, width), tokens.dtype),
        scratch_shapes=scratch,
        compiler_params=pltpu.CompilerParams(
            collective_id=0, has_side_effects=True, vmem_limit_bytes=56098816
        ),
    )(tokens, expert_ids.T, gate_weights.T, expert_in, expert_out, shared_in, shared_out)


def fits(mesh, args):
    planes, dp = mesh.shape["expert"], mesh.shape["dp"]
    tokens, expert_in = args[0], args[3]
    return (
        dp == 4
        and 1 < planes <= 8
        and expert_in.shape[0] // (mesh.shape["sweep"] * planes) % 2 == 0
        and expert_in.shape[0] // (mesh.shape["sweep"] * planes) <= 16
        and tokens.shape[0] // (mesh.shape["sweep"] * planes * dp) == 128
    )


def solution(mesh):
    placed = (
        P(("sweep", "expert", "dp"), None),
        P(("sweep", "expert", "dp"), None),
        P(("sweep", "expert", "dp"), None),
        P(("sweep", "expert"), "dp", None),
        P(("sweep", "expert"), None, "dp"),
        P(("sweep", "dp"), None),
        P("sweep", "dp"),
    )

    def run(*args):
        return jax.shard_map(
            fused if fits(mesh, args) else per_device,
            mesh=mesh,
            in_specs=placed,
            out_specs=P(("sweep", "expert", "dp"), None),
            check_vma=False,
        )(*args)

    return run
```

```python
import functools

import jax
import jax.numpy as jnp
from jax import lax
from jax.experimental import pallas as pl
from jax.experimental.pallas import tpu as pltpu
from jax.sharding import PartitionSpec as P

CAP = 20
GROUP = 4


def layer_norm(tokens):
    values = tokens.astype(jnp.float32)
    center = values - jnp.mean(values, axis=-1, keepdims=True)
    spread = jnp.mean(center * center, axis=-1, keepdims=True)
    return (center * lax.rsqrt(spread + 1e-06)).astype(jnp.bfloat16)


def first_kernel(runs, run_tokens, x_ref, key_ref, w_ref, out_ref, rows_ref):
    slots = out_ref.shape[3]
    for j in range(runs):
        span = slice(j * run_tokens, (j + 1) * run_tokens)
        row = lax.broadcasted_iota(jnp.int32, (slots, run_tokens), 0)
        pick = jnp.where(row == key_ref[0, :, span], 1.0, 0.0).astype(jnp.bfloat16)
        rows_ref[j * slots : (j + 1) * slots, :] = jnp.dot(
            pick, x_ref[span, :], preferred_element_type=jnp.float32
        ).astype(jnp.bfloat16)
    pre = jnp.dot(rows_ref[...], w_ref[0], preferred_element_type=jnp.float32)
    for j in range(runs):
        out_ref[j, 0, 0] = pre[j * slots : (j + 1) * slots].astype(jnp.bfloat16)


def first_projection(x, keys, weight, first, count, runs, run_tokens, slots):
    width, hidden = weight.shape[1:]
    chunk = runs * run_tokens
    chunks = x.shape[0] // chunk
    total = count * chunks * runs * slots
    return pl.pallas_call(
        functools.partial(first_kernel, runs, run_tokens),
        grid=(count, chunks),
        in_specs=[
            pl.BlockSpec((chunk, width), lambda e, c: (c, 0)),
            pl.BlockSpec((1, 1, chunk), lambda e, c: (e + first, 0, c)),
            pl.BlockSpec((1, width, hidden), lambda e, c: (e + first, 0, 0)),
        ],
        out_specs=pl.BlockSpec((runs, 1, 1, slots, hidden), lambda e, c: (0, e, c, 0, 0)),
        out_shape=jax.ShapeDtypeStruct((runs, count, chunks, slots, hidden), jnp.bfloat16),
        scratch_shapes=[pltpu.VMEM((runs * slots, width), jnp.bfloat16)],
        cost_estimate=pl.CostEstimate(
            flops=2 * total * width * (hidden + run_tokens),
            bytes_accessed=2 * (count * width * hidden + total * hidden + x.size),
            transcendentals=0,
        ),
    )(x, keys, weight)


def second_kernel(runs, run_tokens, h_ref, key_ref, gate_ref, w_ref, *refs):
    carry_ref, (out_ref, total_ref) = refs[0] if len(refs) == 3 else None, refs[-2:]
    expert = pl.program_id(1)
    slots = h_ref.shape[3]

    @pl.when(expert == 0)
    def _():
        total_ref[...] = jnp.zeros_like(total_ref) if carry_ref is None else carry_ref[...]

    h = jnp.concatenate([h_ref[j, 0, 0] for j in range(runs)], axis=0)
    result = jnp.dot(h, w_ref[0], preferred_element_type=jnp.float32)
    for j in range(runs):
        span = slice(j * run_tokens, (j + 1) * run_tokens)
        row = lax.broadcasted_iota(jnp.int32, (slots, run_tokens), 0)
        match = row == key_ref[0, :, span]
        gate = jnp.sum(jnp.where(match, gate_ref[0, :, span], 0.0), axis=1, keepdims=True)
        scaled = (result[j * slots : (j + 1) * slots] * gate).astype(jnp.bfloat16)
        total_ref[span, :] += lax.dot_general(
            jnp.where(match, 1.0, 0.0).astype(jnp.bfloat16),
            scaled,
            (((0,), (0,)), ((), ())),
            preferred_element_type=jnp.float32,
        )

    @pl.when(expert == pl.num_programs(1) - 1)
    def _():
        out_ref[...] = total_ref[...].astype(out_ref.dtype)


def second_projection(hidden, keys, gates, weight, carry, kind, first, runs, run_tokens):
    _, count, chunks, slots, depth = hidden.shape
    width = weight.shape[2]
    chunk = runs * run_tokens
    total = count * chunks * runs * slots
    carries = [] if carry is None else [carry]
    return pl.pallas_call(
        functools.partial(second_kernel, runs, run_tokens),
        grid=(chunks, count),
        in_specs=[
            pl.BlockSpec((runs, 1, 1, slots, depth), lambda c, e: (0, e, c, 0, 0)),
            pl.BlockSpec((1, 1, chunk), lambda c, e: (e + first, 0, c)),
            pl.BlockSpec((1, 1, chunk), lambda c, e: (e + first, 0, c)),
            pl.BlockSpec((1, depth, width), lambda c, e: (e + first, 0, 0)),
        ]
        + [pl.BlockSpec((chunk, width), lambda c, e: (c, 0)) for _ in carries],
        out_specs=pl.BlockSpec((chunk, width), lambda c, e: (c, 0)),
        out_shape=jax.ShapeDtypeStruct((chunks * chunk, width), kind),
        scratch_shapes=[pltpu.VMEM((chunk, width), jnp.float32)],
        cost_estimate=pl.CostEstimate(
            flops=2 * total * width * (depth + 3 * run_tokens),
            bytes_accessed=2 * (count * depth * width + total * depth) + 4 * chunks * chunk * width,
            transcendentals=0,
        ),
    )(hidden, keys, gates, weight, *carries)


def per_device(tokens, expert_ids, gate_weights, expert_in, expert_out, shared_in, shared_out):
    row_count, model_width = tokens.shape
    pick_count = expert_ids.shape[1]
    local_count = expert_in.shape[0]
    runs = lax.axis_size("dp")
    block_count = runs * lax.axis_size("expert")
    run_tokens = GROUP * row_count
    slots = GROUP * CAP
    halves = 2 if local_count % 2 == 0 else 1

    normed = layer_norm(tokens)
    full_shared_in = lax.all_gather(shared_in, "dp", axis=0, tiled=True)
    full_shared_out = lax.all_gather(shared_out, "dp", axis=1, tiled=True)

    named = jnp.concatenate([expert_ids.astype(jnp.float32), gate_weights], axis=1).T
    named = lax.all_gather(named, ("expert", "dp"), axis=0, tiled=False)
    ids, gates = named[:, :pick_count], named[:, pick_count:]
    columns = lax.all_to_all(normed, "dp", split_axis=1, concat_axis=0, tiled=True)
    columns, full_shared_in, full_shared_out = lax.optimization_barrier(
        (columns, full_shared_in, full_shared_out)
    )
    x = lax.all_gather(columns, "expert", axis=0, tiled=True)

    owned = lax.axis_index("expert") * local_count + jnp.arange(local_count, dtype=jnp.int32)
    matches = ids[:, :, None, :] == owned.astype(jnp.float32)[:, None]
    chosen = jnp.any(matches, axis=1)
    gate_of = jnp.sum(jnp.where(matches, gates[:, :, None, :], 0.0), axis=1)
    order = jnp.arange(row_count, dtype=jnp.int32)
    before = (order[:, None] < order[None, :]).astype(jnp.bfloat16)
    earlier = jnp.einsum(
        "bej,ji->bei", chosen.astype(jnp.bfloat16), before, preferred_element_type=jnp.float32
    ).astype(jnp.int32)
    base = jnp.arange(block_count, dtype=jnp.int32) % GROUP * CAP
    keys = jnp.where(chosen, earlier + base[:, None, None], -1)

    def by_expert(table):
        return table.transpose(1, 0, 2).reshape(local_count, 1, block_count * row_count)

    keys, gate_of = by_expert(keys), by_expert(gate_of)

    count = local_count // halves
    parts = []
    for half in range(halves):
        pre = first_projection(
            x, keys, expert_in, half * count, count, runs, run_tokens, slots
        )
        parts.append(lax.psum_scatter(pre, "dp", scatter_dimension=0, tiled=True))

    hidden = []
    for pre in parts:
        act = jax.nn.gelu(pre.astype(jnp.float32)).astype(jnp.bfloat16)
        hidden.append(lax.all_gather(act, "dp", axis=0, tiled=True))

    shared_pre = jnp.dot(normed, full_shared_in, preferred_element_type=jnp.float32)
    shared_hidden = jax.nn.gelu(shared_pre).astype(jnp.bfloat16)
    shared_result = jnp.dot(shared_hidden, full_shared_out, preferred_element_type=jnp.float32)

    routed = None
    for half, h in enumerate(hidden):
        kind = jnp.bfloat16 if half == halves - 1 else jnp.float32
        routed = second_projection(
            h, keys, gate_of, expert_out, routed, kind, half * count, runs, run_tokens
        )
    width = routed.shape[1]
    pieces = lax.all_to_all(
        routed.reshape(block_count, row_count, width),
        ("expert", "dp"),
        split_axis=0,
        concat_axis=0,
        tiled=True,
    ).reshape(-1, runs, row_count, width)
    own = jnp.sum(pieces.astype(jnp.float32), axis=0).transpose(1, 0, 2)
    own = own.reshape(row_count, model_width)
    return (tokens.astype(jnp.float32) + shared_result + own).astype(jnp.bfloat16)


def start_of(index, size):
    return pl.ds(pl.multiple_of(index * size, size), size)


HEAD = 3


def plane_orders(planes):
    if planes == 4:
        return ((1, 2, 1, 2), (3, 3, 0, 0), (2, 0, 3, 1))
    return tuple(tuple((z + k) % planes for z in range(planes)) for k in range(1, planes))


def fused_kernel(
    sizes,
    tok_hbm,
    ids_hbm,
    gate_hbm,
    win_hbm,
    wout_hbm,
    sin_hbm,
    sout_hbm,
    out_ref,
    tok,
    ids_in,
    gate_in,
    norm,
    xall,
    meta,
    win,
    wout,
    sin,
    sout,
    keys,
    gates,
    pick,
    gslot,
    rows,
    send,
    recv,
    ssend,
    srecv,
    scaled,
    own,
    other,
    psend,
    precv,
    osend,
    orecv,
    zsend,
    zrecv,
    fsend,
    frecv,
    isem,
    lsem,
    wssem,
    wrsem,
    xssem,
    xrsem,
    zssem,
    zrsem,
    rssem,
    rrsem,
    pssem,
    prsem,
    ssem,
    srsem,
    dssem,
    drsem,
    bssem,
    brsem,
    ossem,
    orsem,
    fssem,
    frsem,
):
    planes, chips, cores = sizes
    dp = chips * cores
    tok_rows, width = tok.shape
    picks = ids_in.shape[0]
    half = width // chips
    part = half // cores
    experts = win.shape[0]
    local = experts * cores
    slots, span = pick.shape[2:]
    own_rows = chips * tok_rows
    last = planes - 1
    head = min(HEAD, experts // 2)
    close = max(experts - 1, head + 1)

    z = lax.axis_index("expert")
    d = lax.axis_index("dp")
    c = d % cores
    x = d // cores
    oc = 1 - c
    ox = 1 - x
    partner = {"dp": x * cores + oc}
    across = {"dp": ox * cores + c}
    mesh_ids = pl.DeviceIdType.MESH

    def remote(src, dst, s_sem, r_sem, device):
        return pltpu.make_async_remote_copy(
            src_ref=src,
            dst_ref=dst,
            send_sem=s_sem,
            recv_sem=r_sem,
            device_id=device,
            device_id_type=mesh_ids,
        )

    def loop(first, end, body):
        def step(i, carry):
            body(i)
            return carry

        lax.fori_loop(first, end, step, 0)

    orders = plane_orders(planes)

    def at_step(k):
        found = 0
        for step, order in enumerate(orders):
            for place, p in enumerate(order):
                hit = jnp.logical_and(k == step, z == place)
                found = jnp.where(hit, p, found)
        return jnp.where(k == last, z, found)

    def mine_of(core):
        return pl.ds(core * experts, experts)

    def local_in():
        return pltpu.make_async_copy(
            win_hbm.at[mine_of(c)], win.at[:, start_of(c, part)], lsem.at[0]
        )

    def local_out():
        return pltpu.make_async_copy(
            wout_hbm.at[mine_of(c)], wout.at[:, :, start_of(c, part)], lsem.at[1]
        )

    def local_shared_in():
        return pltpu.make_async_copy(sin_hbm, sin.at[start_of(c, part)], lsem.at[2])

    def local_shared_out():
        return pltpu.make_async_copy(sout_hbm, sout.at[:, start_of(c, part)], lsem.at[3])

    def partner_in(group):
        first, count = ((0, head), (head, experts - head))[group]
        return remote(
            win_hbm.at[pl.ds(oc * experts + first, count)],
            win.at[pl.ds(first, count), start_of(c, part)],
            wssem.at[group],
            wrsem.at[group],
            partner,
        )

    def partner_out():
        return remote(
            wout_hbm.at[mine_of(oc)],
            wout.at[:, :, start_of(c, part)],
            wssem.at[2],
            wrsem.at[2],
            partner,
        )

    def partner_shared_in():
        return remote(sin_hbm, sin.at[start_of(c, part)], wssem.at[3], wrsem.at[3], partner)

    def partner_shared_out():
        return remote(
            sout_hbm, sout.at[:, start_of(c, part)], wssem.at[4], wrsem.at[4], partner
        )

    def block(p, b, kind):
        return meta.at[p, c * chips + b] if kind else xall.at[p, c, b]

    def token_swap(kind):
        src = meta.at[z, c * chips + x] if kind else norm.at[:, start_of(ox, half)]
        return remote(src, block(z, x, kind), xssem.at[kind], xrsem.at[kind], across)

    def both(p, kind):
        return meta.at[p, pl.ds(c * chips, chips)] if kind else xall.at[p, c]

    def to_plane(p, b, kind):
        ref = block(z, b, kind)
        return remote(ref, ref, zssem.at[kind], zrsem.at[z, kind], {"expert": p})

    def from_plane(p, kind):
        ref = both(p, kind)
        return remote(ref, ref, zssem.at[kind], zrsem.at[p, kind], {"expert": p})

    def send_tokens(k, b):
        for p in range(planes):

            @pl.when(z == orders[k][p])
            def _():
                for kind in (1, 0):
                    to_plane(p, b, kind).start()

    def relay_block(b, kind):
        ref = block(z, b, kind)
        return remote(ref, ref, rssem.at[kind], rrsem.at[z, kind], partner)

    def relay(p, kind):
        ref = both(p, kind)
        return remote(ref, ref, rssem.at[kind], rrsem.at[p, kind], partner)

    def tokens_sent(kind, count, s_sem):
        ref = meta.at[pl.ds(0, count), pl.ds(0, chips)] if kind else xall.at[pl.ds(0, count), 0]
        return remote(ref, ref, s_sem.at[kind], zrsem.at[0, kind], partner)

    def swap(k, e):
        return remote(send.at[k, e], recv.at[k, e], pssem.at[0], prsem.at[k, e], across)

    def shared_swap(b):
        return remote(ssend.at[b], srecv.at[b], ssem.at[0], srsem.at[b], across)

    def pair(k):
        return remote(psend.at[k], precv.at[k], dssem.at[0], drsem.at[k], partner)

    def own_pair(b):
        return remote(osend.at[b], orecv.at[b], bssem.at[0], brsem.at[b], partner)

    def give(k):
        return remote(
            zsend.at[k], zrecv.at[z], ossem.at[0], orsem.at[0], {"expert": at_step(k)}
        )

    def given():
        return remote(zsend, zrecv.at[pl.ds(0, last)], ossem.at[0], orsem.at[0], partner)

    def finish():
        return remote(fsend, frecv, fssem.at[0], frsem.at[0], across)

    barrier = pltpu.get_barrier_semaphore()
    peers = [{"expert": lax.rem(z + i, planes)} for i in range(1, planes)]
    for device in [across, partner] + peers:
        pl.semaphore_signal(barrier, inc=1, device_id=device, device_id_type=mesh_ids)
    read_tok = pltpu.make_async_copy(tok_hbm, tok, isem.at[0])
    read_ids = pltpu.make_async_copy(ids_hbm, ids_in, isem.at[1])
    read_gate = pltpu.make_async_copy(gate_hbm, gate_in, isem.at[2])
    read_tok.start()
    read_ids.start()
    read_gate.start()
    local_shared_in().start()
    local_in().start()
    local_shared_out().start()
    local_out().start()
    read_ids.wait()
    read_gate.wait()
    meta[z, c * chips + x, :picks] = ids_in[...].astype(jnp.float32)
    meta[z, c * chips + x, picks:] = gate_in[...]
    read_tok.wait()
    values = tok[...].astype(jnp.float32)
    center = values - jnp.mean(values, axis=-1, keepdims=True)
    spread = jnp.mean(center * center, axis=-1, keepdims=True)
    norm[...] = (center * lax.rsqrt(spread + 1e-06)).astype(jnp.bfloat16)
    xall[z, c, x] = norm[:, start_of(x, half)]

    pl.semaphore_wait(barrier, planes + 1)
    for kind in (1, 0):
        token_swap(kind).start()
    partner_shared_in().start()
    for kind in (1, 0):
        relay_block(x, kind).start()
    partner_in(0).start()
    send_tokens(0, x)

    def shared_first(b):
        pre = jnp.dot(xall[z, c, b], sin[...], preferred_element_type=jnp.float32)
        ssend[b] = pre.astype(jnp.bfloat16)

    local_shared_in().wait()
    partner_shared_in().wait_recv()
    shared_first(x)
    shared_swap(x).start()
    for kind in (1, 0):
        token_swap(kind).wait_recv()
        relay_block(ox, kind).start()
    send_tokens(0, ox)
    partner_in(1).start()
    partner_shared_out().start()
    partner_out().start()
    shared_first(ox)
    shared_swap(ox).start()

    before = jnp.where(
        lax.broadcasted_iota(jnp.int32, (tok_rows, tok_rows), 0)
        < lax.broadcasted_iota(jnp.int32, (tok_rows, tok_rows), 1),
        1.0,
        0.0,
    ).astype(jnp.bfloat16)

    def first_stage(k, turn, mine):
        p = z if mine else at_step(k)
        if not mine:
            for kind in (1, 0):
                from_plane(p, kind).wait_recv()
                relay(p, kind).start()
            for step in range(1, last):

                @pl.when(k == step - 1)
                def _():
                    for b in (x, ox):
                        send_tokens(step, b)

        relay(p, 1).wait_recv()

        ids = jnp.concatenate([meta[p, b, :picks] for b in range(dp)], axis=1)
        weights = jnp.concatenate([meta[p, b, picks:] for b in range(dp)], axis=1)
        chosen, gate = [], []
        for e in range(experts):
            match = ids == (z * local + c * experts + e).astype(jnp.float32)
            chosen.append(jnp.max(jnp.where(match, 1.0, 0.0), axis=0, keepdims=True))
            gate.append(jnp.sum(jnp.where(match, weights, 0.0), axis=0, keepdims=True))
        chosen = jnp.concatenate(chosen, axis=0)
        gates[...] = jnp.concatenate(gate, axis=0)
        for b in range(dp):
            lanes = slice(b * tok_rows, (b + 1) * tok_rows)
            named = chosen[:, lanes]
            earlier = jnp.dot(
                named.astype(jnp.bfloat16), before, preferred_element_type=jnp.float32
            )
            keys[:, lanes] = jnp.where(named > 0.5, earlier + float(b * CAP), -1.0).astype(
                jnp.int32
            )

        def choose(e):
            row = lax.broadcasted_iota(jnp.int32, (slots, span), 0)
            match = row == keys[pl.ds(e, 1), :]
            pick[turn, e] = jnp.where(match, 1.0, 0.0).astype(jnp.bfloat16)
            gate = jnp.sum(
                jnp.where(match, gates[pl.ds(e, 1), :], 0.0), axis=1, keepdims=True
            )
            gslot[turn, e] = jnp.broadcast_to(gate, gslot.shape[2:])

        loop(0, experts, choose)
        relay(p, 0).wait_recv()
        plane = xall[p].reshape(span, half)
        chosen_rows = jnp.dot(
            pick[turn].reshape(experts * slots, span), plane, preferred_element_type=jnp.float32
        )
        rows[...] = chosen_rows.astype(jnp.bfloat16).reshape(rows.shape)

        def project(e):
            pre = jnp.dot(rows[e], win[e], preferred_element_type=jnp.float32)
            send[k, e] = pre.astype(jnp.bfloat16)

        def project_and_send(e):
            project(e)
            swap(k, e).start()

        if mine:
            local_in().wait()
            partner_in(0).wait_recv()
            loop(0, head, project_and_send)
            partner_in(1).wait_recv()
            loop(head, experts, project)
        else:
            loop(0, experts, project_and_send)

    def second_stage(k, turn, first, end):
        def project(e):
            swap(k, e).wait_recv()
            total = send[k, e].astype(jnp.float32) + recv[k, e].astype(jnp.float32)
            h = jax.nn.gelu(total).astype(jnp.bfloat16)
            result = jnp.dot(h, wout[e], preferred_element_type=jnp.float32)
            scaled[e] = (result * gslot[turn, e][:, :1]).astype(jnp.bfloat16)

        loop(first, end, project)

    def combine(turn, first, end, lanes, count):
        return lax.dot_general(
            pick[turn, first:end, :, lanes].reshape((end - first) * slots, count),
            scaled[first:end].reshape((end - first) * slots, half),
            (((0,), (0,)), ((), ())),
            preferred_element_type=jnp.float32,
        )

    first_stage(last, 2, True)
    first_stage(0, 0, False)

    local_shared_out().wait()
    partner_shared_out().wait_recv()

    def shared_second(b):
        shared_swap(b).wait_recv()
        total = ssend[b].astype(jnp.float32) + srecv[b].astype(jnp.float32)
        h = jax.nn.gelu(total).astype(jnp.bfloat16)
        own[start_of(b, tok_rows), :] += jnp.dot(
            h, sout[...], preferred_element_type=jnp.float32
        )

    local_out().wait()
    partner_out().wait_recv()

    second_stage(last, 2, 0, head)
    own[...] = combine(2, 0, head, start_of(c, own_rows), own_rows)
    other[...] = combine(2, 0, head, start_of(oc, own_rows), own_rows)
    for b in range(chips):
        shared_second(b)

    def plane_step(k):
        turn = lax.rem(k, 2)

        @pl.when(k < last - 1)
        def _():
            first_stage(k + 1, lax.rem(k + 1, 2), False)

        @pl.when(k == last - 1)
        def _():
            loop(head, experts, lambda e: swap(last, e).start())

        second_stage(k, turn, 0, experts)
        psend[k] = combine(turn, 0, experts, start_of(oc, own_rows), own_rows).astype(
            jnp.bfloat16
        )
        pair(k).start()
        mine = combine(turn, 0, experts, start_of(c, own_rows), own_rows)
        pair(k).wait_recv()
        zsend[k] = (mine + precv[k].astype(jnp.float32)).astype(jnp.bfloat16)
        give(k).start()

    loop(0, last, plane_step)

    second_stage(last, 2, head, close)
    own[...] += combine(2, head, close, start_of(c, own_rows), own_rows)
    other[...] += combine(2, head, close, start_of(oc, own_rows), own_rows)
    second_stage(last, 2, close, experts)
    for b in (ox, x):
        lanes = start_of(oc * chips + b, tok_rows)
        extra = combine(2, close, experts, lanes, tok_rows)
        osend[b] = (other[start_of(b, tok_rows), :] + extra).astype(jnp.bfloat16)
        own_pair(b).start()
    total = own[...] + combine(2, close, experts, start_of(c, own_rows), own_rows)
    given().wait_recv()
    for r in range(1, planes):
        total = total + zrecv[lax.rem(z + r, planes)].astype(jnp.float32)
    own[...] = total
    mine = start_of(x, half)
    theirs = start_of(ox, half)
    own_pair(ox).wait_recv()
    fsend[...] = (own[start_of(ox, tok_rows), :] + orecv[ox].astype(jnp.float32)).astype(
        jnp.bfloat16
    )
    finish().start()
    own_pair(x).wait_recv()
    out_ref[:, mine] = (
        tok[:, mine].astype(jnp.float32)
        + own[start_of(x, tok_rows), :]
        + orecv[x].astype(jnp.float32)
    ).astype(out_ref.dtype)

    for kind in (0, 1):
        token_swap(kind).wait_send()
        tokens_sent(kind, last, zssem).wait_send()
        tokens_sent(kind, planes, rssem).wait_send()
        partner_in(kind).wait_send()
    partner_shared_in().wait_send()
    partner_shared_out().wait_send()
    partner_out().wait_send()
    remote(send, recv, pssem.at[0], prsem.at[0, 0], across).wait_send()
    remote(ssend, srecv, ssem.at[0], srsem.at[0], across).wait_send()
    remote(osend, orecv, bssem.at[0], brsem.at[0], partner).wait_send()
    remote(psend, precv, dssem.at[0], drsem.at[0], partner).wait_send()
    given().wait_send()

    finish().wait()
    out_ref[:, theirs] = (
        tok[:, theirs].astype(jnp.float32) + frecv[...].astype(jnp.float32)
    ).astype(out_ref.dtype)


def fused(tokens, expert_ids, gate_weights, expert_in, expert_out, shared_in, shared_out):
    tok_rows, width = tokens.shape
    picks = expert_ids.shape[1]
    planes, dp = lax.axis_size("expert"), lax.axis_size("dp")
    cores, chips = 2, dp // 2
    local, part, hidden = expert_in.shape
    experts = local // cores
    half = width // chips
    slots, span = dp * CAP, dp * tok_rows
    own_rows = chips * tok_rows
    bf16, f32 = jnp.bfloat16, jnp.float32
    vmem, dma = pltpu.VMEM, pltpu.SemaphoreType.DMA
    scratch = [
        vmem((tok_rows, width), bf16),
        vmem((picks, tok_rows), jnp.int32),
        vmem((picks, tok_rows), f32),
        vmem((tok_rows, width), bf16),
        vmem((planes, cores, chips, tok_rows, half), bf16),
        vmem((planes, dp, 2 * picks, tok_rows), f32),
        vmem((experts, half, hidden), bf16),
        vmem((experts, hidden, half), bf16),
        vmem((half, hidden), bf16),
        vmem((hidden, half), bf16),
        vmem((experts, span), jnp.int32),
        vmem((experts, span), f32),
        vmem((3, experts, slots, span), bf16),
        vmem((3, experts, slots, 128), f32),
        vmem((experts, slots, half), bf16),
        vmem((planes, experts, slots, hidden), bf16),
        vmem((planes, experts, slots, hidden), bf16),
        vmem((chips, tok_rows, hidden), bf16),
        vmem((chips, tok_rows, hidden), bf16),
        vmem((experts, slots, half), bf16),
        vmem((own_rows, half), f32),
        vmem((own_rows, half), f32),
        vmem((planes - 1, own_rows, half), bf16),
        vmem((planes - 1, own_rows, half), bf16),
        vmem((chips, tok_rows, half), bf16),
        vmem((chips, tok_rows, half), bf16),
        vmem((planes - 1, own_rows, half), bf16),
        vmem((planes, own_rows, half), bf16),
        vmem((tok_rows, half), bf16),
        vmem((tok_rows, half), bf16),
        dma((3,)),
        dma((4,)),
    ]
    pairs = [
        ((5,), (5,)),
        ((2,), (2,)),
        ((2,), (planes, 2)),
        ((2,), (planes, 2)),
        ((1,), (planes, experts)),
        ((1,), (chips,)),
        ((1,), (planes - 1,)),
        ((1,), (chips,)),
        ((1,), (1,)),
        ((1,), (1,)),
    ]
    for sent, received in pairs:
        scratch += [dma(sent), dma(received)]
    given = (tokens, expert_ids.T, gate_weights.T, expert_in, expert_out, shared_in, shared_out)
    given = [pltpu.with_memory_space_constraint(a, pltpu.HBM) for a in given]
    apart = pl.BlockSpec(memory_space=pl.ANY)
    return pl.pallas_call(
        functools.partial(fused_kernel, (planes, chips, cores)),
        in_specs=[apart] * 7,
        out_specs=pl.BlockSpec(memory_space=pltpu.VMEM),
        out_shape=jax.ShapeDtypeStruct((tok_rows, width), tokens.dtype),
        scratch_shapes=scratch,
        compiler_params=pltpu.CompilerParams(
            collective_id=0, has_side_effects=True, vmem_limit_bytes=56098816
        ),
    )(*given)


def fits(mesh, args):
    planes, dp = mesh.shape["expert"], mesh.shape["dp"]
    tokens, expert_in = args[0], args[3]
    return (
        dp == 4
        and 1 < planes <= 8
        and expert_in.shape[0] // (mesh.shape["sweep"] * planes) % 2 == 0
        and expert_in.shape[0] // (mesh.shape["sweep"] * planes) <= 16
        and tokens.shape[0] // (mesh.shape["sweep"] * planes * dp) == 128
    )


def solution(mesh):
    placed = (
        P(("sweep", "expert", "dp"), None),
        P(("sweep", "expert", "dp"), None),
        P(("sweep", "expert", "dp"), None),
        P(("sweep", "expert"), "dp", None),
        P(("sweep", "expert"), None, "dp"),
        P(("sweep", "dp"), None),
        P("sweep", "dp"),
    )

    def run(*args):
        return jax.shard_map(
            fused if fits(mesh, args) else per_device,
            mesh=mesh,
            in_specs=placed,
            out_specs=P(("sweep", "expert", "dp"), None),
            check_vma=False,
        )(*args)

    return run
```

```python
import functools

import jax
import jax.numpy as jnp
from jax import lax
from jax.experimental import pallas as pl
from jax.experimental.pallas import tpu as pltpu
from jax.sharding import PartitionSpec as P

CAP = 20
GROUP = 4


def layer_norm(tokens):
    values = tokens.astype(jnp.float32)
    center = values - jnp.mean(values, axis=-1, keepdims=True)
    spread = jnp.mean(center * center, axis=-1, keepdims=True)
    return (center * lax.rsqrt(spread + 1e-06)).astype(jnp.bfloat16)


def first_kernel(runs, run_tokens, x_ref, key_ref, w_ref, out_ref, rows_ref):
    slots = out_ref.shape[3]
    for j in range(runs):
        span = slice(j * run_tokens, (j + 1) * run_tokens)
        row = lax.broadcasted_iota(jnp.int32, (slots, run_tokens), 0)
        pick = jnp.where(row == key_ref[0, :, span], 1.0, 0.0).astype(jnp.bfloat16)
        rows_ref[j * slots : (j + 1) * slots, :] = jnp.dot(
            pick, x_ref[span, :], preferred_element_type=jnp.float32
        ).astype(jnp.bfloat16)
    pre = jnp.dot(rows_ref[...], w_ref[0], preferred_element_type=jnp.float32)
    for j in range(runs):
        out_ref[j, 0, 0] = pre[j * slots : (j + 1) * slots].astype(jnp.bfloat16)


def first_projection(x, keys, weight, first, count, runs, run_tokens, slots):
    width, hidden = weight.shape[1:]
    chunk = runs * run_tokens
    chunks = x.shape[0] // chunk
    total = count * chunks * runs * slots
    return pl.pallas_call(
        functools.partial(first_kernel, runs, run_tokens),
        grid=(count, chunks),
        in_specs=[
            pl.BlockSpec((chunk, width), lambda e, c: (c, 0)),
            pl.BlockSpec((1, 1, chunk), lambda e, c: (e + first, 0, c)),
            pl.BlockSpec((1, width, hidden), lambda e, c: (e + first, 0, 0)),
        ],
        out_specs=pl.BlockSpec((runs, 1, 1, slots, hidden), lambda e, c: (0, e, c, 0, 0)),
        out_shape=jax.ShapeDtypeStruct((runs, count, chunks, slots, hidden), jnp.bfloat16),
        scratch_shapes=[pltpu.VMEM((runs * slots, width), jnp.bfloat16)],
        cost_estimate=pl.CostEstimate(
            flops=2 * total * width * (hidden + run_tokens),
            bytes_accessed=2 * (count * width * hidden + total * hidden + x.size),
            transcendentals=0,
        ),
    )(x, keys, weight)


def second_kernel(runs, run_tokens, h_ref, key_ref, gate_ref, w_ref, *refs):
    carry_ref, (out_ref, total_ref) = refs[0] if len(refs) == 3 else None, refs[-2:]
    expert = pl.program_id(1)
    slots = h_ref.shape[3]

    @pl.when(expert == 0)
    def _():
        total_ref[...] = jnp.zeros_like(total_ref) if carry_ref is None else carry_ref[...]

    h = jnp.concatenate([h_ref[j, 0, 0] for j in range(runs)], axis=0)
    result = jnp.dot(h, w_ref[0], preferred_element_type=jnp.float32)
    for j in range(runs):
        span = slice(j * run_tokens, (j + 1) * run_tokens)
        row = lax.broadcasted_iota(jnp.int32, (slots, run_tokens), 0)
        match = row == key_ref[0, :, span]
        gate = jnp.sum(jnp.where(match, gate_ref[0, :, span], 0.0), axis=1, keepdims=True)
        scaled = (result[j * slots : (j + 1) * slots] * gate).astype(jnp.bfloat16)
        total_ref[span, :] += lax.dot_general(
            jnp.where(match, 1.0, 0.0).astype(jnp.bfloat16),
            scaled,
            (((0,), (0,)), ((), ())),
            preferred_element_type=jnp.float32,
        )

    @pl.when(expert == pl.num_programs(1) - 1)
    def _():
        out_ref[...] = total_ref[...].astype(out_ref.dtype)


def second_projection(hidden, keys, gates, weight, carry, kind, first, runs, run_tokens):
    _, count, chunks, slots, depth = hidden.shape
    width = weight.shape[2]
    chunk = runs * run_tokens
    total = count * chunks * runs * slots
    carries = [] if carry is None else [carry]
    return pl.pallas_call(
        functools.partial(second_kernel, runs, run_tokens),
        grid=(chunks, count),
        in_specs=[
            pl.BlockSpec((runs, 1, 1, slots, depth), lambda c, e: (0, e, c, 0, 0)),
            pl.BlockSpec((1, 1, chunk), lambda c, e: (e + first, 0, c)),
            pl.BlockSpec((1, 1, chunk), lambda c, e: (e + first, 0, c)),
            pl.BlockSpec((1, depth, width), lambda c, e: (e + first, 0, 0)),
        ]
        + [pl.BlockSpec((chunk, width), lambda c, e: (c, 0)) for _ in carries],
        out_specs=pl.BlockSpec((chunk, width), lambda c, e: (c, 0)),
        out_shape=jax.ShapeDtypeStruct((chunks * chunk, width), kind),
        scratch_shapes=[pltpu.VMEM((chunk, width), jnp.float32)],
        cost_estimate=pl.CostEstimate(
            flops=2 * total * width * (depth + 3 * run_tokens),
            bytes_accessed=2 * (count * depth * width + total * depth) + 4 * chunks * chunk * width,
            transcendentals=0,
        ),
    )(hidden, keys, gates, weight, *carries)


def per_device(tokens, expert_ids, gate_weights, expert_in, expert_out, shared_in, shared_out):
    row_count, model_width = tokens.shape
    pick_count = expert_ids.shape[1]
    local_count = expert_in.shape[0]
    runs = lax.axis_size("dp")
    block_count = runs * lax.axis_size("expert")
    run_tokens = GROUP * row_count
    slots = GROUP * CAP
    halves = 2 if local_count % 2 == 0 else 1

    normed = layer_norm(tokens)
    full_shared_in = lax.all_gather(shared_in, "dp", axis=0, tiled=True)
    full_shared_out = lax.all_gather(shared_out, "dp", axis=1, tiled=True)

    named = jnp.concatenate([expert_ids.astype(jnp.float32), gate_weights], axis=1).T
    named = lax.all_gather(named, ("expert", "dp"), axis=0, tiled=False)
    ids, gates = named[:, :pick_count], named[:, pick_count:]
    columns = lax.all_to_all(normed, "dp", split_axis=1, concat_axis=0, tiled=True)
    columns, full_shared_in, full_shared_out = lax.optimization_barrier(
        (columns, full_shared_in, full_shared_out)
    )
    x = lax.all_gather(columns, "expert", axis=0, tiled=True)

    owned = lax.axis_index("expert") * local_count + jnp.arange(local_count, dtype=jnp.int32)
    matches = ids[:, :, None, :] == owned.astype(jnp.float32)[:, None]
    chosen = jnp.any(matches, axis=1)
    gate_of = jnp.sum(jnp.where(matches, gates[:, :, None, :], 0.0), axis=1)
    order = jnp.arange(row_count, dtype=jnp.int32)
    before = (order[:, None] < order[None, :]).astype(jnp.bfloat16)
    earlier = jnp.einsum(
        "bej,ji->bei", chosen.astype(jnp.bfloat16), before, preferred_element_type=jnp.float32
    ).astype(jnp.int32)
    base = jnp.arange(block_count, dtype=jnp.int32) % GROUP * CAP
    keys = jnp.where(chosen, earlier + base[:, None, None], -1)

    def by_expert(table):
        return table.transpose(1, 0, 2).reshape(local_count, 1, block_count * row_count)

    keys, gate_of = by_expert(keys), by_expert(gate_of)

    count = local_count // halves
    parts = []
    for half in range(halves):
        pre = first_projection(
            x, keys, expert_in, half * count, count, runs, run_tokens, slots
        )
        parts.append(lax.psum_scatter(pre, "dp", scatter_dimension=0, tiled=True))

    hidden = []
    for pre in parts:
        act = jax.nn.gelu(pre.astype(jnp.float32)).astype(jnp.bfloat16)
        hidden.append(lax.all_gather(act, "dp", axis=0, tiled=True))

    shared_pre = jnp.dot(normed, full_shared_in, preferred_element_type=jnp.float32)
    shared_hidden = jax.nn.gelu(shared_pre).astype(jnp.bfloat16)
    shared_result = jnp.dot(shared_hidden, full_shared_out, preferred_element_type=jnp.float32)

    routed = None
    for half, h in enumerate(hidden):
        kind = jnp.bfloat16 if half == halves - 1 else jnp.float32
        routed = second_projection(
            h, keys, gate_of, expert_out, routed, kind, half * count, runs, run_tokens
        )
    width = routed.shape[1]
    pieces = lax.all_to_all(
        routed.reshape(block_count, row_count, width),
        ("expert", "dp"),
        split_axis=0,
        concat_axis=0,
        tiled=True,
    ).reshape(-1, runs, row_count, width)
    own = jnp.sum(pieces.astype(jnp.float32), axis=0).transpose(1, 0, 2)
    own = own.reshape(row_count, model_width)
    return (tokens.astype(jnp.float32) + shared_result + own).astype(jnp.bfloat16)


def start_of(index, size):
    return pl.ds(pl.multiple_of(index * size, size), size)


HEAD = 2


def plane_orders(planes):
    if planes == 4:
        return ((1, 2, 1, 2), (3, 3, 0, 0), (2, 0, 3, 1))
    return tuple(tuple((z + k) % planes for z in range(planes)) for k in range(1, planes))


def fused_kernel(
    sizes,
    tok_hbm,
    ids_hbm,
    gate_hbm,
    win_hbm,
    wout_hbm,
    sin_hbm,
    sout_hbm,
    out_ref,
    tok,
    ids_in,
    gate_in,
    norm,
    xall,
    meta,
    win,
    wout,
    sin,
    sout,
    keys,
    gates,
    pick,
    gslot,
    rows,
    send,
    recv,
    ssend,
    srecv,
    scaled,
    own,
    other,
    psend,
    precv,
    osend,
    orecv,
    zsend,
    zrecv,
    fsend,
    frecv,
    isem,
    lsem,
    wssem,
    wrsem,
    xssem,
    xrsem,
    zssem,
    zrsem,
    rssem,
    rrsem,
    pssem,
    prsem,
    ssem,
    srsem,
    dssem,
    drsem,
    bssem,
    brsem,
    ossem,
    orsem,
    fssem,
    frsem,
):
    planes, chips, cores = sizes
    dp = chips * cores
    tok_rows, width = tok.shape
    picks = ids_in.shape[0]
    half = width // chips
    part = half // cores
    experts = win.shape[0]
    local = experts * cores
    slots, span = pick.shape[2:]
    own_rows = chips * tok_rows
    last = planes - 1
    head = min(HEAD, experts // 2)
    close = max(experts - 1, head + 1)

    z = lax.axis_index("expert")
    d = lax.axis_index("dp")
    c = d % cores
    x = d // cores
    oc = 1 - c
    ox = 1 - x
    partner = {"dp": x * cores + oc}
    across = {"dp": ox * cores + c}
    mesh_ids = pl.DeviceIdType.MESH

    def remote(src, dst, s_sem, r_sem, device):
        return pltpu.make_async_remote_copy(
            src_ref=src,
            dst_ref=dst,
            send_sem=s_sem,
            recv_sem=r_sem,
            device_id=device,
            device_id_type=mesh_ids,
        )

    def loop(first, end, body):
        def step(i, carry):
            body(i)
            return carry

        lax.fori_loop(first, end, step, 0)

    orders = plane_orders(planes)

    def at_step(k):
        found = 0
        for step, order in enumerate(orders):
            for place, p in enumerate(order):
                hit = jnp.logical_and(k == step, z == place)
                found = jnp.where(hit, p, found)
        return jnp.where(k == last, z, found)

    def mine_of(core):
        return pl.ds(core * experts, experts)

    def local_in():
        return pltpu.make_async_copy(
            win_hbm.at[mine_of(c)], win.at[:, start_of(c, part)], lsem.at[0]
        )

    def local_out():
        return pltpu.make_async_copy(
            wout_hbm.at[mine_of(c)], wout.at[:, :, start_of(c, part)], lsem.at[1]
        )

    def local_shared_in():
        return pltpu.make_async_copy(sin_hbm, sin.at[start_of(c, part)], lsem.at[2])

    def local_shared_out():
        return pltpu.make_async_copy(sout_hbm, sout.at[:, start_of(c, part)], lsem.at[3])

    def partner_in(group):
        first, count = ((0, head), (head, experts - head))[group]
        return remote(
            win_hbm.at[pl.ds(oc * experts + first, count)],
            win.at[pl.ds(first, count), start_of(c, part)],
            wssem.at[group],
            wrsem.at[group],
            partner,
        )

    def partner_out():
        return remote(
            wout_hbm.at[mine_of(oc)],
            wout.at[:, :, start_of(c, part)],
            wssem.at[2],
            wrsem.at[2],
            partner,
        )

    def partner_shared_in():
        return remote(sin_hbm, sin.at[start_of(c, part)], wssem.at[3], wrsem.at[3], partner)

    def partner_shared_out():
        return remote(
            sout_hbm, sout.at[:, start_of(c, part)], wssem.at[4], wrsem.at[4], partner
        )

    def block(p, b, kind):
        return meta.at[p, c * chips + b] if kind else xall.at[p, c, b]

    def token_swap(kind):
        src = meta.at[z, c * chips + x] if kind else norm.at[:, start_of(ox, half)]
        return remote(src, block(z, x, kind), xssem.at[kind], xrsem.at[kind], across)

    def both(p, kind):
        return meta.at[p, pl.ds(c * chips, chips)] if kind else xall.at[p, c]

    def to_plane(p, b, kind):
        ref = block(z, b, kind)
        return remote(ref, ref, zssem.at[kind], zrsem.at[z, kind], {"expert": p})

    def from_plane(p, kind):
        ref = both(p, kind)
        return remote(ref, ref, zssem.at[kind], zrsem.at[p, kind], {"expert": p})

    def send_tokens(k, b):
        for p in range(planes):

            @pl.when(z == orders[k][p])
            def _():
                for kind in (1, 0):
                    to_plane(p, b, kind).start()

    def relay_block(b, kind):
        ref = block(z, b, kind)
        return remote(ref, ref, rssem.at[kind], rrsem.at[z, kind], partner)

    def relay(p, kind):
        ref = both(p, kind)
        return remote(ref, ref, rssem.at[kind], rrsem.at[p, kind], partner)

    def tokens_sent(kind, count, s_sem):
        ref = meta.at[pl.ds(0, count), pl.ds(0, chips)] if kind else xall.at[pl.ds(0, count), 0]
        return remote(ref, ref, s_sem.at[kind], zrsem.at[0, kind], partner)

    def swap(k, e):
        return remote(send.at[k, e], recv.at[k, e], pssem.at[0], prsem.at[k, e], across)

    def shared_swap(b):
        return remote(ssend.at[b], srecv.at[b], ssem.at[0], srsem.at[b], across)

    def pair(k):
        return remote(psend.at[k], precv.at[k], dssem.at[0], drsem.at[k], partner)

    def own_pair(b):
        return remote(osend.at[b], orecv.at[b], bssem.at[0], brsem.at[b], partner)

    def give(k):
        return remote(
            zsend.at[k], zrecv.at[z], ossem.at[0], orsem.at[0], {"expert": at_step(k)}
        )

    def given():
        return remote(zsend, zrecv.at[pl.ds(0, last)], ossem.at[0], orsem.at[0], partner)

    def finish():
        return remote(fsend, frecv, fssem.at[0], frsem.at[0], across)

    barrier = pltpu.get_barrier_semaphore()
    peers = [{"expert": lax.rem(z + i, planes)} for i in range(1, planes)]
    for device in [across, partner] + peers:
        pl.semaphore_signal(barrier, inc=1, device_id=device, device_id_type=mesh_ids)
    read_tok = pltpu.make_async_copy(tok_hbm, tok, isem.at[0])
    read_ids = pltpu.make_async_copy(ids_hbm, ids_in, isem.at[1])
    read_gate = pltpu.make_async_copy(gate_hbm, gate_in, isem.at[2])
    read_tok.start()
    read_ids.start()
    read_gate.start()
    local_shared_in().start()
    local_in().start()
    local_shared_out().start()
    local_out().start()
    read_ids.wait()
    read_gate.wait()
    meta[z, c * chips + x, :picks] = ids_in[...].astype(jnp.float32)
    meta[z, c * chips + x, picks:] = gate_in[...]
    read_tok.wait()
    values = tok[...].astype(jnp.float32)
    center = values - jnp.mean(values, axis=-1, keepdims=True)
    spread = jnp.mean(center * center, axis=-1, keepdims=True)
    norm[...] = (center * lax.rsqrt(spread + 1e-06)).astype(jnp.bfloat16)
    xall[z, c, x] = norm[:, start_of(x, half)]

    pl.semaphore_wait(barrier, planes + 1)
    for kind in (1, 0):
        token_swap(kind).start()
    partner_shared_in().start()
    for kind in (1, 0):
        relay_block(x, kind).start()
    partner_in(0).start()
    send_tokens(0, x)

    def shared_first(b):
        pre = jnp.dot(xall[z, c, b], sin[...], preferred_element_type=jnp.float32)
        ssend[b] = pre.astype(jnp.bfloat16)

    local_shared_in().wait()
    partner_shared_in().wait_recv()
    shared_first(x)
    shared_swap(x).start()
    for kind in (1, 0):
        token_swap(kind).wait_recv()
        relay_block(ox, kind).start()
    send_tokens(0, ox)
    partner_in(1).start()
    shared_first(ox)
    shared_swap(ox).start()

    before = jnp.where(
        lax.broadcasted_iota(jnp.int32, (tok_rows, tok_rows), 0)
        < lax.broadcasted_iota(jnp.int32, (tok_rows, tok_rows), 1),
        1.0,
        0.0,
    ).astype(jnp.bfloat16)

    def first_stage(k, turn, mine, weights_next=False):
        p = z if mine else at_step(k)
        if not mine:
            for kind in (1, 0):
                from_plane(p, kind).wait_recv()
                relay(p, kind).start()
            if weights_next:
                partner_shared_out().start()
                partner_out().start()
            for step in range(1, last):

                @pl.when(k == step - 1)
                def _():
                    for b in (x, ox):
                        send_tokens(step, b)

        relay(p, 1).wait_recv()

        ids = jnp.concatenate([meta[p, b, :picks] for b in range(dp)], axis=1)
        weights = jnp.concatenate([meta[p, b, picks:] for b in range(dp)], axis=1)
        chosen, gate = [], []
        for e in range(experts):
            match = ids == (z * local + c * experts + e).astype(jnp.float32)
            chosen.append(jnp.max(jnp.where(match, 1.0, 0.0), axis=0, keepdims=True))
            gate.append(jnp.sum(jnp.where(match, weights, 0.0), axis=0, keepdims=True))
        chosen = jnp.concatenate(chosen, axis=0)
        gates[...] = jnp.concatenate(gate, axis=0)
        for b in range(dp):
            lanes = slice(b * tok_rows, (b + 1) * tok_rows)
            named = chosen[:, lanes]
            earlier = jnp.dot(
                named.astype(jnp.bfloat16), before, preferred_element_type=jnp.float32
            )
            keys[:, lanes] = jnp.where(named > 0.5, earlier + float(b * CAP), -1.0).astype(
                jnp.int32
            )

        def choose(e):
            row = lax.broadcasted_iota(jnp.int32, (slots, span), 0)
            match = row == keys[pl.ds(e, 1), :]
            pick[turn, e] = jnp.where(match, 1.0, 0.0).astype(jnp.bfloat16)
            gate = jnp.sum(
                jnp.where(match, gates[pl.ds(e, 1), :], 0.0), axis=1, keepdims=True
            )
            gslot[turn, e] = jnp.broadcast_to(gate, gslot.shape[2:])

        loop(0, experts, choose)
        relay(p, 0).wait_recv()
        plane = xall[p].reshape(span, half)
        chosen_rows = jnp.dot(
            pick[turn].reshape(experts * slots, span), plane, preferred_element_type=jnp.float32
        )
        rows[...] = chosen_rows.astype(jnp.bfloat16).reshape(rows.shape)

        def project(e):
            pre = jnp.dot(rows[e], win[e], preferred_element_type=jnp.float32)
            send[k, e] = pre.astype(jnp.bfloat16)

        def project_and_send(e):
            project(e)
            swap(k, e).start()

        if mine:
            local_in().wait()
            partner_in(0).wait_recv()
            loop(0, head, project_and_send)
            partner_in(1).wait_recv()
            loop(head, experts, project)
        else:
            loop(0, experts, project_and_send)

    def second_stage(k, turn, first, end):
        def project(e):
            swap(k, e).wait_recv()
            total = send[k, e].astype(jnp.float32) + recv[k, e].astype(jnp.float32)
            h = jax.nn.gelu(total).astype(jnp.bfloat16)
            result = jnp.dot(h, wout[e], preferred_element_type=jnp.float32)
            scaled[e] = (result * gslot[turn, e][:, :1]).astype(jnp.bfloat16)

        loop(first, end, project)

    def combine(turn, first, end, lanes, count):
        return lax.dot_general(
            pick[turn, first:end, :, lanes].reshape((end - first) * slots, count),
            scaled[first:end].reshape((end - first) * slots, half),
            (((0,), (0,)), ((), ())),
            preferred_element_type=jnp.float32,
        )

    first_stage(last, 2, True)
    first_stage(0, 0, False, True)

    local_shared_out().wait()
    partner_shared_out().wait_recv()

    def shared_second(b):
        shared_swap(b).wait_recv()
        total = ssend[b].astype(jnp.float32) + srecv[b].astype(jnp.float32)
        h = jax.nn.gelu(total).astype(jnp.bfloat16)
        own[start_of(b, tok_rows), :] += jnp.dot(
            h, sout[...], preferred_element_type=jnp.float32
        )

    local_out().wait()
    partner_out().wait_recv()

    second_stage(last, 2, 0, head)
    own[...] = combine(2, 0, head, start_of(c, own_rows), own_rows)
    other[...] = combine(2, 0, head, start_of(oc, own_rows), own_rows)
    for b in range(chips):
        shared_second(b)

    def plane_step(k):
        turn = lax.rem(k, 2)

        @pl.when(k < last - 1)
        def _():
            first_stage(k + 1, lax.rem(k + 1, 2), False)

        @pl.when(k == last - 1)
        def _():
            loop(head, experts, lambda e: swap(last, e).start())

        second_stage(k, turn, 0, experts)
        psend[k] = combine(turn, 0, experts, start_of(oc, own_rows), own_rows).astype(
            jnp.bfloat16
        )
        pair(k).start()
        mine = combine(turn, 0, experts, start_of(c, own_rows), own_rows)
        pair(k).wait_recv()
        zsend[k] = (mine + precv[k].astype(jnp.float32)).astype(jnp.bfloat16)
        give(k).start()

    loop(0, last, plane_step)

    second_stage(last, 2, head, close)
    own[...] += combine(2, head, close, start_of(c, own_rows), own_rows)
    other[...] += combine(2, head, close, start_of(oc, own_rows), own_rows)
    given().wait_recv()
    for r in range(1, planes):
        own[...] += zrecv[lax.rem(z + r, planes)].astype(jnp.float32)
    second_stage(last, 2, close, experts)

    def last_part(core, b):
        lanes = start_of(core * chips + b, tok_rows)
        return combine(2, close, experts, lanes, tok_rows)

    def to_partner(b):
        total = other[start_of(b, tok_rows), :] + last_part(oc, b)
        osend[b] = total.astype(jnp.bfloat16)
        own_pair(b).start()

    mine = start_of(x, half)
    theirs = start_of(ox, half)
    to_partner(ox)
    total = own[start_of(ox, tok_rows), :] + last_part(c, ox)
    own_pair(ox).wait_recv()
    fsend[...] = (total + orecv[ox].astype(jnp.float32)).astype(jnp.bfloat16)
    finish().start()
    to_partner(x)
    total = own[start_of(x, tok_rows), :] + last_part(c, x)
    own_pair(x).wait_recv()
    out_ref[:, mine] = (
        tok[:, mine].astype(jnp.float32) + total + orecv[x].astype(jnp.float32)
    ).astype(out_ref.dtype)

    for kind in (0, 1):
        token_swap(kind).wait_send()
        tokens_sent(kind, last, zssem).wait_send()
        tokens_sent(kind, planes, rssem).wait_send()
        partner_in(kind).wait_send()
    partner_shared_in().wait_send()
    partner_shared_out().wait_send()
    partner_out().wait_send()
    remote(send, recv, pssem.at[0], prsem.at[0, 0], across).wait_send()
    remote(ssend, srecv, ssem.at[0], srsem.at[0], across).wait_send()
    remote(osend, orecv, bssem.at[0], brsem.at[0], partner).wait_send()
    remote(psend, precv, dssem.at[0], drsem.at[0], partner).wait_send()
    given().wait_send()

    finish().wait()
    out_ref[:, theirs] = (
        tok[:, theirs].astype(jnp.float32) + frecv[...].astype(jnp.float32)
    ).astype(out_ref.dtype)


def fused(tokens, expert_ids, gate_weights, expert_in, expert_out, shared_in, shared_out):
    tok_rows, width = tokens.shape
    picks = expert_ids.shape[1]
    planes, dp = lax.axis_size("expert"), lax.axis_size("dp")
    cores, chips = 2, dp // 2
    local, part, hidden = expert_in.shape
    experts = local // cores
    half = width // chips
    slots, span = dp * CAP, dp * tok_rows
    own_rows = chips * tok_rows
    bf16, f32 = jnp.bfloat16, jnp.float32
    vmem, dma = pltpu.VMEM, pltpu.SemaphoreType.DMA
    scratch = [
        vmem((tok_rows, width), bf16),
        vmem((picks, tok_rows), jnp.int32),
        vmem((picks, tok_rows), f32),
        vmem((tok_rows, width), bf16),
        vmem((planes, cores, chips, tok_rows, half), bf16),
        vmem((planes, dp, 2 * picks, tok_rows), f32),
        vmem((experts, half, hidden), bf16),
        vmem((experts, hidden, half), bf16),
        vmem((half, hidden), bf16),
        vmem((hidden, half), bf16),
        vmem((experts, span), jnp.int32),
        vmem((experts, span), f32),
        vmem((3, experts, slots, span), bf16),
        vmem((3, experts, slots, 128), f32),
        vmem((experts, slots, half), bf16),
        vmem((planes, experts, slots, hidden), bf16),
        vmem((planes, experts, slots, hidden), bf16),
        vmem((chips, tok_rows, hidden), bf16),
        vmem((chips, tok_rows, hidden), bf16),
        vmem((experts, slots, half), bf16),
        vmem((own_rows, half), f32),
        vmem((own_rows, half), f32),
        vmem((planes - 1, own_rows, half), bf16),
        vmem((planes - 1, own_rows, half), bf16),
        vmem((chips, tok_rows, half), bf16),
        vmem((chips, tok_rows, half), bf16),
        vmem((planes - 1, own_rows, half), bf16),
        vmem((planes, own_rows, half), bf16),
        vmem((tok_rows, half), bf16),
        vmem((tok_rows, half), bf16),
        dma((3,)),
        dma((4,)),
    ]
    pairs = [
        ((5,), (5,)),
        ((2,), (2,)),
        ((2,), (planes, 2)),
        ((2,), (planes, 2)),
        ((1,), (planes, experts)),
        ((1,), (chips,)),
        ((1,), (planes - 1,)),
        ((1,), (chips,)),
        ((1,), (1,)),
        ((1,), (1,)),
    ]
    for sent, received in pairs:
        scratch += [dma(sent), dma(received)]
    given = (tokens, expert_ids.T, gate_weights.T, expert_in, expert_out, shared_in, shared_out)
    given = [pltpu.with_memory_space_constraint(a, pltpu.HBM) for a in given]
    apart = pl.BlockSpec(memory_space=pl.ANY)
    return pl.pallas_call(
        functools.partial(fused_kernel, (planes, chips, cores)),
        in_specs=[apart] * 7,
        out_specs=pl.BlockSpec(memory_space=pltpu.VMEM),
        out_shape=jax.ShapeDtypeStruct((tok_rows, width), tokens.dtype),
        scratch_shapes=scratch,
        compiler_params=pltpu.CompilerParams(
            collective_id=0, has_side_effects=True, vmem_limit_bytes=56098816
        ),
    )(*given)


def fits(mesh, args):
    planes, dp = mesh.shape["expert"], mesh.shape["dp"]
    tokens, expert_in = args[0], args[3]
    return (
        dp == 4
        and 1 < planes <= 8
        and expert_in.shape[0] // (mesh.shape["sweep"] * planes) % 2 == 0
        and expert_in.shape[0] // (mesh.shape["sweep"] * planes) <= 16
        and tokens.shape[0] // (mesh.shape["sweep"] * planes * dp) == 128
    )


def solution(mesh):
    placed = (
        P(("sweep", "expert", "dp"), None),
        P(("sweep", "expert", "dp"), None),
        P(("sweep", "expert", "dp"), None),
        P(("sweep", "expert"), "dp", None),
        P(("sweep", "expert"), None, "dp"),
        P(("sweep", "dp"), None),
        P("sweep", "dp"),
    )

    def run(*args):
        return jax.shard_map(
            fused if fits(mesh, args) else per_device,
            mesh=mesh,
            in_specs=placed,
            out_specs=P(("sweep", "expert", "dp"), None),
            check_vma=False,
        )(*args)

    return run
```

```python
import functools

import jax
import jax.numpy as jnp
from jax import lax
from jax.experimental import pallas as pl
from jax.experimental.pallas import tpu as pltpu
from jax.sharding import PartitionSpec as P

CAP = 20
GROUP = 4


def layer_norm(tokens):
    values = tokens.astype(jnp.float32)
    center = values - jnp.mean(values, axis=-1, keepdims=True)
    spread = jnp.mean(center * center, axis=-1, keepdims=True)
    return (center * lax.rsqrt(spread + 1e-06)).astype(jnp.bfloat16)


def first_kernel(runs, run_tokens, x_ref, key_ref, w_ref, out_ref, rows_ref):
    slots = out_ref.shape[3]
    for j in range(runs):
        span = slice(j * run_tokens, (j + 1) * run_tokens)
        row = lax.broadcasted_iota(jnp.int32, (slots, run_tokens), 0)
        pick = jnp.where(row == key_ref[0, :, span], 1.0, 0.0).astype(jnp.bfloat16)
        rows_ref[j * slots : (j + 1) * slots, :] = jnp.dot(
            pick, x_ref[span, :], preferred_element_type=jnp.float32
        ).astype(jnp.bfloat16)
    pre = jnp.dot(rows_ref[...], w_ref[0], preferred_element_type=jnp.float32)
    for j in range(runs):
        out_ref[j, 0, 0] = pre[j * slots : (j + 1) * slots].astype(jnp.bfloat16)


def first_projection(x, keys, weight, first, count, runs, run_tokens, slots):
    width, hidden = weight.shape[1:]
    chunk = runs * run_tokens
    chunks = x.shape[0] // chunk
    total = count * chunks * runs * slots
    return pl.pallas_call(
        functools.partial(first_kernel, runs, run_tokens),
        grid=(count, chunks),
        in_specs=[
            pl.BlockSpec((chunk, width), lambda e, c: (c, 0)),
            pl.BlockSpec((1, 1, chunk), lambda e, c: (e + first, 0, c)),
            pl.BlockSpec((1, width, hidden), lambda e, c: (e + first, 0, 0)),
        ],
        out_specs=pl.BlockSpec((runs, 1, 1, slots, hidden), lambda e, c: (0, e, c, 0, 0)),
        out_shape=jax.ShapeDtypeStruct((runs, count, chunks, slots, hidden), jnp.bfloat16),
        scratch_shapes=[pltpu.VMEM((runs * slots, width), jnp.bfloat16)],
        cost_estimate=pl.CostEstimate(
            flops=2 * total * width * (hidden + run_tokens),
            bytes_accessed=2 * (count * width * hidden + total * hidden + x.size),
            transcendentals=0,
        ),
    )(x, keys, weight)


def second_kernel(runs, run_tokens, h_ref, key_ref, gate_ref, w_ref, *refs):
    carry_ref, (out_ref, total_ref) = refs[0] if len(refs) == 3 else None, refs[-2:]
    expert = pl.program_id(1)
    slots = h_ref.shape[3]

    @pl.when(expert == 0)
    def _():
        total_ref[...] = jnp.zeros_like(total_ref) if carry_ref is None else carry_ref[...]

    h = jnp.concatenate([h_ref[j, 0, 0] for j in range(runs)], axis=0)
    result = jnp.dot(h, w_ref[0], preferred_element_type=jnp.float32)
    for j in range(runs):
        span = slice(j * run_tokens, (j + 1) * run_tokens)
        row = lax.broadcasted_iota(jnp.int32, (slots, run_tokens), 0)
        match = row == key_ref[0, :, span]
        gate = jnp.sum(jnp.where(match, gate_ref[0, :, span], 0.0), axis=1, keepdims=True)
        scaled = (result[j * slots : (j + 1) * slots] * gate).astype(jnp.bfloat16)
        total_ref[span, :] += lax.dot_general(
            jnp.where(match, 1.0, 0.0).astype(jnp.bfloat16),
            scaled,
            (((0,), (0,)), ((), ())),
            preferred_element_type=jnp.float32,
        )

    @pl.when(expert == pl.num_programs(1) - 1)
    def _():
        out_ref[...] = total_ref[...].astype(out_ref.dtype)


def second_projection(hidden, keys, gates, weight, carry, kind, first, runs, run_tokens):
    _, count, chunks, slots, depth = hidden.shape
    width = weight.shape[2]
    chunk = runs * run_tokens
    total = count * chunks * runs * slots
    carries = [] if carry is None else [carry]
    return pl.pallas_call(
        functools.partial(second_kernel, runs, run_tokens),
        grid=(chunks, count),
        in_specs=[
            pl.BlockSpec((runs, 1, 1, slots, depth), lambda c, e: (0, e, c, 0, 0)),
            pl.BlockSpec((1, 1, chunk), lambda c, e: (e + first, 0, c)),
            pl.BlockSpec((1, 1, chunk), lambda c, e: (e + first, 0, c)),
            pl.BlockSpec((1, depth, width), lambda c, e: (e + first, 0, 0)),
        ]
        + [pl.BlockSpec((chunk, width), lambda c, e: (c, 0)) for _ in carries],
        out_specs=pl.BlockSpec((chunk, width), lambda c, e: (c, 0)),
        out_shape=jax.ShapeDtypeStruct((chunks * chunk, width), kind),
        scratch_shapes=[pltpu.VMEM((chunk, width), jnp.float32)],
        cost_estimate=pl.CostEstimate(
            flops=2 * total * width * (depth + 3 * run_tokens),
            bytes_accessed=2 * (count * depth * width + total * depth) + 4 * chunks * chunk * width,
            transcendentals=0,
        ),
    )(hidden, keys, gates, weight, *carries)


def per_device(tokens, expert_ids, gate_weights, expert_in, expert_out, shared_in, shared_out):
    row_count, model_width = tokens.shape
    pick_count = expert_ids.shape[1]
    local_count = expert_in.shape[0]
    runs = lax.axis_size("dp")
    block_count = runs * lax.axis_size("expert")
    run_tokens = GROUP * row_count
    slots = GROUP * CAP
    halves = 2 if local_count % 2 == 0 else 1

    normed = layer_norm(tokens)
    full_shared_in = lax.all_gather(shared_in, "dp", axis=0, tiled=True)
    full_shared_out = lax.all_gather(shared_out, "dp", axis=1, tiled=True)

    named = jnp.concatenate([expert_ids.astype(jnp.float32), gate_weights], axis=1).T
    named = lax.all_gather(named, ("expert", "dp"), axis=0, tiled=False)
    ids, gates = named[:, :pick_count], named[:, pick_count:]
    columns = lax.all_to_all(normed, "dp", split_axis=1, concat_axis=0, tiled=True)
    columns, full_shared_in, full_shared_out = lax.optimization_barrier(
        (columns, full_shared_in, full_shared_out)
    )
    x = lax.all_gather(columns, "expert", axis=0, tiled=True)

    owned = lax.axis_index("expert") * local_count + jnp.arange(local_count, dtype=jnp.int32)
    matches = ids[:, :, None, :] == owned.astype(jnp.float32)[:, None]
    chosen = jnp.any(matches, axis=1)
    gate_of = jnp.sum(jnp.where(matches, gates[:, :, None, :], 0.0), axis=1)
    order = jnp.arange(row_count, dtype=jnp.int32)
    before = (order[:, None] < order[None, :]).astype(jnp.bfloat16)
    earlier = jnp.einsum(
        "bej,ji->bei", chosen.astype(jnp.bfloat16), before, preferred_element_type=jnp.float32
    ).astype(jnp.int32)
    base = jnp.arange(block_count, dtype=jnp.int32) % GROUP * CAP
    keys = jnp.where(chosen, earlier + base[:, None, None], -1)

    def by_expert(table):
        return table.transpose(1, 0, 2).reshape(local_count, 1, block_count * row_count)

    keys, gate_of = by_expert(keys), by_expert(gate_of)

    count = local_count // halves
    parts = []
    for half in range(halves):
        pre = first_projection(
            x, keys, expert_in, half * count, count, runs, run_tokens, slots
        )
        parts.append(lax.psum_scatter(pre, "dp", scatter_dimension=0, tiled=True))

    hidden = []
    for pre in parts:
        act = jax.nn.gelu(pre.astype(jnp.float32)).astype(jnp.bfloat16)
        hidden.append(lax.all_gather(act, "dp", axis=0, tiled=True))

    shared_pre = jnp.dot(normed, full_shared_in, preferred_element_type=jnp.float32)
    shared_hidden = jax.nn.gelu(shared_pre).astype(jnp.bfloat16)
    shared_result = jnp.dot(shared_hidden, full_shared_out, preferred_element_type=jnp.float32)

    routed = None
    for half, h in enumerate(hidden):
        kind = jnp.bfloat16 if half == halves - 1 else jnp.float32
        routed = second_projection(
            h, keys, gate_of, expert_out, routed, kind, half * count, runs, run_tokens
        )
    width = routed.shape[1]
    pieces = lax.all_to_all(
        routed.reshape(block_count, row_count, width),
        ("expert", "dp"),
        split_axis=0,
        concat_axis=0,
        tiled=True,
    ).reshape(-1, runs, row_count, width)
    own = jnp.sum(pieces.astype(jnp.float32), axis=0).transpose(1, 0, 2)
    own = own.reshape(row_count, model_width)
    return (tokens.astype(jnp.float32) + shared_result + own).astype(jnp.bfloat16)


def start_of(index, size):
    return pl.ds(pl.multiple_of(index * size, size), size)


HEAD = 2


def plane_orders(planes):
    if planes == 4:
        return ((1, 2, 1, 2), (3, 3, 0, 0), (2, 0, 3, 1))
    return tuple(tuple((z + k) % planes for z in range(planes)) for k in range(1, planes))


def fused_kernel(
    sizes,
    tok_hbm,
    ids_hbm,
    gate_hbm,
    win_hbm,
    wout_hbm,
    sin_hbm,
    sout_hbm,
    out_ref,
    tok,
    ids_in,
    gate_in,
    norm,
    xall,
    meta,
    win,
    wout,
    sin,
    sout,
    keys,
    gates,
    pick,
    gslot,
    rows,
    send,
    recv,
    ssend,
    srecv,
    scaled,
    own,
    other,
    psend,
    precv,
    osend,
    orecv,
    zsend,
    zrecv,
    fsend,
    frecv,
    lsend,
    lrecv,
    lpick,
    lscaled,
    isem,
    lsem,
    wssem,
    wrsem,
    xssem,
    xrsem,
    zssem,
    zrsem,
    rssem,
    rrsem,
    pssem,
    prsem,
    ssem,
    srsem,
    dssem,
    drsem,
    bssem,
    brsem,
    ossem,
    orsem,
    fssem,
    frsem,
    lssem,
    lrsem,
):
    planes, chips, cores = sizes
    dp = chips * cores
    tok_rows, width = tok.shape
    picks = ids_in.shape[0]
    half = width // chips
    part = half // cores
    experts = win.shape[0]
    local = experts * cores
    slots, span = pick.shape[2:]
    own_rows = chips * tok_rows
    last = planes - 1
    head = min(HEAD, experts // 2)
    close = experts - 2
    piece = slots // cores

    z = lax.axis_index("expert")
    d = lax.axis_index("dp")
    c = d % cores
    x = d // cores
    oc = 1 - c
    ox = 1 - x
    partner = {"dp": x * cores + oc}
    across = {"dp": ox * cores + c}
    mesh_ids = pl.DeviceIdType.MESH

    def remote(src, dst, s_sem, r_sem, device):
        return pltpu.make_async_remote_copy(
            src_ref=src,
            dst_ref=dst,
            send_sem=s_sem,
            recv_sem=r_sem,
            device_id=device,
            device_id_type=mesh_ids,
        )

    def loop(first, end, body):
        def step(i, carry):
            body(i)
            return carry

        lax.fori_loop(first, end, step, 0)

    orders = plane_orders(planes)

    def at_step(k):
        found = 0
        for step, order in enumerate(orders):
            for place, p in enumerate(order):
                hit = jnp.logical_and(k == step, z == place)
                found = jnp.where(hit, p, found)
        return jnp.where(k == last, z, found)

    def mine_of(core):
        return pl.ds(core * experts, experts)

    def local_in():
        return pltpu.make_async_copy(
            win_hbm.at[mine_of(c)], win.at[:, start_of(c, part)], lsem.at[0]
        )

    def local_out():
        return pltpu.make_async_copy(
            wout_hbm.at[mine_of(c)], wout.at[:, :, start_of(c, part)], lsem.at[1]
        )

    def local_shared_in():
        return pltpu.make_async_copy(sin_hbm, sin.at[start_of(c, part)], lsem.at[2])

    def local_shared_out():
        return pltpu.make_async_copy(sout_hbm, sout.at[:, start_of(c, part)], lsem.at[3])

    def partner_in(group):
        first, count = ((0, head), (head, experts - head))[group]
        return remote(
            win_hbm.at[pl.ds(oc * experts + first, count)],
            win.at[pl.ds(first, count), start_of(c, part)],
            wssem.at[group],
            wrsem.at[group],
            partner,
        )

    def partner_out():
        return remote(
            wout_hbm.at[mine_of(oc)],
            wout.at[:, :, start_of(c, part)],
            wssem.at[2],
            wrsem.at[2],
            partner,
        )

    def partner_shared_in():
        return remote(sin_hbm, sin.at[start_of(c, part)], wssem.at[3], wrsem.at[3], partner)

    def partner_shared_out():
        return remote(
            sout_hbm, sout.at[:, start_of(c, part)], wssem.at[4], wrsem.at[4], partner
        )

    def block(p, b, kind):
        return meta.at[p, c * chips + b] if kind else xall.at[p, c, b]

    def token_swap(kind):
        src = meta.at[z, c * chips + x] if kind else norm.at[:, start_of(ox, half)]
        return remote(src, block(z, x, kind), xssem.at[kind], xrsem.at[kind], across)

    def both(p, kind):
        return meta.at[p, pl.ds(c * chips, chips)] if kind else xall.at[p, c]

    def to_plane(p, b, kind):
        ref = block(z, b, kind)
        return remote(ref, ref, zssem.at[kind], zrsem.at[z, kind], {"expert": p})

    def from_plane(p, kind):
        ref = both(p, kind)
        return remote(ref, ref, zssem.at[kind], zrsem.at[p, kind], {"expert": p})

    def send_tokens(k, b):
        for p in range(planes):

            @pl.when(z == orders[k][p])
            def _():
                for kind in (1, 0):
                    to_plane(p, b, kind).start()

    def relay_block(b, kind):
        ref = block(z, b, kind)
        return remote(ref, ref, rssem.at[kind], rrsem.at[z, kind], partner)

    def relay(p, kind):
        ref = both(p, kind)
        return remote(ref, ref, rssem.at[kind], rrsem.at[p, kind], partner)

    def tokens_sent(kind, count, s_sem):
        ref = meta.at[pl.ds(0, count), pl.ds(0, chips)] if kind else xall.at[pl.ds(0, count), 0]
        return remote(ref, ref, s_sem.at[kind], zrsem.at[0, kind], partner)

    def swap(k, e):
        return remote(send.at[k, e], recv.at[k, e], pssem.at[lax.div(k, last)], prsem.at[k, e], across)

    def last_swap(e, g):
        return remote(lsend.at[e, g], lrecv.at[e, g], lssem.at[0], lrsem.at[e, g], across)

    def shared_swap(b):
        return remote(ssend.at[b], srecv.at[b], ssem.at[0], srsem.at[b], across)

    def pair(k):
        return remote(psend.at[k], precv.at[k], dssem.at[0], drsem.at[k], partner)

    def own_pair(b):
        return remote(osend.at[b], orecv.at[b], bssem.at[0], brsem.at[b], partner)

    def give(k):
        return remote(
            zsend.at[k], zrecv.at[z], ossem.at[0], orsem.at[0], {"expert": at_step(k)}
        )

    def given():
        return remote(zsend, zrecv.at[pl.ds(0, last)], ossem.at[0], orsem.at[0], partner)

    def finish():
        return remote(fsend, frecv, fssem.at[0], frsem.at[0], across)

    barrier = pltpu.get_barrier_semaphore()
    peers = [{"expert": lax.rem(z + i, planes)} for i in range(1, planes)]
    for device in [across, partner] + peers:
        pl.semaphore_signal(barrier, inc=1, device_id=device, device_id_type=mesh_ids)
    read_tok = pltpu.make_async_copy(tok_hbm, tok, isem.at[0])
    read_ids = pltpu.make_async_copy(ids_hbm, ids_in, isem.at[1])
    read_gate = pltpu.make_async_copy(gate_hbm, gate_in, isem.at[2])
    read_tok.start()
    read_ids.start()
    read_gate.start()
    local_shared_in().start()
    local_in().start()
    local_shared_out().start()
    local_out().start()
    read_ids.wait()
    read_gate.wait()
    meta[z, c * chips + x, :picks] = ids_in[...].astype(jnp.float32)
    meta[z, c * chips + x, picks:] = gate_in[...]
    read_tok.wait()
    values = tok[...].astype(jnp.float32)
    center = values - jnp.mean(values, axis=-1, keepdims=True)
    spread = jnp.mean(center * center, axis=-1, keepdims=True)
    norm[...] = (center * lax.rsqrt(spread + 1e-06)).astype(jnp.bfloat16)
    xall[z, c, x] = norm[:, start_of(x, half)]

    pl.semaphore_wait(barrier, planes + 1)
    for kind in (1, 0):
        token_swap(kind).start()
    partner_shared_in().start()
    for kind in (1, 0):
        relay_block(x, kind).start()
    partner_in(0).start()
    send_tokens(0, x)

    def shared_first(b):
        pre = jnp.dot(xall[z, c, b], sin[...], preferred_element_type=jnp.float32)
        ssend[b] = pre.astype(jnp.bfloat16)

    local_shared_in().wait()
    partner_shared_in().wait_recv()
    shared_first(x)
    shared_swap(x).start()
    for kind in (1, 0):
        token_swap(kind).wait_recv()
        relay_block(ox, kind).start()
    send_tokens(0, ox)
    partner_in(1).start()
    shared_first(ox)
    shared_swap(ox).start()

    before = jnp.where(
        lax.broadcasted_iota(jnp.int32, (tok_rows, tok_rows), 0)
        < lax.broadcasted_iota(jnp.int32, (tok_rows, tok_rows), 1),
        1.0,
        0.0,
    ).astype(jnp.bfloat16)

    def first_stage(k, turn, mine, weights_next=False):
        p = z if mine else at_step(k)
        if not mine:
            for kind in (1, 0):
                from_plane(p, kind).wait_recv()
                relay(p, kind).start()
            if weights_next:
                partner_shared_out().start()
                partner_out().start()
            for step in range(1, last):

                @pl.when(k == step - 1)
                def _():
                    for b in (x, ox):
                        send_tokens(step, b)

        relay(p, 1).wait_recv()

        ids = jnp.concatenate([meta[p, b, :picks] for b in range(dp)], axis=1)
        weights = jnp.concatenate([meta[p, b, picks:] for b in range(dp)], axis=1)
        chosen, gate = [], []
        for e in range(experts):
            match = ids == (z * local + c * experts + e).astype(jnp.float32)
            chosen.append(jnp.max(jnp.where(match, 1.0, 0.0), axis=0, keepdims=True))
            gate.append(jnp.sum(jnp.where(match, weights, 0.0), axis=0, keepdims=True))
        chosen = jnp.concatenate(chosen, axis=0)
        gates[...] = jnp.concatenate(gate, axis=0)
        for b in range(dp):
            lanes = slice(b * tok_rows, (b + 1) * tok_rows)
            named = chosen[:, lanes]
            earlier = jnp.dot(
                named.astype(jnp.bfloat16), before, preferred_element_type=jnp.float32
            )
            keys[:, lanes] = jnp.where(named > 0.5, earlier + float(b * CAP), -1.0).astype(
                jnp.int32
            )

        def choose(e):
            row = lax.broadcasted_iota(jnp.int32, (slots, span), 0)
            match = row == keys[pl.ds(e, 1), :]
            pick[turn, e] = jnp.where(match, 1.0, 0.0).astype(jnp.bfloat16)
            gate = jnp.sum(
                jnp.where(match, gates[pl.ds(e, 1), :], 0.0), axis=1, keepdims=True
            )
            gslot[turn, e] = jnp.broadcast_to(gate, gslot.shape[2:])

        loop(0, experts, choose)
        relay(p, 0).wait_recv()
        plane = xall[p].reshape(span, half)
        chosen_rows = jnp.dot(
            pick[turn].reshape(experts * slots, span), plane, preferred_element_type=jnp.float32
        )
        rows[...] = chosen_rows.astype(jnp.bfloat16).reshape(rows.shape)

        def project(e):
            pre = jnp.dot(rows[e], win[e], preferred_element_type=jnp.float32)
            send[k, e] = pre.astype(jnp.bfloat16)

        def project_and_send(e):
            project(e)
            swap(k, e).start()

        if mine:
            local_in().wait()
            partner_in(0).wait_recv()
            loop(0, head, project_and_send)
            partner_in(1).wait_recv()
            loop(head, close, project)
            for e in range(close, experts):
                pre = jnp.dot(rows[e], win[e], preferred_element_type=jnp.float32)
                for g in range(cores):
                    lanes = slice(g * own_rows, (g + 1) * own_rows)
                    row = lax.broadcasted_iota(jnp.int32, (piece, own_rows), 0) + g * piece
                    match = row == keys[e : e + 1, lanes]
                    lpick[e - close, g] = jnp.where(match, 1.0, 0.0).astype(jnp.bfloat16)
                    lsend[e - close, g] = pre[g * piece : (g + 1) * piece].astype(jnp.bfloat16)
        else:
            loop(0, experts, project_and_send)

    def second_stage(k, turn, first, end):
        def project(e):
            swap(k, e).wait_recv()
            total = send[k, e].astype(jnp.float32) + recv[k, e].astype(jnp.float32)
            h = jax.nn.gelu(total).astype(jnp.bfloat16)
            result = jnp.dot(h, wout[e], preferred_element_type=jnp.float32)
            scaled[e] = (result * gslot[turn, e][:, :1]).astype(jnp.bfloat16)

        loop(first, end, project)

    def combine(turn, first, end, lanes, count):
        return lax.dot_general(
            pick[turn, first:end, :, lanes].reshape((end - first) * slots, count),
            scaled[first:end].reshape((end - first) * slots, half),
            (((0,), (0,)), ((), ())),
            preferred_element_type=jnp.float32,
        )

    first_stage(last, 2, True)
    first_stage(0, 0, False, True)

    local_shared_out().wait()
    partner_shared_out().wait_recv()

    def shared_second(b):
        shared_swap(b).wait_recv()
        total = ssend[b].astype(jnp.float32) + srecv[b].astype(jnp.float32)
        h = jax.nn.gelu(total).astype(jnp.bfloat16)
        own[start_of(b, tok_rows), :] += jnp.dot(
            h, sout[...], preferred_element_type=jnp.float32
        )

    local_out().wait()
    partner_out().wait_recv()

    second_stage(last, 2, 0, head)
    own[...] = combine(2, 0, head, start_of(c, own_rows), own_rows)
    other[...] = combine(2, 0, head, start_of(oc, own_rows), own_rows)
    for b in range(chips):
        shared_second(b)

    def plane_step(k):
        turn = lax.rem(k, 2)

        @pl.when(k < last - 1)
        def _():
            first_stage(k + 1, lax.rem(k + 1, 2), False)

        @pl.when(k == last - 1)
        def _():
            loop(head, close, lambda e: swap(last, e).start())
            for g in range(cores):
                for e in range(experts - close):
                    last_swap(e, g).start()

        second_stage(k, turn, 0, experts)
        psend[k] = combine(turn, 0, experts, start_of(oc, own_rows), own_rows).astype(
            jnp.bfloat16
        )
        pair(k).start()
        mine = combine(turn, 0, experts, start_of(c, own_rows), own_rows)
        pair(k).wait_recv()
        zsend[k] = (mine + precv[k].astype(jnp.float32)).astype(jnp.bfloat16)
        give(k).start()

    loop(0, last, plane_step)

    second_stage(last, 2, head, close)
    own[...] += combine(2, head, close, start_of(c, own_rows), own_rows)
    other[...] += combine(2, head, close, start_of(oc, own_rows), own_rows)
    given().wait_recv()
    for r in range(1, planes):
        own[...] += zrecv[lax.rem(z + r, planes)].astype(jnp.float32)
    mine = start_of(x, half)
    theirs = start_of(ox, half)

    def last_stage(g):
        extra = None
        for e in range(experts - close):
            last_swap(e, g).wait_recv()
            total = lsend[e, g].astype(jnp.float32) + lrecv[e, g].astype(jnp.float32)
            h = jax.nn.gelu(total).astype(jnp.bfloat16)
            result = jnp.dot(h, wout[close + e], preferred_element_type=jnp.float32)
            gate = gslot[2, close + e, g * piece : (g + 1) * piece, :1]
            lscaled[e, g] = (result * gate).astype(jnp.bfloat16)
            part_sum = lax.dot_general(
                lpick[e, g],
                lscaled[e, g],
                (((0,), (0,)), ((), ())),
                preferred_element_type=jnp.float32,
            )
            extra = part_sum if extra is None else extra + part_sum

        @pl.when(c != g)
        def _():
            other[...] += extra
            for b in (ox, x):
                osend[b] = other[start_of(b, tok_rows), :].astype(jnp.bfloat16)
                own_pair(b).start()

        @pl.when(c == g)
        def _():
            own[...] += extra
            own_pair(ox).wait_recv()
            total = own[start_of(ox, tok_rows), :] + orecv[ox].astype(jnp.float32)
            fsend[...] = total.astype(jnp.bfloat16)
            finish().start()

    for g in range(cores):
        last_stage(g)
    own_pair(x).wait_recv()
    total = own[start_of(x, tok_rows), :] + orecv[x].astype(jnp.float32)
    out_ref[:, mine] = (tok[:, mine].astype(jnp.float32) + total).astype(out_ref.dtype)

    for kind in (0, 1):
        token_swap(kind).wait_send()
        tokens_sent(kind, last, zssem).wait_send()
        tokens_sent(kind, planes, rssem).wait_send()
        partner_in(kind).wait_send()
    partner_shared_in().wait_send()
    partner_shared_out().wait_send()
    partner_out().wait_send()
    remote(send.at[pl.ds(0, last)], recv.at[pl.ds(0, last)], pssem.at[0], prsem.at[0, 0], across).wait_send()
    remote(
        send.at[last, pl.ds(0, close)],
        recv.at[last, pl.ds(0, close)],
        pssem.at[1],
        prsem.at[0, 0],
        across,
    ).wait_send()
    remote(lsend, lrecv, lssem.at[0], lrsem.at[0, 0], across).wait_send()
    remote(ssend, srecv, ssem.at[0], srsem.at[0], across).wait_send()
    remote(osend, orecv, bssem.at[0], brsem.at[0], partner).wait_send()
    remote(psend, precv, dssem.at[0], drsem.at[0], partner).wait_send()
    given().wait_send()

    finish().wait()
    out_ref[:, theirs] = (
        tok[:, theirs].astype(jnp.float32) + frecv[...].astype(jnp.float32)
    ).astype(out_ref.dtype)


def fused(tokens, expert_ids, gate_weights, expert_in, expert_out, shared_in, shared_out):
    tok_rows, width = tokens.shape
    picks = expert_ids.shape[1]
    planes, dp = lax.axis_size("expert"), lax.axis_size("dp")
    cores, chips = 2, dp // 2
    local, part, hidden = expert_in.shape
    experts = local // cores
    half = width // chips
    slots, span = dp * CAP, dp * tok_rows
    own_rows = chips * tok_rows
    bf16, f32 = jnp.bfloat16, jnp.float32
    vmem, dma = pltpu.VMEM, pltpu.SemaphoreType.DMA
    scratch = [
        vmem((tok_rows, width), bf16),
        vmem((picks, tok_rows), jnp.int32),
        vmem((picks, tok_rows), f32),
        vmem((tok_rows, width), bf16),
        vmem((planes, cores, chips, tok_rows, half), bf16),
        vmem((planes, dp, 2 * picks, tok_rows), f32),
        vmem((experts, half, hidden), bf16),
        vmem((experts, hidden, half), bf16),
        vmem((half, hidden), bf16),
        vmem((hidden, half), bf16),
        vmem((experts, span), jnp.int32),
        vmem((experts, span), f32),
        vmem((3, experts, slots, span), bf16),
        vmem((3, experts, slots, 128), f32),
        vmem((experts, slots, half), bf16),
        vmem((planes, experts, slots, hidden), bf16),
        vmem((planes, experts, slots, hidden), bf16),
        vmem((chips, tok_rows, hidden), bf16),
        vmem((chips, tok_rows, hidden), bf16),
        vmem((experts, slots, half), bf16),
        vmem((own_rows, half), f32),
        vmem((own_rows, half), f32),
        vmem((planes - 1, own_rows, half), bf16),
        vmem((planes - 1, own_rows, half), bf16),
        vmem((chips, tok_rows, half), bf16),
        vmem((chips, tok_rows, half), bf16),
        vmem((planes - 1, own_rows, half), bf16),
        vmem((planes, own_rows, half), bf16),
        vmem((tok_rows, half), bf16),
        vmem((tok_rows, half), bf16),
        vmem((2, cores, slots // cores, hidden), bf16),
        vmem((2, cores, slots // cores, hidden), bf16),
        vmem((2, cores, slots // cores, own_rows), bf16),
        vmem((2, cores, slots // cores, half), bf16),
        dma((3,)),
        dma((4,)),
    ]
    pairs = [
        ((5,), (5,)),
        ((2,), (2,)),
        ((2,), (planes, 2)),
        ((2,), (planes, 2)),
        ((2,), (planes, experts)),
        ((1,), (chips,)),
        ((1,), (planes - 1,)),
        ((1,), (chips,)),
        ((1,), (1,)),
        ((1,), (1,)),
        ((1,), (2, cores)),
    ]
    for sent, received in pairs:
        scratch += [dma(sent), dma(received)]
    given = (tokens, expert_ids.T, gate_weights.T, expert_in, expert_out, shared_in, shared_out)
    given = [pltpu.with_memory_space_constraint(a, pltpu.HBM) for a in given]
    apart = pl.BlockSpec(memory_space=pl.ANY)
    return pl.pallas_call(
        functools.partial(fused_kernel, (planes, chips, cores)),
        in_specs=[apart] * 7,
        out_specs=pl.BlockSpec(memory_space=pltpu.VMEM),
        out_shape=jax.ShapeDtypeStruct((tok_rows, width), tokens.dtype),
        scratch_shapes=scratch,
        compiler_params=pltpu.CompilerParams(
            collective_id=0, has_side_effects=True, vmem_limit_bytes=56098816
        ),
    )(*given)


def fits(mesh, args):
    planes, dp = mesh.shape["expert"], mesh.shape["dp"]
    tokens, expert_in = args[0], args[3]
    return (
        dp == 4
        and 1 < planes <= 8
        and expert_in.shape[0] // (mesh.shape["sweep"] * planes) % 2 == 0
        and expert_in.shape[0] // (mesh.shape["sweep"] * planes) <= 16
        and tokens.shape[0] // (mesh.shape["sweep"] * planes * dp) == 128
    )


def solution(mesh):
    placed = (
        P(("sweep", "expert", "dp"), None),
        P(("sweep", "expert", "dp"), None),
        P(("sweep", "expert", "dp"), None),
        P(("sweep", "expert"), "dp", None),
        P(("sweep", "expert"), None, "dp"),
        P(("sweep", "dp"), None),
        P("sweep", "dp"),
    )

    def run(*args):
        return jax.shard_map(
            fused if fits(mesh, args) else per_device,
            mesh=mesh,
            in_specs=placed,
            out_specs=P(("sweep", "expert", "dp"), None),
            check_vma=False,
        )(*args)

    return run
```

```python
import functools

import jax
import jax.numpy as jnp
from jax import lax
from jax.experimental import pallas as pl
from jax.experimental.pallas import tpu as pltpu
from jax.sharding import PartitionSpec as P

CAP = 20
GROUP = 4


def layer_norm(tokens):
    values = tokens.astype(jnp.float32)
    center = values - jnp.mean(values, axis=-1, keepdims=True)
    spread = jnp.mean(center * center, axis=-1, keepdims=True)
    return (center * lax.rsqrt(spread + 1e-06)).astype(jnp.bfloat16)


def first_kernel(runs, run_tokens, x_ref, key_ref, w_ref, out_ref, rows_ref):
    slots = out_ref.shape[3]
    for j in range(runs):
        span = slice(j * run_tokens, (j + 1) * run_tokens)
        row = lax.broadcasted_iota(jnp.int32, (slots, run_tokens), 0)
        pick = jnp.where(row == key_ref[0, :, span], 1.0, 0.0).astype(jnp.bfloat16)
        rows_ref[j * slots : (j + 1) * slots, :] = jnp.dot(
            pick, x_ref[span, :], preferred_element_type=jnp.float32
        ).astype(jnp.bfloat16)
    pre = jnp.dot(rows_ref[...], w_ref[0], preferred_element_type=jnp.float32)
    for j in range(runs):
        out_ref[j, 0, 0] = pre[j * slots : (j + 1) * slots].astype(jnp.bfloat16)


def first_projection(x, keys, weight, first, count, runs, run_tokens, slots):
    width, hidden = weight.shape[1:]
    chunk = runs * run_tokens
    chunks = x.shape[0] // chunk
    total = count * chunks * runs * slots
    return pl.pallas_call(
        functools.partial(first_kernel, runs, run_tokens),
        grid=(count, chunks),
        in_specs=[
            pl.BlockSpec((chunk, width), lambda e, c: (c, 0)),
            pl.BlockSpec((1, 1, chunk), lambda e, c: (e + first, 0, c)),
            pl.BlockSpec((1, width, hidden), lambda e, c: (e + first, 0, 0)),
        ],
        out_specs=pl.BlockSpec((runs, 1, 1, slots, hidden), lambda e, c: (0, e, c, 0, 0)),
        out_shape=jax.ShapeDtypeStruct((runs, count, chunks, slots, hidden), jnp.bfloat16),
        scratch_shapes=[pltpu.VMEM((runs * slots, width), jnp.bfloat16)],
        cost_estimate=pl.CostEstimate(
            flops=2 * total * width * (hidden + run_tokens),
            bytes_accessed=2 * (count * width * hidden + total * hidden + x.size),
            transcendentals=0,
        ),
    )(x, keys, weight)


def second_kernel(runs, run_tokens, h_ref, key_ref, gate_ref, w_ref, *refs):
    carry_ref, (out_ref, total_ref) = refs[0] if len(refs) == 3 else None, refs[-2:]
    expert = pl.program_id(1)
    slots = h_ref.shape[3]

    @pl.when(expert == 0)
    def _():
        total_ref[...] = jnp.zeros_like(total_ref) if carry_ref is None else carry_ref[...]

    h = jnp.concatenate([h_ref[j, 0, 0] for j in range(runs)], axis=0)
    result = jnp.dot(h, w_ref[0], preferred_element_type=jnp.float32)
    for j in range(runs):
        span = slice(j * run_tokens, (j + 1) * run_tokens)
        row = lax.broadcasted_iota(jnp.int32, (slots, run_tokens), 0)
        match = row == key_ref[0, :, span]
        gate = jnp.sum(jnp.where(match, gate_ref[0, :, span], 0.0), axis=1, keepdims=True)
        scaled = (result[j * slots : (j + 1) * slots] * gate).astype(jnp.bfloat16)
        total_ref[span, :] += lax.dot_general(
            jnp.where(match, 1.0, 0.0).astype(jnp.bfloat16),
            scaled,
            (((0,), (0,)), ((), ())),
            preferred_element_type=jnp.float32,
        )

    @pl.when(expert == pl.num_programs(1) - 1)
    def _():
        out_ref[...] = total_ref[...].astype(out_ref.dtype)


def second_projection(hidden, keys, gates, weight, carry, kind, first, runs, run_tokens):
    _, count, chunks, slots, depth = hidden.shape
    width = weight.shape[2]
    chunk = runs * run_tokens
    total = count * chunks * runs * slots
    carries = [] if carry is None else [carry]
    return pl.pallas_call(
        functools.partial(second_kernel, runs, run_tokens),
        grid=(chunks, count),
        in_specs=[
            pl.BlockSpec((runs, 1, 1, slots, depth), lambda c, e: (0, e, c, 0, 0)),
            pl.BlockSpec((1, 1, chunk), lambda c, e: (e + first, 0, c)),
            pl.BlockSpec((1, 1, chunk), lambda c, e: (e + first, 0, c)),
            pl.BlockSpec((1, depth, width), lambda c, e: (e + first, 0, 0)),
        ]
        + [pl.BlockSpec((chunk, width), lambda c, e: (c, 0)) for _ in carries],
        out_specs=pl.BlockSpec((chunk, width), lambda c, e: (c, 0)),
        out_shape=jax.ShapeDtypeStruct((chunks * chunk, width), kind),
        scratch_shapes=[pltpu.VMEM((chunk, width), jnp.float32)],
        cost_estimate=pl.CostEstimate(
            flops=2 * total * width * (depth + 3 * run_tokens),
            bytes_accessed=2 * (count * depth * width + total * depth) + 4 * chunks * chunk * width,
            transcendentals=0,
        ),
    )(hidden, keys, gates, weight, *carries)


def per_device(tokens, expert_ids, gate_weights, expert_in, expert_out, shared_in, shared_out):
    row_count, model_width = tokens.shape
    pick_count = expert_ids.shape[1]
    local_count = expert_in.shape[0]
    runs = lax.axis_size("dp")
    block_count = runs * lax.axis_size("expert")
    run_tokens = GROUP * row_count
    slots = GROUP * CAP
    halves = 2 if local_count % 2 == 0 else 1

    normed = layer_norm(tokens)
    full_shared_in = lax.all_gather(shared_in, "dp", axis=0, tiled=True)
    full_shared_out = lax.all_gather(shared_out, "dp", axis=1, tiled=True)

    named = jnp.concatenate([expert_ids.astype(jnp.float32), gate_weights], axis=1).T
    named = lax.all_gather(named, ("expert", "dp"), axis=0, tiled=False)
    ids, gates = named[:, :pick_count], named[:, pick_count:]
    columns = lax.all_to_all(normed, "dp", split_axis=1, concat_axis=0, tiled=True)
    columns, full_shared_in, full_shared_out = lax.optimization_barrier(
        (columns, full_shared_in, full_shared_out)
    )
    x = lax.all_gather(columns, "expert", axis=0, tiled=True)

    owned = lax.axis_index("expert") * local_count + jnp.arange(local_count, dtype=jnp.int32)
    matches = ids[:, :, None, :] == owned.astype(jnp.float32)[:, None]
    chosen = jnp.any(matches, axis=1)
    gate_of = jnp.sum(jnp.where(matches, gates[:, :, None, :], 0.0), axis=1)
    order = jnp.arange(row_count, dtype=jnp.int32)
    before = (order[:, None] < order[None, :]).astype(jnp.bfloat16)
    earlier = jnp.einsum(
        "bej,ji->bei", chosen.astype(jnp.bfloat16), before, preferred_element_type=jnp.float32
    ).astype(jnp.int32)
    base = jnp.arange(block_count, dtype=jnp.int32) % GROUP * CAP
    keys = jnp.where(chosen, earlier + base[:, None, None], -1)

    def by_expert(table):
        return table.transpose(1, 0, 2).reshape(local_count, 1, block_count * row_count)

    keys, gate_of = by_expert(keys), by_expert(gate_of)

    count = local_count // halves
    parts = []
    for half in range(halves):
        pre = first_projection(
            x, keys, expert_in, half * count, count, runs, run_tokens, slots
        )
        parts.append(lax.psum_scatter(pre, "dp", scatter_dimension=0, tiled=True))

    hidden = []
    for pre in parts:
        act = jax.nn.gelu(pre.astype(jnp.float32)).astype(jnp.bfloat16)
        hidden.append(lax.all_gather(act, "dp", axis=0, tiled=True))

    shared_pre = jnp.dot(normed, full_shared_in, preferred_element_type=jnp.float32)
    shared_hidden = jax.nn.gelu(shared_pre).astype(jnp.bfloat16)
    shared_result = jnp.dot(shared_hidden, full_shared_out, preferred_element_type=jnp.float32)

    routed = None
    for half, h in enumerate(hidden):
        kind = jnp.bfloat16 if half == halves - 1 else jnp.float32
        routed = second_projection(
            h, keys, gate_of, expert_out, routed, kind, half * count, runs, run_tokens
        )
    width = routed.shape[1]
    pieces = lax.all_to_all(
        routed.reshape(block_count, row_count, width),
        ("expert", "dp"),
        split_axis=0,
        concat_axis=0,
        tiled=True,
    ).reshape(-1, runs, row_count, width)
    own = jnp.sum(pieces.astype(jnp.float32), axis=0).transpose(1, 0, 2)
    own = own.reshape(row_count, model_width)
    return (tokens.astype(jnp.float32) + shared_result + own).astype(jnp.bfloat16)


def start_of(index, size):
    return pl.ds(pl.multiple_of(index * size, size), size)


HEAD = 2


def plane_orders(planes):
    if planes == 4:
        return ((1, 2, 1, 2), (3, 3, 0, 0), (2, 0, 3, 1))
    return tuple(tuple((z + k) % planes for z in range(planes)) for k in range(1, planes))


def fused_kernel(
    sizes,
    tok_hbm,
    ids_hbm,
    gate_hbm,
    win_hbm,
    wout_hbm,
    sin_hbm,
    sout_hbm,
    out_ref,
    tok,
    ids_in,
    gate_in,
    norm,
    xall,
    meta,
    win,
    wout,
    sin,
    sout,
    keys,
    gates,
    pick,
    gslot,
    rows,
    send,
    recv,
    ssend,
    srecv,
    scaled,
    own,
    other,
    psend,
    precv,
    osend,
    orecv,
    zsend,
    zrecv,
    fsend,
    frecv,
    lsend,
    lrecv,
    lpick,
    lscaled,
    isem,
    lsem,
    wssem,
    wrsem,
    xssem,
    xrsem,
    zssem,
    zrsem,
    rssem,
    rrsem,
    pssem,
    prsem,
    ssem,
    srsem,
    dssem,
    drsem,
    bssem,
    brsem,
    ossem,
    orsem,
    fssem,
    frsem,
    lssem,
    lrsem,
    known,
):
    planes, chips, cores = sizes
    dp = chips * cores
    tok_rows, width = tok.shape
    picks = ids_in.shape[0]
    half = width // chips
    part = half // cores
    experts = win.shape[0]
    local = experts * cores
    slots, span = pick.shape[2:]
    own_rows = chips * tok_rows
    last = planes - 1
    head = min(HEAD, experts // 2)
    close = experts - 2
    piece = slots // cores

    z = lax.axis_index("expert")
    d = lax.axis_index("dp")
    c = d % cores
    x = d // cores
    oc = 1 - c
    ox = 1 - x
    partner = {"dp": x * cores + oc}
    across = {"dp": ox * cores + c}
    mesh_ids = pl.DeviceIdType.MESH

    def remote(src, dst, s_sem, r_sem, device):
        return pltpu.make_async_remote_copy(
            src_ref=src,
            dst_ref=dst,
            send_sem=s_sem,
            recv_sem=r_sem,
            device_id=device,
            device_id_type=mesh_ids,
        )

    def loop(first, end, body):
        def step(i, carry):
            body(i)
            return carry

        lax.fori_loop(first, end, step, 0)

    orders = plane_orders(planes)

    def at_step(k):
        found = 0
        for step, order in enumerate(orders):
            for place, p in enumerate(order):
                hit = jnp.logical_and(k == step, z == place)
                found = jnp.where(hit, p, found)
        return jnp.where(k == last, z, found)

    def mine_of(core):
        return pl.ds(core * experts, experts)

    def local_in():
        return pltpu.make_async_copy(
            win_hbm.at[mine_of(c)], win.at[:, start_of(c, part)], lsem.at[0]
        )

    def local_out():
        return pltpu.make_async_copy(
            wout_hbm.at[mine_of(c)], wout.at[:, :, start_of(c, part)], lsem.at[1]
        )

    def local_shared_in():
        return pltpu.make_async_copy(sin_hbm, sin.at[start_of(c, part)], lsem.at[2])

    def local_shared_out():
        return pltpu.make_async_copy(sout_hbm, sout.at[:, start_of(c, part)], lsem.at[3])

    def partner_in(group):
        first, count = ((0, head), (head, experts - head))[group]
        return remote(
            win_hbm.at[pl.ds(oc * experts + first, count)],
            win.at[pl.ds(first, count), start_of(c, part)],
            wssem.at[group],
            wrsem.at[group],
            partner,
        )

    def partner_out():
        return remote(
            wout_hbm.at[mine_of(oc)],
            wout.at[:, :, start_of(c, part)],
            wssem.at[2],
            wrsem.at[2],
            partner,
        )

    def partner_shared_in():
        return remote(sin_hbm, sin.at[start_of(c, part)], wssem.at[3], wrsem.at[3], partner)

    def partner_shared_out():
        return remote(
            sout_hbm, sout.at[:, start_of(c, part)], wssem.at[4], wrsem.at[4], partner
        )

    def block(p, b, kind):
        return meta.at[p, c * chips + b] if kind else xall.at[p, c, b]

    def token_swap(kind):
        src = meta.at[z, c * chips + x] if kind else norm.at[:, start_of(ox, half)]
        return remote(src, block(z, x, kind), xssem.at[kind], xrsem.at[kind], across)

    def both(p, kind):
        return meta.at[p, pl.ds(c * chips, chips)] if kind else xall.at[p, c]

    def to_plane(p, b, kind):
        ref = block(z, b, kind)
        return remote(ref, ref, zssem.at[kind], zrsem.at[z, kind], {"expert": p})

    def from_plane(p, kind):
        ref = both(p, kind)
        return remote(ref, ref, zssem.at[kind], zrsem.at[p, kind], {"expert": p})

    def send_tokens(k, b):
        for p in range(planes):

            @pl.when(z == orders[k][p])
            def _():
                for kind in (1, 0):
                    to_plane(p, b, kind).start()

    def relay_block(b, kind):
        ref = block(z, b, kind)
        return remote(ref, ref, rssem.at[kind], rrsem.at[z, kind], partner)

    def relay(p, kind):
        ref = both(p, kind)
        return remote(ref, ref, rssem.at[kind], rrsem.at[p, kind], partner)

    def tokens_sent(kind, count, s_sem):
        ref = meta.at[pl.ds(0, count), pl.ds(0, chips)] if kind else xall.at[pl.ds(0, count), 0]
        return remote(ref, ref, s_sem.at[kind], zrsem.at[0, kind], partner)

    def swap(k, e):
        return remote(send.at[k, e], recv.at[k, e], pssem.at[lax.div(k, last)], prsem.at[k, e], across)

    def last_swap(e, g):
        return remote(lsend.at[e, g], lrecv.at[e, g], lssem.at[0], lrsem.at[e, g], across)

    def shared_swap(b):
        return remote(ssend.at[b], srecv.at[b], ssem.at[0], srsem.at[b], across)

    def pair(k):
        return remote(psend.at[k], precv.at[k], dssem.at[0], drsem.at[k], partner)

    def own_pair(b):
        return remote(osend.at[b], orecv.at[b], bssem.at[0], brsem.at[b], partner)

    def give(k):
        return remote(
            zsend.at[k], zrecv.at[z], ossem.at[0], orsem.at[0], {"expert": at_step(k)}
        )

    def given():
        return remote(zsend, zrecv.at[pl.ds(0, last)], ossem.at[0], orsem.at[0], partner)

    def finish():
        return remote(fsend, frecv, fssem.at[0], frsem.at[0], across)

    barrier = pltpu.get_barrier_semaphore()
    hops = (z > 0).astype(jnp.int32) + (z < last).astype(jnp.int32)

    def greet(semaphore):
        for move, there in ((-1, z > 0), (1, z < last)):

            @pl.when(there)
            def _():
                pl.semaphore_signal(
                    semaphore,
                    inc=1,
                    device_id={"expert": z + move},
                    device_id_type=mesh_ids,
                )

    for device in (across, partner):
        pl.semaphore_signal(barrier, inc=1, device_id=device, device_id_type=mesh_ids)
    greet(barrier)
    read_tok = pltpu.make_async_copy(tok_hbm, tok, isem.at[0])
    read_ids = pltpu.make_async_copy(ids_hbm, ids_in, isem.at[1])
    read_gate = pltpu.make_async_copy(gate_hbm, gate_in, isem.at[2])
    read_tok.start()
    read_ids.start()
    read_gate.start()
    local_shared_in().start()
    read_ids.wait()
    read_gate.wait()
    meta[z, c * chips + x, :picks] = ids_in[...].astype(jnp.float32)
    meta[z, c * chips + x, picks:] = gate_in[...]
    read_tok.wait()
    values = tok[...].astype(jnp.float32)
    center = values - jnp.mean(values, axis=-1, keepdims=True)
    spread = jnp.mean(center * center, axis=-1, keepdims=True)
    norm[...] = (center * lax.rsqrt(spread + 1e-06)).astype(jnp.bfloat16)
    xall[z, c, x] = norm[:, start_of(x, half)]

    local_in().start()
    local_shared_out().start()
    local_out().start()
    pl.semaphore_wait(barrier, 2 + hops)
    greet(known.at[0])
    for kind in (1, 0):
        token_swap(kind).start()
    partner_shared_in().start()
    for kind in (1, 0):
        relay_block(x, kind).start()
    partner_in(0).start()
    send_tokens(0, x)

    def shared_first(b):
        pre = jnp.dot(xall[z, c, b], sin[...], preferred_element_type=jnp.float32)
        ssend[b] = pre.astype(jnp.bfloat16)

    local_shared_in().wait()
    partner_shared_in().wait_recv()
    shared_first(x)
    shared_swap(x).start()
    for kind in (1, 0):
        token_swap(kind).wait_recv()
        relay_block(ox, kind).start()
    send_tokens(0, ox)
    partner_in(1).start()
    shared_first(ox)
    shared_swap(ox).start()
    for step in range(1, last):
        pl.semaphore_wait(known.at[step - 1], hops)
        if step < last - 1:
            greet(known.at[step])

    before = jnp.where(
        lax.broadcasted_iota(jnp.int32, (tok_rows, tok_rows), 0)
        < lax.broadcasted_iota(jnp.int32, (tok_rows, tok_rows), 1),
        1.0,
        0.0,
    ).astype(jnp.bfloat16)

    def first_stage(k, turn, mine, weights_next=False):
        p = z if mine else at_step(k)
        if not mine:
            for kind in (1, 0):
                from_plane(p, kind).wait_recv()
                relay(p, kind).start()
            if weights_next:
                partner_shared_out().start()
                partner_out().start()
            for step in range(1, last):

                @pl.when(k == step - 1)
                def _():
                    for b in (x, ox):
                        send_tokens(step, b)

        relay(p, 1).wait_recv()

        ids = jnp.concatenate([meta[p, b, :picks] for b in range(dp)], axis=1)
        weights = jnp.concatenate([meta[p, b, picks:] for b in range(dp)], axis=1)
        chosen, gate = [], []
        for e in range(experts):
            match = ids == (z * local + c * experts + e).astype(jnp.float32)
            chosen.append(jnp.max(jnp.where(match, 1.0, 0.0), axis=0, keepdims=True))
            gate.append(jnp.sum(jnp.where(match, weights, 0.0), axis=0, keepdims=True))
        chosen = jnp.concatenate(chosen, axis=0)
        gates[...] = jnp.concatenate(gate, axis=0)
        for b in range(dp):
            lanes = slice(b * tok_rows, (b + 1) * tok_rows)
            named = chosen[:, lanes]
            earlier = jnp.dot(
                named.astype(jnp.bfloat16), before, preferred_element_type=jnp.float32
            )
            keys[:, lanes] = jnp.where(named > 0.5, earlier + float(b * CAP), -1.0).astype(
                jnp.int32
            )

        def choose(e):
            row = lax.broadcasted_iota(jnp.int32, (slots, span), 0)
            match = row == keys[pl.ds(e, 1), :]
            pick[turn, e] = jnp.where(match, 1.0, 0.0).astype(jnp.bfloat16)
            gate = jnp.sum(
                jnp.where(match, gates[pl.ds(e, 1), :], 0.0), axis=1, keepdims=True
            )
            gslot[turn, e] = jnp.broadcast_to(gate, gslot.shape[2:])

        loop(0, experts, choose)
        relay(p, 0).wait_recv()
        plane = xall[p].reshape(span, half)
        chosen_rows = jnp.dot(
            pick[turn].reshape(experts * slots, span), plane, preferred_element_type=jnp.float32
        )
        rows[...] = chosen_rows.astype(jnp.bfloat16).reshape(rows.shape)

        def project(e):
            pre = jnp.dot(rows[e], win[e], preferred_element_type=jnp.float32)
            send[k, e] = pre.astype(jnp.bfloat16)

        def project_and_send(e):
            project(e)
            swap(k, e).start()

        if mine:
            local_in().wait()
            partner_in(0).wait_recv()
            loop(0, head, project_and_send)
            partner_in(1).wait_recv()
            loop(head, close, project)
            for e in range(close, experts):
                pre = jnp.dot(rows[e], win[e], preferred_element_type=jnp.float32)
                for g in range(cores):
                    lanes = slice(g * own_rows, (g + 1) * own_rows)
                    row = lax.broadcasted_iota(jnp.int32, (piece, own_rows), 0) + g * piece
                    match = row == keys[e : e + 1, lanes]
                    lpick[e - close, g] = jnp.where(match, 1.0, 0.0).astype(jnp.bfloat16)
                    lsend[e - close, g] = pre[g * piece : (g + 1) * piece].astype(jnp.bfloat16)
        else:
            loop(0, experts, project_and_send)

    def second_stage(k, turn, first, end):
        def project(e):
            swap(k, e).wait_recv()
            total = send[k, e].astype(jnp.float32) + recv[k, e].astype(jnp.float32)
            h = jax.nn.gelu(total).astype(jnp.bfloat16)
            result = jnp.dot(h, wout[e], preferred_element_type=jnp.float32)
            scaled[e] = (result * gslot[turn, e][:, :1]).astype(jnp.bfloat16)

        loop(first, end, project)

    def combine(turn, first, end, lanes, count):
        return lax.dot_general(
            pick[turn, first:end, :, lanes].reshape((end - first) * slots, count),
            scaled[first:end].reshape((end - first) * slots, half),
            (((0,), (0,)), ((), ())),
            preferred_element_type=jnp.float32,
        )

    first_stage(last, 2, True)
    first_stage(0, 0, False, True)

    local_shared_out().wait()
    partner_shared_out().wait_recv()

    def shared_second(b):
        shared_swap(b).wait_recv()
        total = ssend[b].astype(jnp.float32) + srecv[b].astype(jnp.float32)
        h = jax.nn.gelu(total).astype(jnp.bfloat16)
        own[start_of(b, tok_rows), :] += jnp.dot(
            h, sout[...], preferred_element_type=jnp.float32
        )

    local_out().wait()
    partner_out().wait_recv()

    second_stage(last, 2, 0, head)
    own[...] = combine(2, 0, head, start_of(c, own_rows), own_rows)
    other[...] = combine(2, 0, head, start_of(oc, own_rows), own_rows)
    for b in range(chips):
        shared_second(b)

    def plane_step(k):
        turn = lax.rem(k, 2)

        @pl.when(k < last - 1)
        def _():
            first_stage(k + 1, lax.rem(k + 1, 2), False)

        @pl.when(k == last - 1)
        def _():
            loop(head, close, lambda e: swap(last, e).start())
            for g in range(cores):
                for e in range(experts - close):
                    last_swap(e, g).start()

        second_stage(k, turn, 0, experts)
        psend[k] = combine(turn, 0, experts, start_of(oc, own_rows), own_rows).astype(
            jnp.bfloat16
        )
        pair(k).start()
        mine = combine(turn, 0, experts, start_of(c, own_rows), own_rows)
        pair(k).wait_recv()
        zsend[k] = (mine + precv[k].astype(jnp.float32)).astype(jnp.bfloat16)
        give(k).start()

    loop(0, last, plane_step)

    second_stage(last, 2, head, close)
    own[...] += combine(2, head, close, start_of(c, own_rows), own_rows)
    other[...] += combine(2, head, close, start_of(oc, own_rows), own_rows)
    given().wait_recv()
    for r in range(1, planes):
        own[...] += zrecv[lax.rem(z + r, planes)].astype(jnp.float32)
    mine = start_of(x, half)
    theirs = start_of(ox, half)

    def last_stage(g):
        extra = None
        for e in range(experts - close):
            last_swap(e, g).wait_recv()
            total = lsend[e, g].astype(jnp.float32) + lrecv[e, g].astype(jnp.float32)
            h = jax.nn.gelu(total).astype(jnp.bfloat16)
            result = jnp.dot(h, wout[close + e], preferred_element_type=jnp.float32)
            gate = gslot[2, close + e, g * piece : (g + 1) * piece, :1]
            lscaled[e, g] = (result * gate).astype(jnp.bfloat16)
            part_sum = lax.dot_general(
                lpick[e, g],
                lscaled[e, g],
                (((0,), (0,)), ((), ())),
                preferred_element_type=jnp.float32,
            )
            extra = part_sum if extra is None else extra + part_sum

        @pl.when(c != g)
        def _():
            other[...] += extra
            for b in (ox, x):
                osend[b] = other[start_of(b, tok_rows), :].astype(jnp.bfloat16)
                own_pair(b).start()

        @pl.when(c == g)
        def _():
            own[...] += extra
            own_pair(ox).wait_recv()
            total = own[start_of(ox, tok_rows), :] + orecv[ox].astype(jnp.float32)
            fsend[...] = total.astype(jnp.bfloat16)
            finish().start()

    for g in range(cores):
        last_stage(g)
    own_pair(x).wait_recv()
    total = own[start_of(x, tok_rows), :] + orecv[x].astype(jnp.float32)
    out_ref[:, mine] = (tok[:, mine].astype(jnp.float32) + total).astype(out_ref.dtype)

    for kind in (0, 1):
        token_swap(kind).wait_send()
        tokens_sent(kind, last, zssem).wait_send()
        tokens_sent(kind, planes, rssem).wait_send()
        partner_in(kind).wait_send()
    partner_shared_in().wait_send()
    partner_shared_out().wait_send()
    partner_out().wait_send()
    remote(send.at[pl.ds(0, last)], recv.at[pl.ds(0, last)], pssem.at[0], prsem.at[0, 0], across).wait_send()
    remote(
        send.at[last, pl.ds(0, close)],
        recv.at[last, pl.ds(0, close)],
        pssem.at[1],
        prsem.at[0, 0],
        across,
    ).wait_send()
    remote(lsend, lrecv, lssem.at[0], lrsem.at[0, 0], across).wait_send()
    remote(ssend, srecv, ssem.at[0], srsem.at[0], across).wait_send()
    remote(osend, orecv, bssem.at[0], brsem.at[0], partner).wait_send()
    remote(psend, precv, dssem.at[0], drsem.at[0], partner).wait_send()
    given().wait_send()

    finish().wait()
    out_ref[:, theirs] = (
        tok[:, theirs].astype(jnp.float32) + frecv[...].astype(jnp.float32)
    ).astype(out_ref.dtype)


def fused(tokens, expert_ids, gate_weights, expert_in, expert_out, shared_in, shared_out):
    tok_rows, width = tokens.shape
    picks = expert_ids.shape[1]
    planes, dp = lax.axis_size("expert"), lax.axis_size("dp")
    cores, chips = 2, dp // 2
    local, part, hidden = expert_in.shape
    experts = local // cores
    half = width // chips
    slots, span = dp * CAP, dp * tok_rows
    own_rows = chips * tok_rows
    bf16, f32 = jnp.bfloat16, jnp.float32
    vmem, dma = pltpu.VMEM, pltpu.SemaphoreType.DMA
    scratch = [
        vmem((tok_rows, width), bf16),
        vmem((picks, tok_rows), jnp.int32),
        vmem((picks, tok_rows), f32),
        vmem((tok_rows, width), bf16),
        vmem((planes, cores, chips, tok_rows, half), bf16),
        vmem((planes, dp, 2 * picks, tok_rows), f32),
        vmem((experts, half, hidden), bf16),
        vmem((experts, hidden, half), bf16),
        vmem((half, hidden), bf16),
        vmem((hidden, half), bf16),
        vmem((experts, span), jnp.int32),
        vmem((experts, span), f32),
        vmem((3, experts, slots, span), bf16),
        vmem((3, experts, slots, 128), f32),
        vmem((experts, slots, half), bf16),
        vmem((planes, experts, slots, hidden), bf16),
        vmem((planes, experts, slots, hidden), bf16),
        vmem((chips, tok_rows, hidden), bf16),
        vmem((chips, tok_rows, hidden), bf16),
        vmem((experts, slots, half), bf16),
        vmem((own_rows, half), f32),
        vmem((own_rows, half), f32),
        vmem((planes - 1, own_rows, half), bf16),
        vmem((planes - 1, own_rows, half), bf16),
        vmem((chips, tok_rows, half), bf16),
        vmem((chips, tok_rows, half), bf16),
        vmem((planes - 1, own_rows, half), bf16),
        vmem((planes, own_rows, half), bf16),
        vmem((tok_rows, half), bf16),
        vmem((tok_rows, half), bf16),
        vmem((2, cores, slots // cores, hidden), bf16),
        vmem((2, cores, slots // cores, hidden), bf16),
        vmem((2, cores, slots // cores, own_rows), bf16),
        vmem((2, cores, slots // cores, half), bf16),
        dma((3,)),
        dma((4,)),
    ]
    pairs = [
        ((5,), (5,)),
        ((2,), (2,)),
        ((2,), (planes, 2)),
        ((2,), (planes, 2)),
        ((2,), (planes, experts)),
        ((1,), (chips,)),
        ((1,), (planes - 1,)),
        ((1,), (chips,)),
        ((1,), (1,)),
        ((1,), (1,)),
        ((1,), (2, cores)),
    ]
    for sent, received in pairs:
        scratch += [dma(sent), dma(received)]
    scratch.append(pltpu.SemaphoreType.REGULAR((planes - 2,)))
    given = (tokens, expert_ids.T, gate_weights.T, expert_in, expert_out, shared_in, shared_out)
    given = [pltpu.with_memory_space_constraint(a, pltpu.HBM) for a in given]
    apart = pl.BlockSpec(memory_space=pl.ANY)
    return pl.pallas_call(
        functools.partial(fused_kernel, (planes, chips, cores)),
        in_specs=[apart] * 7,
        out_specs=pl.BlockSpec(memory_space=pltpu.VMEM),
        out_shape=jax.ShapeDtypeStruct((tok_rows, width), tokens.dtype),
        scratch_shapes=scratch,
        compiler_params=pltpu.CompilerParams(
            collective_id=0, has_side_effects=True, vmem_limit_bytes=56098816
        ),
    )(*given)


def fits(mesh, args):
    planes, dp = mesh.shape["expert"], mesh.shape["dp"]
    tokens, expert_in = args[0], args[3]
    return (
        dp == 4
        and planes == 4
        and expert_in.shape[0] // (mesh.shape["sweep"] * planes) % 2 == 0
        and expert_in.shape[0] // (mesh.shape["sweep"] * planes) <= 16
        and tokens.shape[0] // (mesh.shape["sweep"] * planes * dp) == 128
    )


def solution(mesh):
    placed = (
        P(("sweep", "expert", "dp"), None),
        P(("sweep", "expert", "dp"), None),
        P(("sweep", "expert", "dp"), None),
        P(("sweep", "expert"), "dp", None),
        P(("sweep", "expert"), None, "dp"),
        P(("sweep", "dp"), None),
        P("sweep", "dp"),
    )

    def run(*args):
        return jax.shard_map(
            fused if fits(mesh, args) else per_device,
            mesh=mesh,
            in_specs=placed,
            out_specs=P(("sweep", "expert", "dp"), None),
            check_vma=False,
        )(*args)

    return run
```
